256 devices in a mesh: section: 2 (over core), fsdp: 8 (over y, x_hi), tp: 16 (over z, x_lo).
Axes of the slice: x: 4 (x_hi: 2, x_lo: 2; x = x_hi * 2 + x_lo), y: 4, z: 8, core: 2. Of those that a mesh axis runs over, the one named last changes fastest.
Arguments:
- saved_inputs: bfloat16 [2, 8, 512, 2560], P('section', None, 'fsdp', 'tp'), may hold values from -6 to 6
- top_grad: bfloat16 [8, 512, 2560], P(None, 'fsdp', 'tp'), may hold values from -6 to 6
- norm_gain: float32 [2, 2560], P('section'), may hold values from 0.5 to 1.5
- gate_weight: bfloat16 [2, 2560, 6912], P('section', 'fsdp', 'tp'), may hold values from -0.125 to 0.125
- up_weight: bfloat16 [2, 2560, 6912], P('section', 'fsdp', 'tp'), may hold values from -0.125 to 0.125
- down_weight: bfloat16 [2, 6912, 2560], P('section', 'tp', 'fsdp'), may hold values from -0.078125 to 0.078125
Outputs:
- input_grads: bfloat16 [2, 8, 512, 2560], P('section', None, 'fsdp', 'tp')
- gate_grad: float32 [2, 2560, 6912], P('section', 'fsdp', 'tp')
- up_grad: float32 [2, 2560, 6912], P('section', 'fsdp', 'tp')
- down_grad: float32 [2, 6912, 2560], P('section', 'tp', 'fsdp')
- gain_grad: float32 [2, 2560], P('section', 'tp')
The draws below stay inside these ranges and needn't reach their ends.
All inputs are finite; a program needn't handle non-finite values.
Results may differ from the reference program's by a relative error of at most 0.0055.
Values may be sent and summed in bfloat16 or wider, within the bound.
A program may use at most 128 MiB of HBM per device.

```python
import jax
import jax.numpy as jnp
from jax import lax

D = 2560
FF = 6912
MICRO = 8
SECTIONS = 2
TOKENS = 512


def block_levels(key, shape, pieces, least, high):
    factor_of = 1.0
    for position, shards_of in pieces:
        steps = jax.random.uniform(jax.random.fold_in(jax.random.fold_in(key, 6), position), (shards_of,), jnp.float32, least / len(pieces), high / len(pieces))
        factor_of = factor_of * jnp.repeat(jnp.exp(steps), shape[position] // shards_of).reshape((-1,) + (1,) * (len(shape) - 1 - position))
    return factor_of


def scatter_about(rng, dims, width, limit, cuts=(), kind=jnp.bfloat16):
    factor_of = block_levels(rng, dims, cuts, -0.22, 0.18) if cuts else 1.0
    drawn = jax.random.normal(rng, dims, jnp.float32) * width * factor_of
    return jnp.minimum(jnp.maximum(drawn, -limit), limit).astype(kind)


def setup_inputs(seed: int = 0) -> dict:
    streams_of = jax.random.split(jax.random.key(seed), 7)
    saved_inputs = scatter_about(streams_of[0], (SECTIONS, MICRO, TOKENS, D), 1.0, 6.0, ((0, 2), (2, 8), (3, 16)))
    top_grad = scatter_about(streams_of[1], (MICRO, TOKENS, D), 1.0, 6.0, ((1, 8), (2, 16)))
    norm_gain = jnp.clip(1.0 + 0.1 * jax.random.normal(streams_of[2], (SECTIONS, D), jnp.float32), 0.5, 1.5)
    gate_weight = scatter_about(streams_of[3], (SECTIONS, D, FF), D ** -0.5, 0.125, ((0, 2), (1, 8), (2, 16)))
    up_weight = scatter_about(streams_of[4], (SECTIONS, D, FF), D ** -0.5, 0.125, ((0, 2), (1, 8), (2, 16)))
    down_weight = scatter_about(streams_of[5], (SECTIONS, FF, D), FF ** -0.5, 0.078125, ((0, 2), (1, 16), (2, 8)))
    return {"saved_inputs": saved_inputs, "top_grad": top_grad, "norm_gain": norm_gain, "gate_weight": gate_weight, "up_weight": up_weight, "down_weight": down_weight}


epsilon = 1e-05

def layer_backward(inputs, cotangent, gain_row, w_gate, w_up, w_down):
    inputs_wide = inputs.astype(jnp.float32)
    row_scale = lax.rsqrt(lax.optimization_barrier(jnp.mean(inputs_wide * inputs_wide, axis=-1, keepdims=True)) + epsilon)
    unit_rows = inputs_wide * row_scale
    normed = (unit_rows * gain_row).astype(jnp.bfloat16)
    gate_pre = jnp.dot(normed, w_gate, preferred_element_type=jnp.float32)
    upward = jnp.dot(normed, w_up, preferred_element_type=jnp.float32)
    gate_sigmoid = jax.nn.sigmoid(gate_pre)
    silu_out = gate_pre * gate_sigmoid
    hidden = (silu_out * upward).astype(jnp.bfloat16)
    d_hidden = jnp.dot(cotangent, w_down.T, preferred_element_type=jnp.float32)
    d_gate = (d_hidden * upward * gate_sigmoid * (1.0 + gate_pre * (1.0 - gate_sigmoid))).astype(jnp.bfloat16)
    d_up = (d_hidden * silu_out).astype(jnp.bfloat16)
    d_normed = jnp.dot(d_gate, w_gate.T, preferred_element_type=jnp.float32) + jnp.dot(d_up, w_up.T, preferred_element_type=jnp.float32)
    scaled = d_normed * gain_row
    norm_stat = lax.optimization_barrier(jnp.mean(scaled * unit_rows, axis=-1, keepdims=True))
    d_inputs = (cotangent.astype(jnp.float32) + row_scale * (scaled - unit_rows * norm_stat)).astype(jnp.bfloat16)
    gate_term = jnp.dot(normed.T, d_gate, preferred_element_type=jnp.float32)
    up_term = jnp.dot(normed.T, d_up, preferred_element_type=jnp.float32)
    down_term = jnp.dot(hidden.T, cotangent, preferred_element_type=jnp.float32)
    gain_term = lax.optimization_barrier(jnp.sum(d_normed * unit_rows, axis=0))
    return (d_inputs, (gate_term, up_term, down_term, gain_term))

def reference(saved_inputs, top_grad, norm_gain, gate_weight, up_weight, down_weight):
    incoming = top_grad
    per_section = []
    for section_number in range(SECTIONS - 1, -1, -1):

        def one_micro(totals, paired):
            d_inputs, gradients = layer_backward(paired[0], paired[1], norm_gain[section_number], gate_weight[section_number], up_weight[section_number], down_weight[section_number])
            summed = (totals[0] + gradients[0], totals[1] + gradients[1], totals[2] + gradients[2], totals[3] + gradients[3])
            return (summed, d_inputs)
        zeros_init = (jnp.zeros((D, FF), jnp.float32), jnp.zeros((D, FF), jnp.float32), jnp.zeros((FF, D), jnp.float32), jnp.zeros((D,), jnp.float32))
        totals, incoming = lax.scan(one_micro, zeros_init, (saved_inputs[section_number], incoming))
        per_section.append((incoming, totals[0], totals[1], totals[2], totals[3]))
    ordered = per_section[::-1]
    input_grads = jnp.stack([item[0] for item in ordered])
    gate_grad = jnp.stack([item[1] for item in ordered])
    up_grad = jnp.stack([item[2] for item in ordered])
    down_grad = jnp.stack([item[3] for item in ordered])
    gain_grad = jnp.stack([item[4] for item in ordered])
    return (input_grads, gate_grad, up_grad, down_grad, gain_grad)
```

```python
import functools

import jax
import jax.numpy as jnp
from jax import lax
from jax.experimental import pallas as pl
from jax.experimental.pallas import tpu as pltpu
from jax.sharding import PartitionSpec as P

EPS = 1e-05
MESH = pl.DeviceIdType.MESH
F32 = jnp.float32
BF16 = jnp.bfloat16

NY, NXH, NZ, NXL = 4, 2, 8, 2
NF, NT = NY * NXH, NZ * NXL
MICRO = 8
ROWS = 64
T = MICRO * ROWS
W = 160
PW = NXL * W
FL = 432
GU = 2 * FL
D = W * NT


def dot(a, b, ca, cb, precision=None):
    return lax.dot_general(
        a, b, (((ca,), (cb,)), ((), ())), preferred_element_type=F32, precision=precision
    )


def fused_kernel(
    x_ref,
    tg_ref,
    gain_ref,
    wg_ref,
    wu_ref,
    wd_ref,
    dx_ref,
    gg_ref,
    ug_ref,
    dg_ref,
    gn_ref,
    wgu,
    wd,
    n_all,
    dy_all,
    gu,
    dh,
    dgu,
    hid,
    unit,
    scale,
    stat,
    ssq_in,
    stat_in,
    gain_in,
    pdn,
    rdn,
    xs,
    xr,
    pgu,
    rgu,
    pd,
    rd,
    ssem,
    rsem,
):
    s = lax.axis_index("section")
    f = lax.axis_index("fsdp")
    t = lax.axis_index("tp")
    y, xh = lax.div(f, NXH), lax.rem(f, NXH)
    z, xl = lax.div(t, NXL), lax.rem(t, NXL)

    def at_y(step, col=None):
        return (s, lax.rem(y + step + NY, NY) * NXH + xh, t)

    def at_z(step):
        return (s, f, lax.rem(z + step + NZ, NZ) * NXL + xl)

    yp, ym, zp, zm = at_y(1), at_y(-1), at_z(1), at_z(-1)
    xhp = (s, y * NXH + (1 - xh), t)
    xlp = (s, f, z * NXL + (1 - xl))
    core = (1 - s, f, t)
    tp_peers = [(s, f, lax.rem(t + k, NT)) for k in range(1, NT)]
    fs_peers = [(s, lax.rem(f + k, NF), t) for k in range(1, NF)]

    count = [0]
    started = []

    def message():
        count[0] += 1
        return count[0] - 1

    def copy(src, dst, m, dev):
        return pltpu.make_async_remote_copy(
            src_ref=src,
            dst_ref=dst,
            send_sem=ssem.at[m],
            recv_sem=rsem.at[m],
            device_id=dev,
            device_id_type=MESH,
        )

    def send(src, dst, m, dev):
        copy(src, dst, m, dev).start()

    def sent(buf, lead, m):
        started.append((buf, lead, m))

    def arrived(dst, m):
        copy(dst, dst, m, core).wait_recv()

    def rows(n, step, fn):
        def body(i, c):
            fn(pl.multiple_of(i * step, step))
            return c

        lax.fori_loop(0, n // step, body, 0)

    barrier = pltpu.get_barrier_semaphore()
    for dev in tp_peers + fs_peers + [core]:
        pl.semaphore_signal(barrier, inc=1, device_id=dev, device_id_type=MESH)

    eye = (
        lax.broadcasted_iota(jnp.int32, (W, W), 0) == lax.broadcasted_iota(jnp.int32, (W, W), 1)
    ).astype(BF16)

    def pack(r):
        wgu[f, pl.ds(r, 32), 0:FL] = wg_ref[pl.ds(r, 32), :]
        wgu[f, pl.ds(r, 32), FL:GU] = wu_ref[pl.ds(r, 32), :]

    rows(PW, 32, pack)

    def pack_down(r):
        wd[f, pl.ds(r, 48), :] = wd_ref[pl.ds(r, 48), :]

    rows(FL, 48, pack_down)
    xt = dot(eye, x_ref[...], 1, 1)
    ssq_in[t] = jnp.sum(xt * xt, axis=0, keepdims=True)
    unit[...] = xt

    @pl.when(s == 1)
    def _():
        dy_all[z, xl] = dot(eye, tg_ref[...], 1, 1).astype(BF16)

    pl.semaphore_wait(barrier, NT - 1 + NF - 1 + 1)

    def weights_own():
        for arr in (wgu, wd):
            for dev in (yp, ym, xhp):
                m = message()
                send(arr.at[f], arr.at[f], m, dev)
                sent(arr, 1, m)

    mark_w = count[0]
    weights_own()

    def left_block(col):
        return lax.rem(y + NY - 1, NY) * NXH + col

    def right_block(col):
        return lax.rem(y + 1, NY) * NXH + col

    far = lax.rem(y + 2, NY) * NXH

    m_ssq = count[0]
    for k, dev in enumerate(tp_peers):
        m = message()
        send(ssq_in.at[t], ssq_in.at[t], m, dev)
        sent(ssq_in, 1, m)

    def gather_steps(buf):
        ms = [message() for _ in range(9)]

        def start():
            send(buf.at[z, xl], buf.at[z, xl], ms[0], xlp)
            sent(buf, 2, ms[0])

        def step(k):
            fwd = lax.rem(z + NZ - (k - 1), NZ)
            bwd = lax.rem(z + (k - 1), NZ)
            if k == 1:
                arrived(buf.at[z, 1 - xl], ms[0])
            else:
                arrived(buf.at[fwd], ms[2 * k - 3])
                arrived(buf.at[bwd], ms[2 * k - 2])
            a = buf.at[fwd] if k < 4 else buf.at[fwd, 0]
            b = buf.at[bwd] if k < 4 else buf.at[bwd, 1]
            send(a, a, ms[2 * k - 1], zp)
            send(b, b, ms[2 * k], zm)
            like = (buf, 1) if k < 4 else (buf, 2)
            sent(*like, ms[2 * k - 1])
            sent(*like, ms[2 * k])

        def finish():
            opp = lax.rem(z + 4, NZ)
            arrived(buf.at[opp, 0], ms[7])
            arrived(buf.at[opp, 1], ms[8])

        return start, step, finish

    n_start, n_step, n_finish = gather_steps(n_all)
    d_start, d_step, d_finish = gather_steps(dy_all)
    m_core = message()

    @pl.when(s == 1)
    def _():
        d_start()

    for k in range(1, NT):
        arrived(ssq_in.at[lax.rem(t + NT - k, NT)], m_ssq + k - 1)
    total = ssq_in[0]
    for k in range(1, NT):
        total = total + ssq_in[k]
    row_scale = lax.rsqrt(total / D + EPS)
    scale[...] = row_scale
    u = unit[...] * row_scale
    unit[...] = u
    n_all[z, xl] = (u * gain_ref[:, 0:1]).astype(BF16)
    n_start()

    m_pass = count[0]
    for _ in range(8):
        message()

    def weights_partner():
        for j, arr in enumerate((wgu, wd)):
            blk = arr.at[y * NXH + (1 - xh)]
            arrived(blk, mark_w + 3 * j + 2)
            for q, dev in enumerate((yp, ym)):
                send(blk, blk, m_pass + 4 * j + q, dev)
                sent(arr, 1, m_pass + 4 * j + q)

    def weights_far():
        for j, arr in enumerate((wgu, wd)):
            arrived(arr.at[left_block(xh)], mark_w + 3 * j + 0)
            arrived(arr.at[right_block(xh)], mark_w + 3 * j + 1)
            arrived(arr.at[left_block(1 - xh)], m_pass + 4 * j + 0)
            arrived(arr.at[right_block(1 - xh)], m_pass + 4 * j + 1)
            a, b = arr.at[left_block(0)], arr.at[right_block(1)]
            send(a, a, m_pass + 4 * j + 2, yp)
            send(b, b, m_pass + 4 * j + 3, ym)
            sent(arr, 1, m_pass + 4 * j + 2)
            sent(arr, 1, m_pass + 4 * j + 3)

    def weights_last():
        for j, arr in enumerate((wgu, wd)):
            arrived(arr.at[far], m_pass + 4 * j + 2)
            arrived(arr.at[far + 1], m_pass + 4 * j + 3)

    @pl.when(s == 1)
    def _():
        d_step(1)
        n_step(1)
        d_step(2)
        n_step(2)
        weights_partner()
        d_step(3)
        n_step(3)
        d_step(4)
        n_step(4)
        weights_far()
        d_finish()
        n_finish()
        weights_last()

    mid = list(started)
    del started[:]

    @pl.when(s == 0)
    def _():
        n_step(1)
        n_step(2)
        weights_partner()
        n_step(3)
        n_step(4)
        weights_far()
        n_finish()
        weights_last()

    del started[:]

    gu[...] = jnp.zeros_like(gu)

    def fwd(i, c):
        gu[...] += dot(wgu[i], n_all[i].reshape(PW, T), 0, 0)
        return c

    lax.fori_loop(0, NF, fwd, 0)

    @pl.when(s == 0)
    def _():
        arrived(dy_all.at[z, xl], m_core)
        d_start()
        for k in range(1, 5):
            d_step(k)
        d_finish()

    del started[:]

    dh[...] = jnp.zeros_like(dh)

    def dhid(i, c):
        dh[...] += dot(wd[i], dy_all[i].reshape(PW, T), 1, 0)
        return c

    lax.fori_loop(0, NF, dhid, 0)

    stat[...] = jnp.zeros_like(stat)

    def elementwise(r):
        gate = gu[pl.ds(r, 16), :]
        up = gu[pl.ds(pl.multiple_of(FL + r, 16), 16), :]
        dd = dh[pl.ds(r, 16), :]
        sig = jax.nn.sigmoid(gate)
        silu = gate * sig
        hid[pl.ds(r, 16), :] = (silu * up).astype(BF16)
        d_gate = (dd * up * sig * (1.0 + gate * (1.0 - sig))).astype(BF16)
        d_up = (dd * silu).astype(BF16)
        dgu[pl.ds(r, 16), :] = d_gate
        dgu[pl.ds(pl.multiple_of(FL + r, 16), 16), :] = d_up
        both = d_gate.astype(F32) * gate + d_up.astype(F32) * up
        stat[...] += both[0:8] + both[8:16]

    rows(FL, 16, elementwise)

    stat_in[t] = jnp.sum(stat[...], axis=0, keepdims=True)
    m_stat = count[0]
    for k, dev in enumerate(tp_peers):
        m = message()
        send(stat_in.at[t], stat_in.at[t], m, dev)
        sent(stat_in, 1, m)

    def dnormed(i, c):
        blk = lax.rem(z + 4 + i, NZ)
        pdn[blk] = dot(wgu[blk], dgu[...], 1, 0).astype(BF16).reshape(NXL, W, T)
        return c

    def add(dst, at, src, at_src, n, step):
        def body(r):
            a = dst[(*at, pl.ds(r, step), slice(None))].astype(F32)
            b = src[(*at_src, pl.ds(r, step), slice(None))].astype(F32)
            dst[(*at, pl.ds(r, step), slice(None))] = (a + b).astype(BF16)

        rows(n, step, body)

    ms = [message() for _ in range(9)]
    lax.fori_loop(0, 1, dnormed, 0)
    opp = lax.rem(z + 4, NZ)
    send(pdn.at[opp, 0], rdn.at[0, 0, 0], ms[0], zp)
    send(pdn.at[opp, 1], rdn.at[1, 0, 1], ms[1], zm)
    sent(pdn, 2, ms[0])
    sent(pdn, 2, ms[1])
    lax.fori_loop(1, NZ, dnormed, 0)
    for k in range(2, 5):
        fwd_blk = lax.rem(z + 5 - k, NZ)
        bwd_blk = lax.rem(z + NZ - 5 + k, NZ)
        for way, blk, dev in ((0, fwd_blk, zp), (1, bwd_blk, zm)):
            m_in = ms[2 * (k - 2) + way]
            halves = (way,) if k == 2 else (0, 1)
            if k == 2:
                arrived(rdn.at[way, 0, way], m_in)
            else:
                arrived(rdn.at[way, k - 2], m_in)
            for hf in halves:
                add(pdn, (blk, hf), rdn, (way, k - 2, hf), W, 32)
            m = ms[2 * (k - 1) + way]
            send(pdn.at[blk], rdn.at[way, k - 1], m, dev)
            sent(pdn, 1, m)
    arrived(rdn.at[0, 3], ms[6])
    arrived(rdn.at[1, 3], ms[7])
    for q in (1 - xl,):
        xs[...] = (
            pdn[z, q].astype(F32) + rdn[0, 3, q].astype(F32) + rdn[1, 3, q].astype(F32)
        ).astype(BF16)
    send(xs, xr, ms[8], xlp)
    sent(xs, 0, ms[8])

    for k in range(1, NT):
        arrived(stat_in.at[lax.rem(t + NT - k, NT)], m_stat + k - 1)
    norm_stat = stat_in[0]
    for k in range(1, NT):
        norm_stat = norm_stat + stat_in[k]
    norm_stat = norm_stat / D
    arrived(xr, ms[8])
    d_normed = (
        pdn[z, xl].astype(F32)
        + rdn[0, 3, xl].astype(F32)
        + rdn[1, 3, xl].astype(F32)
        + xr[...].astype(F32)
    )
    u = unit[...]
    dx = (
        dy_all[z, xl].astype(F32) + scale[...] * (d_normed * gain_ref[:, 0:1] - u * norm_stat)
    ).astype(BF16)
    xs_out = dx

    @pl.when(s == 1)
    def _():
        xr[...] = xs_out
        send(xr, dy_all.at[z, xl], m_core, core)

    gain_part = dot(jnp.ones((8, T), F32), d_normed * u, 1, 1, lax.Precision.HIGHEST)
    gain_in[f] = gain_part
    m_gain = count[0]
    for k, dev in enumerate(fs_peers):
        m = message()
        send(gain_in.at[f], gain_in.at[f], m, dev)
        sent(gain_in, 1, m)
    dx_ref[...] = dot(xs_out, eye, 0, 0).astype(BF16)

    def wgrad(i, c):
        pgu[i] = dot(n_all[i].reshape(PW, T), dgu[...], 1, 1).astype(BF16)
        pd[i] = dot(hid[...], dy_all[i].reshape(PW, T), 1, 1).astype(BF16)
        return c

    lax.fori_loop(0, NF, wgrad, 0)

    m_g = count[0]
    for _ in range(14):
        message()
    groups = ((pgu, rgu, PW, 32, m_g), (pd, rd, FL, 48, m_g + 7))
    for p, r, n, st, m0 in groups:
        send(p.at[far], r.at[0], m0, yp)
        send(p.at[far + 1], r.at[1], m0 + 1, ym)
        sent(p, 1, m0)
        sent(p, 1, m0 + 1)
    for p, r, n, st, m0 in groups:
        right, left = right_block(0), left_block(0)
        send(p.at[right + 1], r.at[3], m0 + 3, yp)
        sent(p, 1, m0 + 3)
        send(p.at[left], r.at[4], m0 + 4, ym)
        sent(p, 1, m0 + 4)
        arrived(r.at[0], m0)
        add(p, (right,), r, (0,), n, st)
        send(p.at[right], r.at[2], m0 + 2, yp)
        sent(p, 1, m0 + 2)
        arrived(r.at[1], m0 + 1)
        add(p, (left + 1,), r, (1,), n, st)
        send(p.at[left + 1], r.at[5], m0 + 5, ym)
        sent(p, 1, m0 + 5)
    for p, r, n, st, m0 in groups:
        for q in range(2, 6):
            arrived(r.at[q], m0 + q)
        other = y * NXH + (1 - xh)

        def partner(rr, p=p, r=r, st=st, other=other):
            p[other, pl.ds(rr, st), :] = (
                p[other, pl.ds(rr, st), :].astype(F32)
                + r[2 + (1 - xh), pl.ds(rr, st), :].astype(F32)
                + r[4 + (1 - xh), pl.ds(rr, st), :].astype(F32)
            ).astype(BF16)

        rows(n, st, partner)
        send(p.at[other], r.at[6], m0 + 6, xhp)
        sent(p, 1, m0 + 6)
    for p, r, n, st, m0 in groups:
        arrived(r.at[6], m0 + 6)

        def final(rr, p=p, r=r, st=st):
            v = (
                p[f, pl.ds(rr, st), :].astype(F32)
                + r[2 + xh, pl.ds(rr, st), :].astype(F32)
                + r[4 + xh, pl.ds(rr, st), :].astype(F32)
                + r[6, pl.ds(rr, st), :].astype(F32)
            )
            if p is pgu:
                gg_ref[pl.ds(rr, st), :] = v[:, 0:FL]
                ug_ref[pl.ds(rr, st), :] = v[:, FL:GU]
            else:
                dg_ref[pl.ds(rr, st), :] = v

        rows(n, st, final)

    for k in range(1, NF):
        arrived(gain_in.at[lax.rem(f + NF - k, NF)], m_gain + k - 1)
    gsum = gain_in[0]
    for k in range(1, NF):
        gsum = gsum + gain_in[k]
    gn_ref[...] = gsum

    for buf, lead, m in mid + started:
        like = buf.at[(0,) * lead] if lead else buf
        copy(like, like, m, core).wait_send()

    @pl.when(s == 1)
    def _():
        copy(xr, xr, m_core, core).wait_send()

    assert count[0] <= ssem.shape[0], count[0]


NSEM = 120


def body(saved_inputs, top_grad, norm_gain, gate_weight, up_weight, down_weight):
    x = saved_inputs.reshape(T, W)
    tg = top_grad.reshape(T, W)
    gain = lax.dynamic_slice_in_dim(norm_gain[0], lax.axis_index("tp") * W, W)
    gain = jnp.broadcast_to(gain[:, None], (W, 128))
    vm = pl.BlockSpec(memory_space=pltpu.VMEM)
    out = pl.pallas_call(
        fused_kernel,
        name="fused",
        out_shape=(
            jax.ShapeDtypeStruct((T, W), BF16),
            jax.ShapeDtypeStruct((PW, FL), F32),
            jax.ShapeDtypeStruct((PW, FL), F32),
            jax.ShapeDtypeStruct((FL, PW), F32),
            jax.ShapeDtypeStruct((8, W), F32),
        ),
        in_specs=[vm] * 6,
        out_specs=[vm] * 5,
        scratch_shapes=[
            pltpu.VMEM((NF, PW, GU), BF16),
            pltpu.VMEM((NF, FL, PW), BF16),
            pltpu.VMEM((NZ, NXL, W, T), BF16),
            pltpu.VMEM((NZ, NXL, W, T), BF16),
            pltpu.VMEM((GU, T), F32),
            pltpu.VMEM((FL, T), F32),
            pltpu.VMEM((GU, T), BF16),
            pltpu.VMEM((FL, T), BF16),
            pltpu.VMEM((W, T), F32),
            pltpu.VMEM((1, T), F32),
            pltpu.VMEM((8, T), F32),
            pltpu.VMEM((NT, 1, T), F32),
            pltpu.VMEM((NT, 1, T), F32),
            pltpu.VMEM((NF, 8, W), F32),
            pltpu.VMEM((NZ, NXL, W, T), BF16),
            pltpu.VMEM((2, 4, NXL, W, T), BF16),
            pltpu.VMEM((W, T), BF16),
            pltpu.VMEM((W, T), BF16),
            pltpu.VMEM((NF, PW, GU), BF16),
            pltpu.VMEM((7, PW, GU), BF16),
            pltpu.VMEM((NF, FL, PW), BF16),
            pltpu.VMEM((7, FL, PW), BF16),
            pltpu.SemaphoreType.DMA((NSEM,)),
            pltpu.SemaphoreType.DMA((NSEM,)),
        ],
        compiler_params=pltpu.CompilerParams(
            collective_id=0, has_side_effects=True, vmem_limit_bytes=62 * 2**20
        ),
    )(x, tg, gain, gate_weight[0], up_weight[0], down_weight[0])
    dx, gg, ug, dg, gn = out
    return (
        dx.reshape(1, MICRO, ROWS, W),
        gg[None],
        ug[None],
        dg[None],
        gn[0:1],
    )


def solution(mesh):
    return jax.shard_map(
        body,
        mesh=mesh,
        in_specs=(
            P("section", None, "fsdp", "tp"),
            P(None, "fsdp", "tp"),
            P("section", None),
            P("section", "fsdp", "tp"),
            P("section", "fsdp", "tp"),
            P("section", "tp", "fsdp"),
        ),
        out_specs=(
            P("section", None, "fsdp", "tp"),
            P("section", "fsdp", "tp"),
            P("section", "fsdp", "tp"),
            P("section", "tp", "fsdp"),
            P("section", "tp"),
        ),
        check_vma=False,
    )
```

```python
import jax
import jax.numpy as jnp
from jax import lax
from jax.experimental import pallas as pl
from jax.experimental.pallas import tpu as pltpu
from jax.sharding import PartitionSpec as P

EPS = 1e-05
MESH = pl.DeviceIdType.MESH
F32 = jnp.float32
BF16 = jnp.bfloat16

NY, NXH, NZ, NXL = 4, 2, 8, 2
NF, NT = NY * NXH, NZ * NXL
MICRO = 8
ROWS = 64
T = MICRO * ROWS
H = 2
TH = T // H
W = 160
PW = NXL * W
FL = 432
GU = 2 * FL
D = W * NT
NSEM = 200


def scope(name):
    return jax.named_scope(name)


def dot(a, b, ca, cb, precision=None):
    return lax.dot_general(
        a, b, (((ca,), (cb,)), ((), ())), preferred_element_type=F32, precision=precision
    )


def fused_kernel(
    x_ref,
    tg_ref,
    gain_ref,
    wg_ref,
    wu_ref,
    wd_ref,
    dx_ref,
    gg_ref,
    ug_ref,
    dg_ref,
    gn_ref,
    wgu,
    wd,
    n_all,
    dy_all,
    gu,
    dh,
    dgu,
    hid,
    unit,
    scale,
    stat,
    ssq_in,
    stat_in,
    gain_in,
    pdn,
    rdn,
    pf,
    pown,
    xs,
    xr,
    dxs,
    sgu,
    rgu,
    fgu,
    sgd,
    rgd,
    fgd,
    ssem,
    rsem,
    go,
):
    s = lax.axis_index("section")
    f = lax.axis_index("fsdp")
    t = lax.axis_index("tp")
    y, xh = lax.div(f, NXH), lax.rem(f, NXH)
    z, xl = lax.div(t, NXL), lax.rem(t, NXL)
    oh, ol = 1 - xh, 1 - xl

    def at_y(step):
        return (s, lax.rem(y + step + NY, NY) * NXH + xh, t)

    def at_z(step):
        return (s, f, lax.rem(z + step + NZ, NZ) * NXL + xl)

    dev = {
        "y+": at_y(1),
        "y-": at_y(-1),
        "z+": at_z(1),
        "z-": at_z(-1),
        "xh": (s, y * NXH + oh, t),
        "xl": (s, f, z * NXL + ol),
        "core": (1 - s, f, t),
    }
    tp_peers = [(s, f, lax.rem(t + k, NT)) for k in range(1, NT)]
    fs_peers = [(s, lax.rem(f + k, NF), t) for k in range(1, NF)]
    zblk = [lax.rem(z + k, NZ) for k in range(NZ)]
    own, left, right, far = (
        {"c": lax.rem(y + k, NY) * NXH + xh, "o": lax.rem(y + k, NY) * NXH + oh} for k in (0, 3, 1, 2)
    )

    ids = {}
    size = [0]
    ctx = [None]
    outgoing = {None: {}, 0: {}, 1: {}}

    def ident(name, n=1):
        if name not in ids:
            ids[name] = size[0]
            size[0] += n
        return ids[name]

    def copy(src, dst, m, to):
        return pltpu.make_async_remote_copy(
            src_ref=src,
            dst_ref=dst,
            send_sem=ssem.at[m],
            recv_sem=rsem.at[m],
            device_id=to,
            device_id_type=MESH,
        )

    def static(idx):
        return tuple(i if isinstance(i, (int, pl.Slice)) else 0 for i in idx)

    def send(src, si, dst, di, name, to, q=None):
        m = ident(name, 1 if q is None else 2)
        copy(src.at[si], dst.at[di], m if q is None else m + q, to).start()
        parts = outgoing[ctx[0]].setdefault(name, [])
        parts.append((q if isinstance(q, int) else len(parts), src, static(si)))

    def arrived(dst, di, name, q=None):
        m = ident(name, 1 if q is None else 2)
        r = dst.at[di]
        copy(r, r, m if q is None else m + q, dev["core"]).wait_recv()

    def wait_sent(which):
        for name, parts in outgoing[which].items():
            for k, src, si in parts:
                r = src.at[si]
                copy(r, r, ids[name] + k, dev["core"]).wait_send()

    def rows(n, step, fn):
        def body(i, c):
            fn(pl.multiple_of(i * step, step))
            return c

        lax.fori_loop(0, n // step, body, 0)

    barrier = pltpu.get_barrier_semaphore()
    for to in tp_peers + fs_peers + [dev["core"]]:
        pl.semaphore_signal(barrier, inc=1, device_id=to, device_id_type=MESH)

    with scope("prep"):
        eye = (
            lax.broadcasted_iota(jnp.int32, (W, W), 0) == lax.broadcasted_iota(jnp.int32, (W, W), 1)
        ).astype(BF16)
        xt = dot(eye, x_ref[...], 1, 1)
        ssq_in[t] = jnp.sum(xt * xt, axis=0, keepdims=True)
        unit[...] = xt

        @pl.when(s == 1)
        def _():
            top = dot(eye, tg_ref[...], 1, 1).astype(BF16)
            for h in range(H):
                dy_all[z, xl, h] = top[:, h * TH : (h + 1) * TH]

        def pack(r):
            wgu[f, pl.ds(r, 32), 0:FL] = wg_ref[pl.ds(r, 32), :]
            wgu[f, pl.ds(r, 32), FL:GU] = wu_ref[pl.ds(r, 32), :]

        rows(PW, 32, pack)

        def pack_down(r):
            wd[f, pl.ds(r, 48), :] = wd_ref[pl.ds(r, 48), :]

        rows(FL, 48, pack_down)

    with scope("barrier"):
        pl.semaphore_wait(barrier, NT - 1 + NF - 1 + 1)

    def spread(buf, name):
        for k, to in enumerate(tp_peers):
            send(buf, (t,), buf, (t,), (name, k), to)

    def collect(buf, name):
        for k in range(1, NT):
            arrived(buf, (lax.rem(t + NT - k, NT),), (name, k - 1))
        total = buf[0]
        for k in range(1, NT):
            total = total + buf[k]
        return total

    spread(ssq_in, "ssq")

    halves = {"u": ((0, 160), (160, 160)), "d": ((0, 208), (208, 224))}
    full = {"u": wgu, "d": wd}

    def w_own(a, dirs):
        for d in dirs:
            send(full[a], (f,), full[a], (f,), ("w", a, "own", d), dev[d])

    def w_fwd(a):
        arr = full[a]
        for d, blk, k in (("y+", left["c"], 0), ("y-", right["c"], 1)):
            arrived(arr, (blk,), ("w", a, "own", d))
            part = pl.ds(*halves[a][k])
            send(arr, (blk, part), arr, (blk, part), ("w", a, "fwd", d), dev[d])

    def w_pass(a):
        arr, blk = full[a], own["o"]
        arrived(arr, (blk,), ("w", a, "own", "xh"))
        for d in ("y+", "y-"):
            send(arr, (blk,), arr, (blk,), ("w", a, "pass", d), dev[d])

    def w_far(a):
        arr, blk = full[a], far["c"]
        for d, k in (("y+", 0), ("y-", 1)):
            arrived(arr, (blk, pl.ds(*halves[a][k])), ("w", a, "fwd", d))
        send(arr, (blk,), arr, (blk,), ("w", a, "far"), dev["xh"])

    def w_last(a):
        arr = full[a]
        arrived(arr, (left["o"],), ("w", a, "pass", "y+"))
        arrived(arr, (right["o"],), ("w", a, "pass", "y-"))
        arrived(arr, (far["o"],), ("w", a, "far"))

    def ag_own(buf, nm, hh=()):
        own_at = (z, xl, *hh)
        send(buf, own_at, buf, own_at, (nm, "xl", *hh), dev["xl"])
        send(buf, own_at, buf, own_at, (nm, "z+", 1, 0, *hh), dev["z+"])
        send(buf, own_at, buf, own_at, (nm, "z-", 1, 0, *hh), dev["z-"])

    def ag_partner(buf, nm, hh=()):
        at = (z, ol, *hh)
        arrived(buf, at, (nm, "xl", *hh))
        send(buf, at, buf, at, (nm, "z+", 1, 1, *hh), dev["z+"])
        send(buf, at, buf, at, (nm, "z-", 1, 1, *hh), dev["z-"])

    def ag_fwd(buf, nm, k, j, hh=()):
        q = (xl, ol)[j]
        for d, blk in (("z+", zblk[NZ - k]), ("z-", zblk[k])):
            at = (blk, q, *hh)
            arrived(buf, at, (nm, d, k, j, *hh))
            send(buf, at, buf, at, (nm, d, k + 1, j, *hh), dev[d])

    def ag_fwd3(buf, nm, hh=()):
        for d, blk, q in (("z+", zblk[5], 0), ("z-", zblk[3], 1)):
            for j in range(2):
                arrived(buf, (blk, (xl, ol)[j], *hh), (nm, d, 3, j, *hh))
            send(buf, (blk, q, *hh), buf, (blk, q, *hh), (nm, d, 4, *hh), dev[d])

    def ag_last(buf, nm, hh=()):
        arrived(buf, (zblk[4], 0, *hh), (nm, "z+", 4, *hh))
        arrived(buf, (zblk[4], 1, *hh), (nm, "z-", 4, *hh))

    def act(buf, i):
        return jnp.concatenate([buf[i, :, h].reshape(PW, TH) for h in range(H)], axis=1)

    def pick(i, table):
        v = table[0]
        for k in range(1, len(table)):
            v = jnp.where(i == k, table[k], v)
        return v

    order = [own["c"], left["c"], right["c"], own["o"], far["c"], left["o"], right["o"], far["o"]]

    def forward(a, b):
        def body(i, c):
            blk = pick(i, order)
            part = dot(wgu[blk], n_all[blk].reshape(PW, T), 0, 0)
            gu[...] = jnp.where(i == 0, part, gu[...] + part)
            return c

        lax.fori_loop(a, b, body, 0)

    dy_order = [zblk[k] for k in (0, 1, 7, 2, 6, 3, 5, 4)]

    def dhidden(a, b):
        def body(i, c):
            blk = pick(i, dy_order)
            part = dot(wd[blk], act(dy_all, blk), 1, 0)
            dh[...] = jnp.where(i == 0, part, dh[...] + part)
            return c

        lax.fori_loop(a, b, body, 0)

    def normalize():
        row_scale = lax.rsqrt(collect(ssq_in, "ssq") / D + EPS)
        scale[...] = row_scale
        u = unit[...] * row_scale
        unit[...] = u
        n_all[z, xl] = (u * gain_ref[:, 0:1]).astype(BF16)

    @pl.when(s == 1)
    def _():
        ctx[0] = 1
        with scope("a_own"):
            ag_own(dy_all, "dy")
            w_own("d", ("y+", "y-", "xh"))
            w_own("u", ("y+", "y-"))
        with scope("a_norm"):
            normalize()
            ag_own(n_all, "n")
            w_own("u", ("xh",))
        with scope("a_dyp"):
            ag_partner(dy_all, "dy")
        with scope("a_np"):
            ag_partner(n_all, "n")
        with scope("a_wfd"):
            w_fwd("d")
        for k in (1, 2):
            with scope(f"a_n{k}"):
                ag_fwd(n_all, "n", k, 0)
                ag_fwd(n_all, "n", k, 1)
            if k == 1:
                with scope("a_wfu"):
                    w_fwd("u")
        with scope("a_wpd"):
            w_pass("d")
        with scope("a_n3"):
            ag_fwd3(n_all, "n")
        with scope("a_dy1"):
            ag_fwd(dy_all, "dy", 1, 0)
            ag_fwd(dy_all, "dy", 1, 1)
        with scope("a_wpu"):
            w_pass("u")
        with scope("a_wxd"):
            w_far("d")
        with scope("a_dy2"):
            ag_fwd(dy_all, "dy", 2, 0)
            ag_fwd(dy_all, "dy", 2, 1)
        with scope("a_nl"):
            ag_last(n_all, "n")
        with scope("a_wxu"):
            w_far("u")
        with scope("a_f5"):
            forward(0, 5)
        with scope("a_dy3"):
            ag_fwd3(dy_all, "dy")
        pl.semaphore_signal(go, inc=1, device_id=dev["core"], device_id_type=MESH)
        with scope("a_wld"):
            w_last("d")
        with scope("a_h7"):
            dhidden(0, 7)
        with scope("a_dyl"):
            ag_last(dy_all, "dy")
            dhidden(7, 8)
        with scope("a_wlu"):
            w_last("u")
        with scope("a_f8"):
            forward(5, 8)
        ctx[0] = None

    @pl.when(s == 0)
    def _():
        ctx[0] = 0
        with scope("b_norm"):
            normalize()
        with scope("b_go"):
            pl.semaphore_wait(go, 1)
        with scope("b_own"):
            ag_own(n_all, "n")
            w_own("d", ("y+", "y-", "xh"))
            w_own("u", ("y+", "y-", "xh"))
        with scope("b_np"):
            ag_partner(n_all, "n")
        with scope("b_n1"):
            ag_fwd(n_all, "n", 1, 0)
            ag_fwd(n_all, "n", 1, 1)
        with scope("b_wfd"):
            w_fwd("d")
        with scope("b_n2"):
            ag_fwd(n_all, "n", 2, 0)
            ag_fwd(n_all, "n", 2, 1)
        with scope("b_wfu"):
            w_fwd("u")
        with scope("b_n3"):
            ag_fwd3(n_all, "n")
        with scope("b_wpd"):
            w_pass("d")
            w_pass("u")
        with scope("b_nl"):
            ag_last(n_all, "n")
        with scope("b_wxd"):
            w_far("d")
        with scope("b_wxu"):
            w_far("u")
        with scope("b_f5"):
            forward(0, 5)
        with scope("b_wl"):
            w_last("d")
            w_last("u")
        with scope("b_f8"):
            forward(5, 8)
        with scope("b_core"):
            for h in range(H):
                arrived(dy_all, (z, xl, h), ("core", h))
                ag_own(dy_all, "e", (h,))
        with scope("b_dyp"):
            for h in range(H):
                ag_partner(dy_all, "e", (h,))
        for k in (1, 2):
            with scope(f"b_dy{k}"):
                for h in range(H):
                    for j in range(2):
                        ag_fwd(dy_all, "e", k, j, (h,))
        with scope("b_dy3"):
            for h in range(H):
                ag_fwd3(dy_all, "e", (h,))
        with scope("b_h7"):
            dhidden(0, 7)
        with scope("b_dyl"):
            for h in range(H):
                ag_last(dy_all, "e", (h,))
            dhidden(7, 8)
        ctx[0] = None

    with scope("elem"):
        stat[...] = jnp.zeros_like(stat)

        def elementwise(r):
            gate = gu[pl.ds(r, 16), :]
            up = gu[pl.ds(pl.multiple_of(FL + r, 16), 16), :]
            dd = dh[pl.ds(r, 16), :]
            sig = jax.nn.sigmoid(gate)
            silu = gate * sig
            hid[pl.ds(r, 16), :] = (silu * up).astype(BF16)
            d_gate = (dd * up * sig * (1.0 + gate * (1.0 - sig))).astype(BF16)
            d_up = (dd * silu).astype(BF16)
            dgu[pl.ds(r, 16), :] = d_gate
            dgu[pl.ds(pl.multiple_of(FL + r, 16), 16), :] = d_up
            both = d_gate.astype(F32) * gate + d_up.astype(F32) * up
            stat[...] += both[0:8] + both[8:16]

        rows(FL, 16, elementwise)
        stat_in[t] = jnp.sum(stat[...], axis=0, keepdims=True)
        spread(stat_in, "stat")

    def partial(blk, h):
        return dot(wgu[blk], dgu[:, h * TH : (h + 1) * TH], 1, 0).reshape(NXL, W, TH)

    ways = (("z+", 0), ("z-", 1))

    def rs_first():
        def body(h, c):
            part = dot(wgu[zblk[4]], dgu[...], 1, 0).reshape(NXL, W, T)
            for hh in range(H):
                pdn[0, hh] = part[:, :, hh * TH : (hh + 1) * TH].astype(BF16)
            return c

        lax.fori_loop(0, 1, body, 0)
        for h in range(H):
            for d, w in ways:
                send(pdn, (0, h, w), rdn, (w, 0, h, w), ("rs", d, 1, h), dev[d], q=w)

    def rs_compute(k):
        def body(w, c):
            blk = jnp.where(w == 0, zblk[5 - k], zblk[3 + k])
            part = dot(wgu[blk], dgu[...], 1, 0).reshape(NXL, W, T)
            for hh in range(H):
                pf[w, hh] = part[:, :, hh * TH : (hh + 1) * TH]
            return c

        lax.fori_loop(0, 2, body, 0)

    def rs_step(k):
        slot = 2 * k - 3
        if k == 2:
            for h in range(H):
                for d, w in ways:
                    q = 1 - w
                    pdn[slot + w, h, q] = pf[w, h, q].astype(BF16)
                    send(pdn, (slot + w, h, q), rdn, (w, k - 1, h, q), ("rs", d, k, h), dev[d], q=q)
        for h in range(H):
            for j in range(2):
                for d, w in ways:
                    if k == 2:
                        q = w
                        if j:
                            continue
                    else:
                        q = (ol, xl)[j]
                    arrived(rdn, (w, k - 2, h, q), ("rs", d, k - 1, h), q=q)
                    pdn[slot + w, h, q] = (pf[w, h, q] + rdn[w, k - 2, h, q].astype(F32)).astype(BF16)
                    send(pdn, (slot + w, h, q), rdn, (w, k - 1, h, q), ("rs", d, k, h), dev[d], q=q)

    def rs_own():
        def body(h, c):
            part = dot(wgu[z], dgu[...], 1, 0).reshape(NXL, W, T)
            for hh in range(H):
                pown[hh] = part[:, :, hh * TH : (hh + 1) * TH]
            return c

        lax.fori_loop(0, 1, body, 0)

    def rs_last():
        for h in range(H):
            for q in (ol, xl):
                for d, w in ways:
                    arrived(rdn, (w, 3, h, q), ("rs", d, 4, h), q=q)
                if q is ol:
                    xs[h] = (
                        pown[h, q] + rdn[0, 3, h, q].astype(F32) + rdn[1, 3, h, q].astype(F32)
                    ).astype(BF16)
                    send(xs, (h,), xr, (h,), ("rx", h), dev["xl"])

    def dx_part(h, norm_stat):
        arrived(xr, (h,), ("rx", h))
        cols = slice(h * TH, (h + 1) * TH)
        d_normed = (
            pown[h, xl]
            + rdn[0, 3, h, xl].astype(F32)
            + rdn[1, 3, h, xl].astype(F32)
            + xr[h].astype(F32)
        )
        u = unit[:, cols]
        dx = dy_all[z, xl, h].astype(F32) + scale[:, cols] * (
            d_normed * gain_ref[:, 0:1] - u * norm_stat[:, cols]
        )
        dxs[h] = dx.astype(BF16)
        return d_normed * u

    def gain_dx(parts):
        total = dot(
            jnp.ones((8, T), F32), jnp.concatenate(parts, axis=1), 1, 1, lax.Precision.HIGHEST
        )
        gain_in[f] = total
        for k, to in enumerate(fs_peers):
            send(gain_in, (f,), gain_in, (f,), ("gain", k), to)
        for h in range(H):
            dx_ref[h * TH : (h + 1) * TH, :] = dot(dxs[h], eye, 0, 0).astype(BF16)

    sg, rg, fg = {"u": sgu, "d": sgd}, {"u": rgu, "d": rgd}, {"u": fgu, "d": fgd}
    size_of = {"u": (PW, 32), "d": (FL, 48)}

    def wgrad(a, blk):
        if a == "u":
            return dot(n_all[blk].reshape(PW, T), dgu[...], 1, 1)
        return dot(hid[...], act(dy_all, blk), 1, 1)

    direct = [far["o"], right["o"], left["o"]]
    kept = [far["c"], right["c"], left["c"], own["o"], own["c"]]

    def g_first(a):
        def body(i, c):
            sg[a][i] = wgrad(a, pick(i, direct)).astype(BF16)
            return c

        lax.fori_loop(0, 3, body, 0)
        for i, d in enumerate(("xh", "y+", "y-")):
            send(sg[a], (i,), rg[a], (i,), ("g", a, i), dev[d])

    def g_kept(a):
        def body(i, c):
            fg[a][i] = wgrad(a, pick(i, kept))
            return c

        lax.fori_loop(0, 5, body, 0)

    def g_sum(a, slot, own_i, recv, span=None):
        n, st = size_of[a]
        lo, n = span if span else (0, n)
        st = 16 if span else st

        def body(r):
            r = pl.multiple_of(r + lo, 16)
            v = fg[a][own_i, pl.ds(r, st), :]
            for k in recv:
                v = v + rg[a][k, pl.ds(r, st), :].astype(F32)
            sg[a][slot, pl.ds(r, st), :] = v.astype(BF16)

        rows(n, st, body)

    def g_far(a):
        arrived(rg[a], (0,), ("g", a, 0))
        g_sum(a, 3, 0, (0,))
        for d, k in (("y+", 0), ("y-", 1)):
            part = pl.ds(*halves[a][k])
            send(sg[a], (3, part), rg[a], (3, part), ("g", a, 3, d), dev[d])

    def g_near(a):
        for d, k, slot in (("y+", 0, 4), ("y-", 1, 5)):
            part = pl.ds(*halves[a][k])
            arrived(rg[a], (3, part), ("g", a, 3, d))
            g_sum(a, slot, 1 + k, (3,), halves[a][k])
            g_sum(a, slot, 1 + k, (), halves[a][1 - k])
            send(sg[a], (slot,), rg[a], (slot,), ("g", a, slot), dev[d])

    def g_partner(a):
        arrived(rg[a], (1,), ("g", a, 1))
        arrived(rg[a], (2,), ("g", a, 2))
        g_sum(a, 6, 3, (1, 2))
        send(sg[a], (6,), rg[a], (6,), ("g", a, 6), dev["xh"])

    def g_last(a):
        for k in (4, 5, 6):
            arrived(rg[a], (k,), ("g", a, k))
        n, st = size_of[a]

        def body(r):
            at = pl.ds(r, st)
            v = fg[a][4, at, :]
            for k in (4, 5, 6):
                v = v + rg[a][k, at, :].astype(F32)
            if a == "u":
                gg_ref[at, :] = v[:, 0:FL]
                ug_ref[at, :] = v[:, FL:GU]
            else:
                dg_ref[at, :] = v

        rows(n, st, body)

    @pl.when(s == 1)
    def _():
        ctx[0] = 1
        with scope("c_r1"):
            rs_first()
            rs_compute(2)
        for k in (2, 3, 4):
            with scope(f"c_r{k}"):
                rs_step(k)
                if k < 4:
                    rs_compute(k + 1)
                else:
                    rs_own()
        with scope("c_rl"):
            rs_last()
        with scope("c_stat"):
            norm_stat = collect(stat_in, "stat") / D
        with scope("c_dx"):
            parts = []
            for h in range(H):
                parts.append(dx_part(h, norm_stat))
                send(dxs, (h,), dy_all, (z, xl, h), ("core", h), dev["core"])
        with scope("c_gain"):
            gain_dx(parts)
        with scope("c_g1"):
            g_first("d")
            g_first("u")
        with scope("c_gk"):
            g_kept("d")
            g_kept("u")
        with scope("c_gfd"):
            g_far("d")
        with scope("c_gpd"):
            g_partner("d")
        with scope("c_gfu"):
            g_far("u")
        with scope("c_gnd"):
            g_near("d")
        with scope("c_gpu"):
            g_partner("u")
        with scope("c_gnu"):
            g_near("u")
        with scope("c_gld"):
            g_last("d")
        with scope("c_glu"):
            g_last("u")
        wait_sent(1)
        ctx[0] = None

    @pl.when(s == 0)
    def _():
        ctx[0] = 0
        with scope("d_r1"):
            rs_first()
        with scope("d_g1"):
            g_first("d")
            g_first("u")
        with scope("d_r2"):
            rs_compute(2)
            rs_step(2)
        with scope("d_gkd"):
            g_kept("d")
        with scope("d_r3"):
            rs_compute(3)
            rs_step(3)
        with scope("d_gku"):
            g_kept("u")
        with scope("d_gfd"):
            g_far("d")
        with scope("d_r4"):
            rs_compute(4)
            rs_step(4)
        with scope("d_gfu"):
            g_far("u")
        with scope("d_gpd"):
            g_partner("d")
        with scope("d_gnd"):
            g_near("d")
        with scope("d_gpu"):
            g_partner("u")
        with scope("d_gnu"):
            g_near("u")
        with scope("d_rl"):
            rs_own()
            rs_last()
            norm_stat = collect(stat_in, "stat") / D
        with scope("d_dx"):
            parts = [dx_part(h, norm_stat) for h in range(H)]
            gain_dx(parts)
        with scope("d_gld"):
            g_last("d")
        with scope("d_glu"):
            g_last("u")
        wait_sent(0)
        ctx[0] = None

    for k in range(1, NF):
        arrived(gain_in, (lax.rem(f + NF - k, NF),), ("gain", k - 1))
    gsum = gain_in[0]
    for k in range(1, NF):
        gsum = gsum + gain_in[k]
    gn_ref[...] = gsum
    wait_sent(None)
    assert size[0] <= NSEM, size[0]


def body(saved_inputs, top_grad, norm_gain, gate_weight, up_weight, down_weight):
    x = saved_inputs.reshape(T, W)
    tg = top_grad.reshape(T, W)
    gain = lax.dynamic_slice_in_dim(norm_gain[0], lax.axis_index("tp") * W, W)
    gain = jnp.broadcast_to(gain[:, None], (W, 128))
    vm = pl.BlockSpec(memory_space=pltpu.VMEM)
    out = pl.pallas_call(
        fused_kernel,
        name="fused",
        out_shape=(
            jax.ShapeDtypeStruct((T, W), BF16),
            jax.ShapeDtypeStruct((PW, FL), F32),
            jax.ShapeDtypeStruct((PW, FL), F32),
            jax.ShapeDtypeStruct((FL, PW), F32),
            jax.ShapeDtypeStruct((8, W), F32),
        ),
        in_specs=[vm] * 6,
        out_specs=[vm] * 5,
        scratch_shapes=[
            pltpu.VMEM((NF, PW, GU), BF16),
            pltpu.VMEM((NF, FL, PW), BF16),
            pltpu.VMEM((NZ, NXL, W, T), BF16),
            pltpu.VMEM((NZ, NXL, H, W, TH), BF16),
            pltpu.VMEM((GU, T), F32),
            pltpu.VMEM((FL, T), F32),
            pltpu.VMEM((GU, T), BF16),
            pltpu.VMEM((FL, T), BF16),
            pltpu.VMEM((W, T), F32),
            pltpu.VMEM((1, T), F32),
            pltpu.VMEM((8, T), F32),
            pltpu.VMEM((NT, 1, T), F32),
            pltpu.VMEM((NT, 1, T), F32),
            pltpu.VMEM((NF, 8, W), F32),
            pltpu.VMEM((7, H, NXL, W, TH), BF16),
            pltpu.VMEM((2, 4, H, NXL, W, TH), BF16),
            pltpu.VMEM((2, H, NXL, W, TH), F32),
            pltpu.VMEM((H, NXL, W, TH), F32),
            pltpu.VMEM((H, W, TH), BF16),
            pltpu.VMEM((H, W, TH), BF16),
            pltpu.VMEM((H, W, TH), BF16),
            pltpu.VMEM((7, PW, GU), BF16),
            pltpu.VMEM((7, PW, GU), BF16),
            pltpu.VMEM((5, PW, GU), F32),
            pltpu.VMEM((7, FL, PW), BF16),
            pltpu.VMEM((7, FL, PW), BF16),
            pltpu.VMEM((5, FL, PW), F32),
            pltpu.SemaphoreType.DMA((NSEM,)),
            pltpu.SemaphoreType.DMA((NSEM,)),
            pltpu.SemaphoreType.REGULAR,
        ],
        compiler_params=pltpu.CompilerParams(
            collective_id=0, has_side_effects=True, vmem_limit_bytes=62 * 2**20
        ),
    )(x, tg, gain, gate_weight[0], up_weight[0], down_weight[0])
    dx, gg, ug, dg, gn = out
    return (
        dx.reshape(1, MICRO, ROWS, W),
        gg[None],
        ug[None],
        dg[None],
        gn[0:1],
    )


def solution(mesh):
    return jax.shard_map(
        body,
        mesh=mesh,
        in_specs=(
            P("section", None, "fsdp", "tp"),
            P(None, "fsdp", "tp"),
            P("section", None),
            P("section", "fsdp", "tp"),
            P("section", "fsdp", "tp"),
            P("section", "tp", "fsdp"),
        ),
        out_specs=(
            P("section", None, "fsdp", "tp"),
            P("section", "fsdp", "tp"),
            P("section", "fsdp", "tp"),
            P("section", "tp", "fsdp"),
            P("section", "tp"),
        ),
        check_vma=False,
    )
```

```python
import jax
import jax.numpy as jnp
from jax import lax
from jax.experimental import pallas as pl
from jax.experimental.pallas import tpu as pltpu
from jax.sharding import PartitionSpec as P

EPS = 1e-05
MESH = pl.DeviceIdType.MESH
F32 = jnp.float32
BF16 = jnp.bfloat16

NY, NXH, NZ, NXL = 4, 2, 8, 2
NF, NT = NY * NXH, NZ * NXL
MICRO = 8
ROWS = 64
T = MICRO * ROWS
H = 2
TH = T // H
W = 160
PW = NXL * W
FL = 432
GU = 2 * FL
D = W * NT
UW = 896
DH = 384
DR = PW + 16
NSEM = 180


def scope(name):
    return jax.named_scope(name)


def dot(a, b, ca, cb, precision=None):
    return lax.dot_general(
        a, b, (((ca,), (cb,)), ((), ())), preferred_element_type=F32, precision=precision
    )


def fused_kernel(
    x_hbm,
    tg_hbm,
    gain_hbm,
    wg_hbm,
    wu_hbm,
    wd_hbm,
    dx_hbm,
    gg_hbm,
    ug_hbm,
    dg_hbm,
    gn_hbm,
    x_ref,
    tg_ref,
    gain_row,
    wg_ref,
    wu_ref,
    wd_ref,
    dx_ref,
    gg_ref,
    ug_ref,
    dg_ref,
    gn_ref,
    gain,
    wgu,
    wd,
    n_all,
    dy_all,
    gu,
    dh,
    dgu,
    hid,
    hid_mid,
    unit,
    scale,
    stat,
    ssq_in,
    stat_in,
    gain_in,
    pdn,
    rdn,
    pf,
    pown,
    xs,
    xr,
    dxs,
    sgu,
    rgu,
    fgu,
    sgd,
    rgd,
    fgd,
    ssem,
    rsem,
    lsem,
    go,
):
    s = lax.axis_index("section")
    f = lax.axis_index("fsdp")
    t = lax.axis_index("tp")
    y, xh = lax.div(f, NXH), lax.rem(f, NXH)
    z, xl = lax.div(t, NXL), lax.rem(t, NXL)
    oh, ol = 1 - xh, 1 - xl

    def at_y(step):
        return (s, lax.rem(y + step + NY, NY) * NXH + xh, t)

    def at_z(step):
        return (s, f, lax.rem(z + step + NZ, NZ) * NXL + xl)

    dev = {
        "y+": at_y(1),
        "y-": at_y(-1),
        "z+": at_z(1),
        "z-": at_z(-1),
        "xh": (s, y * NXH + oh, t),
        "xl": (s, f, z * NXL + ol),
        "core": (1 - s, f, t),
    }
    tp_peers = [(s, f, lax.rem(t + k, NT)) for k in range(1, NT)]
    fs_peers = [(s, lax.rem(f + k, NF), t) for k in range(1, NF)]
    zblk = [lax.rem(z + k, NZ) for k in range(NZ)]
    own, left, right, far = (
        {"c": lax.rem(y + k, NY) * NXH + xh, "o": lax.rem(y + k, NY) * NXH + oh} for k in (0, 3, 1, 2)
    )

    ids = {}
    size = [0]
    ctx = [None]
    outgoing = {None: {}, 0: {}, 1: {}}

    def ident(name, n=1):
        if name not in ids:
            ids[name] = size[0]
            size[0] += n
        return ids[name]

    def copy(src, dst, m, to):
        return pltpu.make_async_remote_copy(
            src_ref=src,
            dst_ref=dst,
            send_sem=ssem.at[m],
            recv_sem=rsem.at[m],
            device_id=to,
            device_id_type=MESH,
        )

    def static(idx):
        return tuple(i if isinstance(i, (int, pl.Slice)) else 0 for i in idx)

    def send(src, si, dst, di, name, to, q=None):
        m = ident(name, 1 if q is None else 2)
        copy(src.at[si], dst.at[di], m if q is None else m + q, to).start()
        parts = outgoing[ctx[0]].setdefault(name, [])
        parts.append((q if isinstance(q, int) else len(parts), src, static(si)))

    def arrived(dst, di, name, q=None):
        m = ident(name, 1 if q is None else 2)
        r = dst.at[di]
        copy(r, r, m if q is None else m + q, dev["core"]).wait_recv()

    def wait_sent(which):
        for name, parts in outgoing[which].items():
            for k, src, si in parts:
                r = src.at[si]
                copy(r, r, ids[name] + k, dev["core"]).wait_send()

    def rows(n, step, fn):
        def body(i, c):
            fn(pl.multiple_of(i * step, step))
            return c

        lax.fori_loop(0, n // step, body, 0)

    barrier = pltpu.get_barrier_semaphore()
    for to in tp_peers + fs_peers + [dev["core"]]:
        pl.semaphore_signal(barrier, inc=1, device_id=to, device_id_type=MESH)

    loads = [
        pltpu.make_async_copy(src, dst, lsem.at[k])
        for k, (src, dst) in enumerate(
            (
                (x_hbm, x_ref),
                (tg_hbm, tg_ref),
                (gain_hbm, gain_row),
                (wd_hbm, wd_ref),
                (wg_hbm, wg_ref),
                (wu_hbm, wu_ref),
            )
        )
    ]
    for c in loads:
        c.start()
    with scope("prep"):
        eye = (
            lax.broadcasted_iota(jnp.int32, (W, W), 0) == lax.broadcasted_iota(jnp.int32, (W, W), 1)
        ).astype(BF16)
        loads[0].wait()
        xt = dot(eye, x_ref[...], 1, 1)
        ssq_in[t] = jnp.sum(xt * xt, axis=0, keepdims=True)
        unit[...] = xt
        loads[1].wait()

        @pl.when(s == 1)
        def _():
            top = dot(eye, tg_ref[...], 1, 1).astype(BF16)
            for h in range(H):
                dy_all[z, xl, h] = top[:, h * TH : (h + 1) * TH]

        loads[3].wait()

        def pack_down(r):
            wd[f, pl.ds(r, 32), :] = wd_ref[pl.ds(r, 32), 0:DH]
            wgu[f, pl.ds(r, 32), GU:UW] = wd_ref[pl.ds(r, 32), DH : DH + 32]

        rows(PW, 32, pack_down)
        last = (
            lax.broadcasted_iota(jnp.int32, (16, FL), 0) + (FL - 16)
            == lax.broadcasted_iota(jnp.int32, (16, FL), 1)
        ).astype(BF16)
        wd[f, PW:DR, 0:PW] = dot(last, wd_ref[...], 1, 1).astype(BF16)
        loads[4].wait()
        loads[5].wait()

        def pack(r):
            wgu[f, pl.ds(r, 32), 0:FL] = wg_ref[pl.ds(r, 32), :]
            wgu[f, pl.ds(r, 32), FL:GU] = wu_ref[pl.ds(r, 32), :]

        rows(PW, 32, pack)
        loads[2].wait()

        def gains(r):
            mine = lax.broadcasted_iota(jnp.int32, (32, D), 1) == (
                lax.broadcasted_iota(jnp.int32, (32, D), 0) + (t * W + r)
            )
            row = jnp.broadcast_to(gain_row[...], (32, D))
            gain[pl.ds(r, 32), :] = jnp.broadcast_to(
                jnp.sum(jnp.where(mine, row, 0.0), axis=1, keepdims=True), (32, 128)
            )

        rows(W, 32, gains)

    with scope("barrier"):
        pl.semaphore_wait(barrier, NT - 1 + NF - 1 + 1)

    def spread(buf, name):
        for k, to in enumerate(tp_peers):
            send(buf, (t,), buf, (t,), (name, k), to)

    def collect(buf, name):
        for k in range(1, NT):
            arrived(buf, (lax.rem(t + NT - k, NT),), (name, k - 1))
        total = buf[0]
        for k in range(1, NT):
            total = total + buf[k]
        return total

    spread(ssq_in, "ssq")

    halves = {"u": ((0, 160), (160, 160)), "d": ((0, 160), (160, 176))}
    full = {"u": wgu, "d": wd}

    def w_own(a, dirs):
        for d in dirs:
            send(full[a], (f,), full[a], (f,), ("w", a, "own", d), dev[d])

    def w_fwd(a):
        arr = full[a]
        for d, blk, k in (("y+", left["c"], 0), ("y-", right["c"], 1)):
            arrived(arr, (blk,), ("w", a, "own", d))
            part = pl.ds(*halves[a][k])
            send(arr, (blk, part), arr, (blk, part), ("w", a, "fwd", d), dev[d])

    def w_pass(a):
        arr, blk = full[a], own["o"]
        arrived(arr, (blk,), ("w", a, "own", "xh"))
        for d in ("y+", "y-"):
            send(arr, (blk,), arr, (blk,), ("w", a, "pass", d), dev[d])

    def w_far(a):
        arr, blk = full[a], far["c"]
        for d, k in (("y+", 0), ("y-", 1)):
            arrived(arr, (blk, pl.ds(*halves[a][k])), ("w", a, "fwd", d))
        send(arr, (blk,), arr, (blk,), ("w", a, "far"), dev["xh"])

    def w_last(a):
        arr = full[a]
        arrived(arr, (left["o"],), ("w", a, "pass", "y+"))
        arrived(arr, (right["o"],), ("w", a, "pass", "y-"))
        arrived(arr, (far["o"],), ("w", a, "far"))

    def ag_own(buf, nm, hh=()):
        own_at = (z, xl, *hh)
        send(buf, own_at, buf, own_at, (nm, "xl", *hh), dev["xl"])
        send(buf, own_at, buf, own_at, (nm, "z+", 1, 0, *hh), dev["z+"])
        send(buf, own_at, buf, own_at, (nm, "z-", 1, 0, *hh), dev["z-"])

    def ag_partner(buf, nm, hh=()):
        at = (z, ol, *hh)
        arrived(buf, at, (nm, "xl", *hh))
        send(buf, at, buf, at, (nm, "z+", 1, 1, *hh), dev["z+"])
        send(buf, at, buf, at, (nm, "z-", 1, 1, *hh), dev["z-"])

    def ag_fwd(buf, nm, k, j, hh=()):
        q = (xl, ol)[j]
        for d, blk in (("z+", zblk[NZ - k]), ("z-", zblk[k])):
            at = (blk, q, *hh)
            arrived(buf, at, (nm, d, k, j, *hh))
            send(buf, at, buf, at, (nm, d, k + 1, j, *hh), dev[d])

    def ag_fwd3(buf, nm, hh=()):
        for d, blk, q in (("z+", zblk[5], 0), ("z-", zblk[3], 1)):
            for j in range(2):
                arrived(buf, (blk, (xl, ol)[j], *hh), (nm, d, 3, j, *hh))
            send(buf, (blk, q, *hh), buf, (blk, q, *hh), (nm, d, 4, *hh), dev[d])

    def ag_last(buf, nm, hh=()):
        arrived(buf, (zblk[4], 0, *hh), (nm, "z+", 4, *hh))
        arrived(buf, (zblk[4], 1, *hh), (nm, "z-", 4, *hh))

    def agz_pair(buf, nm, k, blk):
        send(buf, (blk, xl), buf, (blk, xl), (nm, "pair", k), dev["xl"])

    def agz_own(buf, nm):
        for d in ("z+", "z-"):
            send(buf, (z, xl), buf, (z, xl), (nm, d, 1), dev[d])
        agz_pair(buf, nm, 0, z)

    def agz_fwd(buf, nm, k):
        for d, blk in (("z+", zblk[NZ - k]), ("z-", zblk[k])):
            arrived(buf, (blk, xl), (nm, d, k))
            part = () if k < 3 else (pl.ds(0, 80),) if d == "z+" else (pl.ds(80, 80),)
            send(buf, (blk, xl, *part), buf, (blk, xl, *part), (nm, d, k + 1), dev[d])
        agz_pair(buf, nm, NZ - k, zblk[NZ - k])
        agz_pair(buf, nm, k, zblk[k])

    def agz_far(buf, nm):
        for d, lo in (("z+", 0), ("z-", 80)):
            arrived(buf, (zblk[4], xl, pl.ds(lo, 80)), (nm, d, 4))
        agz_pair(buf, nm, 4, zblk[4])

    def agz_last(buf, nm):
        for k in range(NZ):
            arrived(buf, (zblk[k], ol), (nm, "pair", k))

    def act(buf, i):
        return jnp.concatenate([buf[i, :, h].reshape(PW, TH) for h in range(H)], axis=1)

    def pick(i, table):
        v = table[0]
        for k in range(1, len(table)):
            v = jnp.where(i == k, table[k], v)
        return v

    groups = ((0, 1, 7), (2, 6), (3, 5, 4))

    def together(parts):
        return jnp.concatenate(parts, axis=0)

    def forward(g):
        blks = [zblk[k] for k in groups[g]]
        part = dot(
            together([wgu[b] for b in blks]),
            together([n_all[b].reshape(PW, T) for b in blks]),
            0,
            0,
        )
        gu[...] = part if g == 0 else gu[...] + part

    def dhidden(g):
        blks = [zblk[k] for k in groups[g]]
        dys = [act(dy_all, b) for b in blks]
        dy = together(dys)
        parts = (
            (0, dot(together([wd[b, 0:PW] for b in blks]), dy, 0, 0)),
            (DH, dot(together([wgu[b, :, UW - 128 : UW] for b in blks]), dy, 0, 0)),
        )
        for r, part in parts:
            at = pl.ds(r, part.shape[0])
            dh[at, :] = part if g == 0 else dh[at, :] + part
        part = dot(wd[blks[0], PW:DR, 0:PW], dys[0], 1, 0)
        for b, d in zip(blks[1:], dys[1:]):
            part = part + dot(wd[b, PW:DR, 0:PW], d, 1, 0)
        at = pl.ds(DH + 128, 16)
        dh[at, :] = part if g == 0 else dh[at, :] + part

    def hidden():
        def body(r):
            gate = gu[pl.ds(r, 16), :]
            up = gu[pl.ds(pl.multiple_of(FL + r, 16), 16), :]
            hid[pl.ds(r, 16), :] = (gate * jax.nn.sigmoid(gate) * up).astype(BF16)

        rows(FL, 16, body)
        hid_mid[0:96, :] = jnp.zeros((96, T), BF16)
        hid_mid[96:128, :] = hid[DH : DH + 32, :]
        dgu[GU:UW, :] = jnp.zeros((UW - GU, T), BF16)

    def normalize():
        row_scale = lax.rsqrt(collect(ssq_in, "ssq") / D + EPS)
        scale[...] = row_scale
        u = unit[...] * row_scale
        unit[...] = u
        n_all[z, xl] = (u * gain[:, 0:1]).astype(BF16)

    @pl.when(s == 1)
    def _():
        ctx[0] = 1
        with scope("a_own"):
            ag_own(dy_all, "dy")
            w_own("d", ("y+", "y-", "xh"))
            w_own("u", ("y+", "y-"))
        with scope("a_norm"):
            normalize()
        with scope("a_nO"):
            ag_own(n_all, "n")
            w_own("u", ("xh",))
        with scope("a_dyP"):
            ag_partner(dy_all, "dy")
        with scope("a_dy10"):
            ag_fwd(dy_all, "dy", 1, 0)
        with scope("a_wfd"):
            w_fwd("d")
        with scope("a_nP"):
            ag_partner(n_all, "n")
        with scope("a_n10"):
            ag_fwd(n_all, "n", 1, 0)
        with scope("a_dy11"):
            ag_fwd(dy_all, "dy", 1, 1)
        with scope("a_wfu"):
            w_fwd("u")
            w_pass("d")
        with scope("a_n11"):
            ag_fwd(n_all, "n", 1, 1)
        with scope("a_wxd"):
            w_far("d")
        with scope("a_dy20"):
            ag_fwd(dy_all, "dy", 2, 0)
        with scope("a_wpu"):
            w_pass("u")
        with scope("a_n20"):
            ag_fwd(n_all, "n", 2, 0)
        with scope("a_wxu"):
            w_far("u")
        with scope("a_n21"):
            ag_fwd(n_all, "n", 2, 1)
        with scope("a_dy21"):
            ag_fwd(dy_all, "dy", 2, 1)
        with scope("a_n3"):
            ag_fwd3(n_all, "n")
            pl.semaphore_signal(go, inc=1, device_id=dev["core"], device_id_type=MESH)
        with scope("a_wl"):
            w_last("d")
            w_last("u")
        with scope("a_h0"):
            dhidden(0)
        with scope("a_dy3"):
            ag_fwd3(dy_all, "dy")
        with scope("a_f0"):
            forward(0)
        with scope("a_f1"):
            forward(1)
        with scope("a_h1"):
            dhidden(1)
        with scope("a_nl"):
            ag_last(n_all, "n")
        with scope("a_f2"):
            forward(2)
            hidden()
        with scope("a_dyl"):
            ag_last(dy_all, "dy")
        with scope("a_h2"):
            dhidden(2)
        ctx[0] = None

    @pl.when(s == 0)
    def _():
        ctx[0] = 0
        with scope("b_norm"):
            normalize()
        with scope("b_go"):
            pl.semaphore_wait(go, 1)
        with scope("b_own"):
            agz_own(n_all, "n")
            w_own("d", ("y+", "y-", "xh"))
            w_own("u", ("y+", "y-", "xh"))
        with scope("b_n1"):
            agz_fwd(n_all, "n", 1)
        with scope("b_wfd"):
            w_fwd("d")
        with scope("b_n2"):
            agz_fwd(n_all, "n", 2)
        with scope("b_wfu"):
            w_fwd("u")
            w_pass("d")
        with scope("b_wxd"):
            w_far("d")
        with scope("b_wpu"):
            w_pass("u")
        with scope("b_n3"):
            agz_fwd(n_all, "n", 3)
        with scope("b_wxu"):
            w_far("u")
        with scope("b_n4"):
            agz_far(n_all, "n")
        with scope("b_nl"):
            agz_last(n_all, "n")
        with scope("b_wl"):
            w_last("d")
            w_last("u")
        with scope("b_f0"):
            forward(0)
        with scope("b_f1"):
            forward(1)
        with scope("b_f2"):
            forward(2)
        with scope("b_hid"):
            hidden()
        with scope("b_core"):
            for h in range(H):
                arrived(dy_all, (z, xl, h), ("core", h))
                ag_own(dy_all, "e", (h,))
        with scope("b_dyp"):
            for h in range(H):
                ag_partner(dy_all, "e", (h,))
        with scope("b_dy1"):
            for h in range(H):
                for j in range(2):
                    ag_fwd(dy_all, "e", 1, j, (h,))
        with scope("b_dy2"):
            for h in range(H):
                for j in range(2):
                    ag_fwd(dy_all, "e", 2, j, (h,))
        with scope("b_h0"):
            dhidden(0)
        with scope("b_dy3"):
            for h in range(H):
                ag_fwd3(dy_all, "e", (h,))
        with scope("b_h1"):
            dhidden(1)
        with scope("b_dyl"):
            for h in range(H):
                ag_last(dy_all, "e", (h,))
        with scope("b_h2"):
            dhidden(2)
        ctx[0] = None

    with scope("elem"):
        stat[...] = jnp.zeros_like(stat)

        def elementwise(r):
            gate = gu[pl.ds(r, 16), :]
            up = gu[pl.ds(pl.multiple_of(FL + r, 16), 16), :]
            dd = dh[pl.ds(pl.multiple_of(jnp.where(r < DH, r, r + 96), 16), 16), :]
            sig = jax.nn.sigmoid(gate)
            silu = gate * sig
            d_gate = (dd * up * sig * (1.0 + gate * (1.0 - sig))).astype(BF16)
            d_up = (dd * silu).astype(BF16)
            dgu[pl.ds(r, 16), :] = d_gate
            dgu[pl.ds(pl.multiple_of(FL + r, 16), 16), :] = d_up
            both = d_gate.astype(F32) * gate + d_up.astype(F32) * up
            stat[...] += both[0:8] + both[8:16]

        rows(FL, 16, elementwise)
        stat_in[t] = jnp.sum(stat[...], axis=0, keepdims=True)
        spread(stat_in, "stat")

    ways = (("z+", 0), ("z-", 1))

    def rs_first():
        def body(h, c):
            part = dot(wgu[zblk[4], :, 0:GU], dgu[0:GU, :], 1, 0).reshape(NXL, W, T)
            for hh in range(H):
                pdn[0, hh] = part[:, :, hh * TH : (hh + 1) * TH].astype(BF16)
            return c

        lax.fori_loop(0, 1, body, 0)
        for h in range(H):
            for d, w in ways:
                send(pdn, (0, h, w), rdn, (w, 0, h, w), ("rs", d, 1, h), dev[d], q=w)

    def rs_compute(k):
        def body(w, c):
            blk = jnp.where(w == 0, zblk[5 - k], zblk[3 + k])
            part = dot(wgu[blk, :, 0:GU], dgu[0:GU, :], 1, 0).reshape(NXL, W, T)
            for hh in range(H):
                pf[w, hh] = part[:, :, hh * TH : (hh + 1) * TH]
            return c

        lax.fori_loop(0, 2, body, 0)

    def rs_step(k):
        slot = 2 * k - 3
        if k == 2:
            for h in range(H):
                for d, w in ways:
                    q = 1 - w
                    pdn[slot + w, h, q] = pf[w, h, q].astype(BF16)
                    send(pdn, (slot + w, h, q), rdn, (w, k - 1, h, q), ("rs", d, k, h), dev[d], q=q)
        for h in range(H):
            for j in range(2):
                for d, w in ways:
                    if k == 2:
                        q = w
                        if j:
                            continue
                    else:
                        q = (ol, xl)[j]
                    arrived(rdn, (w, k - 2, h, q), ("rs", d, k - 1, h), q=q)
                    pdn[slot + w, h, q] = (pf[w, h, q] + rdn[w, k - 2, h, q].astype(F32)).astype(BF16)
                    send(pdn, (slot + w, h, q), rdn, (w, k - 1, h, q), ("rs", d, k, h), dev[d], q=q)

    def rs_own():
        def body(h, c):
            part = dot(wgu[z, :, 0:GU], dgu[0:GU, :], 1, 0).reshape(NXL, W, T)
            for hh in range(H):
                pown[hh] = part[:, :, hh * TH : (hh + 1) * TH]
            return c

        lax.fori_loop(0, 1, body, 0)

    def rs_last():
        for h in range(H):
            for q in (ol, xl):
                for d, w in ways:
                    arrived(rdn, (w, 3, h, q), ("rs", d, 4, h), q=q)
                if q is ol:
                    xs[h] = (
                        pown[h, q] + rdn[0, 3, h, q].astype(F32) + rdn[1, 3, h, q].astype(F32)
                    ).astype(BF16)
                    send(xs, (h,), xr, (h,), ("rx", h), dev["xl"])

    def dx_part(h, norm_stat):
        arrived(xr, (h,), ("rx", h))
        cols = slice(h * TH, (h + 1) * TH)
        d_normed = (
            pown[h, xl]
            + rdn[0, 3, h, xl].astype(F32)
            + rdn[1, 3, h, xl].astype(F32)
            + xr[h].astype(F32)
        )
        u = unit[:, cols]
        dx = dy_all[z, xl, h].astype(F32) + scale[:, cols] * (
            d_normed * gain[:, 0:1] - u * norm_stat[:, cols]
        )
        dxs[h] = dx.astype(BF16)
        return d_normed * u

    stores = []

    def store(src, dst):
        c = pltpu.make_async_copy(src, dst, lsem.at[6 + len(stores)])
        c.start()
        stores.append(c)

    def gain_dx(parts):
        total = dot(
            jnp.ones((8, T), F32), jnp.concatenate(parts, axis=1), 1, 1, lax.Precision.HIGHEST
        )
        gain_in[f] = total
        for k, to in enumerate(fs_peers):
            send(gain_in, (f,), gain_in, (f,), ("gain", k), to)
        for h in range(H):
            dx_ref[h * TH : (h + 1) * TH, :] = dot(dxs[h], eye, 0, 0).astype(BF16)
        store(dx_ref, dx_hbm)

    sg, rg, fg = {"u": sgu, "d": sgd}, {"u": rgu, "d": rgd}, {"u": fgu, "d": fgd}
    size_of = {"u": (PW, 32), "d": (DR, 48)}

    def wgrad(a, blk, dst, i):
        dy = act(dy_all, blk)
        if a == "u":
            cut = UW - 128
            n = n_all[blk].reshape(PW, T)
            dst[i, :, 0:cut] = dot(n, dgu[0:cut, :], 1, 1).astype(dst.dtype)
            edge = dot(n, dgu[cut:UW, :], 1, 1) + dot(dy, hid_mid[...], 1, 1)
            dst[i, :, cut:UW] = edge.astype(dst.dtype)
        else:
            dst[i, 0:PW, :] = dot(dy, hid[0:DH, :], 1, 1).astype(dst.dtype)
            dst[i, PW:DR, 0:PW] = dot(hid[FL - 16 : FL, :], dy, 1, 1).astype(dst.dtype)

    direct = [far["o"], right["o"], left["o"]]
    kept = [far["c"], right["c"], left["c"], own["o"], own["c"]]

    def g_first(a):
        def body(i, c):
            wgrad(a, pick(i, direct), sg[a], i)
            return c

        lax.fori_loop(0, 3, body, 0)
        for i, d in enumerate(("xh", "y+", "y-")):
            send(sg[a], (i,), rg[a], (i,), ("g", a, i), dev[d])

    def g_kept(a):
        def body(i, c):
            wgrad(a, pick(i, kept), fg[a], i)
            return c

        lax.fori_loop(0, 5, body, 0)

    def g_sum(a, slot, own_i, recv, span=None):
        n, st = size_of[a]
        lo, n = span if span else (0, n)
        st = 16 if span else st

        def body(r):
            r = pl.multiple_of(r + lo, 16)
            v = fg[a][own_i, pl.ds(r, st), :]
            for k in recv:
                v = v + rg[a][k, pl.ds(r, st), :].astype(F32)
            sg[a][slot, pl.ds(r, st), :] = v.astype(BF16)

        rows(n, st, body)

    def g_far(a):
        arrived(rg[a], (0,), ("g", a, 0))
        g_sum(a, 3, 0, (0,))
        for d, k in (("y+", 0), ("y-", 1)):
            part = pl.ds(*halves[a][k])
            send(sg[a], (3, part), rg[a], (3, part), ("g", a, 3, d), dev[d])

    def g_near(a):
        for d, k, slot in (("y+", 0, 4), ("y-", 1, 5)):
            part = pl.ds(*halves[a][k])
            arrived(rg[a], (3, part), ("g", a, 3, d))
            g_sum(a, slot, 1 + k, (3,), halves[a][k])
            g_sum(a, slot, 1 + k, (), halves[a][1 - k])
            send(sg[a], (slot,), rg[a], (slot,), ("g", a, slot), dev[d])

    def g_partner(a):
        arrived(rg[a], (1,), ("g", a, 1))
        arrived(rg[a], (2,), ("g", a, 2))
        g_sum(a, 6, 3, (1, 2))
        send(sg[a], (6,), rg[a], (6,), ("g", a, 6), dev["xh"])

    def g_last(a):
        for k in (4, 5, 6):
            arrived(rg[a], (k,), ("g", a, k))

        def total(at):
            v = fg[a][4, at, :]
            for k in (4, 5, 6):
                v = v + rg[a][k, at, :].astype(F32)
            return v

        def body(r):
            at = pl.ds(r, 32)
            v = total(at)
            if a == "u":
                gg_ref[at, :] = v[:, 0:FL]
                ug_ref[at, :] = v[:, FL:GU]
                dg_ref[at, DH : DH + 32] = v[:, GU:UW]
            else:
                dg_ref[at, 0:DH] = v

        if a == "d":
            rows(PW, 32, body)
            v = total(pl.ds(PW, 16))[:, 0:PW]
            unit16 = (
                lax.broadcasted_iota(jnp.int32, (16, 16), 0)
                == lax.broadcasted_iota(jnp.int32, (16, 16), 1)
            ).astype(F32)
            dg_ref[:, DH + 32 : FL] = dot(v, unit16, 0, 0, lax.Precision.HIGHEST)
            return
        for c in range(2):
            def part(r, c=c):
                body(pl.multiple_of(r + c * 160, 16))

            rows(160, 32, part)
            at = pl.ds(c * 160, 160)
            for v_ref, hbm in ((gg_ref, gg_hbm), (ug_ref, ug_hbm), (dg_ref, dg_hbm)):
                store(v_ref.at[at], hbm.at[at])

    def finish():
        for k in range(1, NF):
            arrived(gain_in, (lax.rem(f + NF - k, NF),), ("gain", k - 1))
        gsum = gain_in[0]
        for k in range(1, NF):
            gsum = gsum + gain_in[k]
        gn_ref[...] = gsum[0:1]
        store(gn_ref, gn_hbm)
        for c in stores:
            c.wait()
        del stores[:]

    @pl.when(s == 1)
    def _():
        ctx[0] = 1
        with scope("c_r1"):
            rs_first()
            rs_compute(2)
        with scope("c_r2"):
            rs_step(2)
            rs_compute(3)
        with scope("c_r3"):
            rs_step(3)
            rs_compute(4)
        with scope("c_r4"):
            rs_step(4)
            rs_own()
        with scope("c_rl"):
            rs_last()
        with scope("c_stat"):
            norm_stat = collect(stat_in, "stat") / D
        with scope("c_dx"):
            parts = []
            for h in range(H):
                parts.append(dx_part(h, norm_stat))
                send(dxs, (h,), dy_all, (z, xl, h), ("core", h), dev["core"])
        with scope("c_g1"):
            g_first("d")
            g_first("u")
        with scope("c_gain"):
            gain_dx(parts)
        with scope("c_gk"):
            g_kept("d")
            g_kept("u")
        with scope("c_gfd"):
            g_far("d")
        with scope("c_gpd"):
            g_partner("d")
        with scope("c_gfu"):
            g_far("u")
        with scope("c_gnd"):
            g_near("d")
        with scope("c_gpu"):
            g_partner("u")
        with scope("c_gnu"):
            g_near("u")
        with scope("c_gld"):
            g_last("d")
        with scope("c_glu"):
            g_last("u")
        with scope("c_end"):
            finish()
            wait_sent(1)
        ctx[0] = None

    @pl.when(s == 0)
    def _():
        ctx[0] = 0
        with scope("d_r1"):
            rs_first()
        with scope("d_g1"):
            g_first("d")
            g_first("u")
        with scope("d_r2"):
            rs_compute(2)
            rs_step(2)
        with scope("d_gkd"):
            g_kept("d")
        with scope("d_r3"):
            rs_compute(3)
            rs_step(3)
        with scope("d_gku"):
            g_kept("u")
        with scope("d_gfd"):
            g_far("d")
        with scope("d_r4"):
            rs_compute(4)
            rs_step(4)
        with scope("d_gfu"):
            g_far("u")
        with scope("d_gpd"):
            g_partner("d")
        with scope("d_gnd"):
            g_near("d")
        with scope("d_rl"):
            rs_own()
            rs_last()
            norm_stat = collect(stat_in, "stat") / D
        with scope("d_gpu"):
            g_partner("u")
        with scope("d_gnu"):
            g_near("u")
        with scope("d_dx"):
            parts = [dx_part(h, norm_stat) for h in range(H)]
            gain_dx(parts)
        with scope("d_gld"):
            g_last("d")
        with scope("d_glu"):
            g_last("u")
        with scope("d_end"):
            finish()
            wait_sent(0)
        ctx[0] = None

    wait_sent(None)
    assert size[0] <= NSEM, size[0]


def body(saved_inputs, top_grad, norm_gain, gate_weight, up_weight, down_weight):
    x = saved_inputs.reshape(T, W)
    tg = top_grad.reshape(T, W)
    hbm = pl.BlockSpec(memory_space=pl.ANY)
    outs = (
        jax.ShapeDtypeStruct((T, W), BF16),
        jax.ShapeDtypeStruct((PW, FL), F32),
        jax.ShapeDtypeStruct((PW, FL), F32),
        jax.ShapeDtypeStruct((PW, FL), F32),
        jax.ShapeDtypeStruct((1, W), F32),
    )
    out = pl.pallas_call(
        fused_kernel,
        name="fused",
        out_shape=outs,
        in_specs=[hbm] * 6,
        out_specs=[hbm] * 5,
        scratch_shapes=[
            pltpu.VMEM((T, W), BF16),
            pltpu.VMEM((T, W), BF16),
            pltpu.VMEM((1, D), F32),
            pltpu.VMEM((PW, FL), BF16),
            pltpu.VMEM((PW, FL), BF16),
            pltpu.VMEM((PW, FL), BF16),
            *[pltpu.VMEM(o.shape, o.dtype) for o in outs],
            pltpu.VMEM((W, 128), F32),
            pltpu.VMEM((NF, PW, UW), BF16),
            pltpu.VMEM((NF, DR, DH), BF16),
            pltpu.VMEM((NZ, NXL, W, T), BF16),
            pltpu.VMEM((NZ, NXL, H, W, TH), BF16),
            pltpu.VMEM((UW, T), F32),
            pltpu.VMEM((DH + 128 + 16, T), F32),
            pltpu.VMEM((UW, T), BF16),
            pltpu.VMEM((FL, T), BF16),
            pltpu.VMEM((128, T), BF16),
            pltpu.VMEM((W, T), F32),
            pltpu.VMEM((1, T), F32),
            pltpu.VMEM((8, T), F32),
            pltpu.VMEM((NT, 1, T), F32),
            pltpu.VMEM((NT, 1, T), F32),
            pltpu.VMEM((NF, 8, W), F32),
            pltpu.VMEM((7, H, NXL, W, TH), BF16),
            pltpu.VMEM((2, 4, H, NXL, W, TH), BF16),
            pltpu.VMEM((2, H, NXL, W, TH), F32),
            pltpu.VMEM((H, NXL, W, TH), F32),
            pltpu.VMEM((H, W, TH), BF16),
            pltpu.VMEM((H, W, TH), BF16),
            pltpu.VMEM((H, W, TH), BF16),
            pltpu.VMEM((7, PW, UW), BF16),
            pltpu.VMEM((7, PW, UW), BF16),
            pltpu.VMEM((5, PW, UW), F32),
            pltpu.VMEM((7, DR, DH), BF16),
            pltpu.VMEM((7, DR, DH), BF16),
            pltpu.VMEM((5, DR, DH), F32),
            pltpu.SemaphoreType.DMA((NSEM,)),
            pltpu.SemaphoreType.DMA((NSEM,)),
            pltpu.SemaphoreType.DMA((16,)),
            pltpu.SemaphoreType.REGULAR,
        ],
        compiler_params=pltpu.CompilerParams(
            collective_id=0, has_side_effects=True, vmem_limit_bytes=58 * 2**20
        ),
    )(x, tg, norm_gain, gate_weight[0], up_weight[0], down_weight[0].T)
    dx, gg, ug, dg, gn = out
    return (dx.reshape(1, MICRO, ROWS, W), gg[None], ug[None], dg.T[None], gn)


def solution(mesh):
    return jax.shard_map(
        body,
        mesh=mesh,
        in_specs=(
            P("section", None, "fsdp", "tp"),
            P(None, "fsdp", "tp"),
            P("section", None),
            P("section", "fsdp", "tp"),
            P("section", "fsdp", "tp"),
            P("section", "tp", "fsdp"),
        ),
        out_specs=(
            P("section", None, "fsdp", "tp"),
            P("section", "fsdp", "tp"),
            P("section", "fsdp", "tp"),
            P("section", "tp", "fsdp"),
            P("section", "tp"),
        ),
        check_vma=False,
    )
```

```python
import jax
import jax.numpy as jnp
from jax import lax
from jax.experimental import pallas as pl
from jax.experimental.pallas import tpu as pltpu
from jax.sharding import PartitionSpec as P

EPS = 1e-05
MESH = pl.DeviceIdType.MESH
F32 = jnp.float32
BF16 = jnp.bfloat16

NY, NXH, NZ, NXL = 4, 2, 8, 2
NF, NT = NY * NXH, NZ * NXL
MICRO = 8
ROWS = 64
T = MICRO * ROWS
H = 2
TH = T // H
W = 160
PW = NXL * W
FL = 432
GU = 2 * FL
D = W * NT
UW = 896
DH = 384
DR = PW + 16
NCOMMON = 73
NEACH = 48
NBIG = 18
NSMALL = 27


def scope(name):
    return jax.named_scope(name)


def dot(a, b, ca, cb, precision=None):
    return lax.dot_general(
        a, b, (((ca,), (cb,)), ((), ())), preferred_element_type=F32, precision=precision
    )


def fused_kernel(
    x_hbm,
    tg_hbm,
    gain_hbm,
    wg_hbm,
    wu_hbm,
    wd_hbm,
    dx_ref,
    gg_ref,
    ug_ref,
    dg_ref,
    gn_ref,
    x_ref,
    tg_ref,
    gain_row,
    wg_ref,
    wu_ref,
    wd_ref,
    gain,
    wgu,
    wd,
    n_all,
    dy_all,
    gu,
    dh,
    dgu,
    hid,
    hid_mid,
    unit,
    scale,
    stat,
    ssq_in,
    stat_in,
    gain_in,
    pdn,
    rdn,
    pf,
    pown,
    xs,
    xr,
    dxs,
    sgu,
    rgu,
    fgu,
    sgd,
    rgd,
    fgd,
    ssem,
    rsem,
    lsem,
    go,
):
    s = lax.axis_index("section")
    f = lax.axis_index("fsdp")
    t = lax.axis_index("tp")
    y, xh = lax.div(f, NXH), lax.rem(f, NXH)
    z, xl = lax.div(t, NXL), lax.rem(t, NXL)
    oh, ol = 1 - xh, 1 - xl

    def at_y(step):
        return (s, lax.rem(y + step + NY, NY) * NXH + xh, t)

    def at_z(step):
        return (s, f, lax.rem(z + step + NZ, NZ) * NXL + xl)

    dev = {
        "y+": at_y(1),
        "y-": at_y(-1),
        "z+": at_z(1),
        "z-": at_z(-1),
        "xh": (s, y * NXH + oh, t),
        "xl": (s, f, z * NXL + ol),
        "core": (1 - s, f, t),
    }
    across = {
        "core": (1 - s, f, t),
        "xl": (1 - s, *dev["xl"][1:]),
        "z+": (1 - s, *dev["z+"][1:]),
        "z-": (1 - s, *dev["z-"][1:]),
    }
    tp_peers = [(s, f, lax.rem(t + k, NT)) for k in range(1, NT)]
    fs_peers = [(s, lax.rem(f + k, NF), t) for k in range(1, NF)]
    zblk = [lax.rem(z + k, NZ) for k in range(NZ)]
    own, left, right, far = (
        {"c": lax.rem(y + k, NY) * NXH + xh, "o": lax.rem(y + k, NY) * NXH + oh} for k in (0, 3, 1, 2)
    )

    ids = {}
    size = {None: 0, 0: 0, 1: 0}
    private = {"dy": 1, "n": 1, "m": 0, "e": 0}
    ctx = [None]

    def ident(name, n=1):
        if name not in ids:
            sec = private.get(name[0])
            ids[name] = size[sec] + (0 if sec is None else NCOMMON)
            size[sec] += n
            assert size[sec] <= (NCOMMON if sec is None else NEACH), size
        return ids[name]

    def copy(src, dst, sm, rm, to):
        return pltpu.make_async_remote_copy(
            src_ref=src,
            dst_ref=dst,
            send_sem=ssem.at[sm],
            recv_sem=rsem.at[rm],
            device_id=to,
            device_id_type=MESH,
        )

    def static(idx):
        return tuple(i if isinstance(i, (int, pl.Slice)) else 0 for i in idx)

    turn = {sec: {"big": 0, "small": 0} for sec in (0, 1)}
    flying = {0: {}, 1: {}}

    def left_all(kind=None):
        mine = flying[ctx[0]]
        for m in sorted(mine):
            if kind is None or (m < NBIG) == (kind == "big"):
                src, si = mine.pop(m)
                r = src.at[si]
                copy(r, r, m, 0, dev["core"]).wait_send()

    def take(src, si, kind):
        mine, sec = flying[ctx[0]], ctx[0]
        base, n = (0, NBIG) if kind == "big" else (NBIG, NSMALL)
        m = base + turn[sec][kind] % n
        turn[sec][kind] += 1
        if m in mine:
            was, wi = mine.pop(m)
            r = was.at[wi]
            copy(r, r, m, 0, dev["core"]).wait_send()
        mine[m] = (src, static(si))
        return m

    def send(src, si, dst, di, name, to, q=None, kind="small"):
        rm = ident(name, 1 if q is None else 2)
        sm = take(src, si, kind)
        copy(src.at[si], dst.at[di], sm, rm if q is None else rm + q, to).start()

    def arrived(dst, di, name, q=None):
        m = ident(name, 1 if q is None else 2)
        r = dst.at[di]
        copy(r, r, 0, m if q is None else m + q, dev["core"]).wait_recv()

    def rows(n, step, fn):
        def body(i, c):
            fn(pl.multiple_of(i * step, step))
            return c

        lax.fori_loop(0, n // step, body, 0)

    barrier = pltpu.get_barrier_semaphore()
    everyone = tp_peers + fs_peers + list(across.values())
    for to in everyone:
        pl.semaphore_signal(barrier, inc=1, device_id=to, device_id_type=MESH)

    loads = [
        pltpu.make_async_copy(src, dst, lsem.at[k])
        for k, (src, dst) in enumerate(
            (
                (x_hbm, x_ref),
                (tg_hbm, tg_ref),
                (gain_hbm, gain_row),
                (wd_hbm, wd_ref),
                (wg_hbm, wg_ref),
                (wu_hbm, wu_ref),
            )
        )
    ]
    for c in loads:
        c.start()
    with scope("prep"):
        eye = (
            lax.broadcasted_iota(jnp.int32, (W, W), 0) == lax.broadcasted_iota(jnp.int32, (W, W), 1)
        ).astype(BF16)
        loads[0].wait()
        xt = dot(eye, x_ref[...], 1, 1)
        ssq_in[t] = jnp.sum(xt * xt, axis=0, keepdims=True)
        unit[...] = xt
        loads[1].wait()

        @pl.when(s == 1)
        def _():
            top = dot(eye, tg_ref[...], 1, 1).astype(BF16)
            for h in range(H):
                dy_all[z, xl, h] = top[:, h * TH : (h + 1) * TH]

    def pack_d():
        loads[3].wait()

        def pack(r):
            wd[f, pl.ds(r, 32), :] = wd_ref[pl.ds(r, 32), 0:DH]
            wgu[f, pl.ds(r, 32), GU:UW] = wd_ref[pl.ds(r, 32), DH : DH + 32]

        rows(PW, 32, pack)
        last = (
            lax.broadcasted_iota(jnp.int32, (16, FL), 0) + (FL - 16)
            == lax.broadcasted_iota(jnp.int32, (16, FL), 1)
        ).astype(BF16)
        wd[f, PW:DR, 0:PW] = dot(last, wd_ref[...], 1, 1).astype(BF16)

    def pack_u():
        loads[4].wait()
        loads[5].wait()

        def pack(r):
            wgu[f, pl.ds(r, 32), 0:FL] = wg_ref[pl.ds(r, 32), :]
            wgu[f, pl.ds(r, 32), FL:GU] = wu_ref[pl.ds(r, 32), :]

        rows(PW, 32, pack)

    def take_gain():
        loads[2].wait()

        def gains(r):
            mine = lax.broadcasted_iota(jnp.int32, (32, D), 1) == (
                lax.broadcasted_iota(jnp.int32, (32, D), 0) + (t * W + r)
            )
            row = jnp.broadcast_to(gain_row[...], (32, D))
            gain[pl.ds(r, 32), :] = jnp.broadcast_to(
                jnp.sum(jnp.where(mine, row, 0.0), axis=1, keepdims=True), (32, 128)
            )

        rows(W, 32, gains)

    def spread(buf, me, peers, name):
        m = ident((name,))
        for to in peers:
            copy(buf.at[me], buf.at[me], NBIG + NSMALL + ("ssq", "stat", "gain").index(name), m, to).start()

    def collect(buf, peers, name):
        n = len(peers)
        r = buf.at[pl.ds(0, n)]
        copy(r, r, 0, ident((name,)), dev["core"]).wait_recv()
        total = buf[0]
        for k in range(1, n + 1):
            total = total + buf[k]
        return total

    def spread_left(buf, peers, name):
        r = buf.at[pl.ds(0, len(peers))]
        copy(r, r, NBIG + NSMALL + ("ssq", "stat", "gain").index(name), 0, dev["core"]).wait_send()

    with scope("pack"):
        pack_d()
        pack_u()

    with scope("barrier"):
        pl.semaphore_wait(barrier, len(everyone))
    spread(ssq_in, t, tp_peers, "ssq")

    halves = {"u": ((0, 160), (160, 160)), "d": ((0, 160), (160, 176))}
    full = {"u": wgu, "d": wd}

    def w_own(a, dirs):
        for d in dirs:
            send(full[a], (f,), full[a], (f,), ("w", a, "own", d), dev[d], kind="big")

    def w_fwd(a):
        arr = full[a]
        for d, blk, k in (("y+", left["c"], 0), ("y-", right["c"], 1)):
            arrived(arr, (blk,), ("w", a, "own", d))
            part = pl.ds(*halves[a][k])
            send(arr, (blk, part), arr, (blk, part), ("w", a, "fwd", d), dev[d], kind="big")

    def w_pass(a):
        arr, blk = full[a], own["o"]
        arrived(arr, (blk,), ("w", a, "own", "xh"))
        for d in ("y+", "y-"):
            send(arr, (blk,), arr, (blk,), ("w", a, "pass", d), dev[d], kind="big")

    def w_far(a):
        arr, blk = full[a], far["c"]
        for d, k in (("y+", 0), ("y-", 1)):
            arrived(arr, (blk, pl.ds(*halves[a][k])), ("w", a, "fwd", d))
        send(arr, (blk,), arr, (blk,), ("w", a, "far"), dev["xh"], kind="big")

    def w_fwd_o(a):
        arr = full[a]
        for d, blk, k in (("y+", left["o"], 0), ("y-", right["o"], 1)):
            arrived(arr, (blk,), ("w", a, "pass", d))
            part = pl.ds(*halves[a][k])
            send(arr, (blk, part), arr, (blk, part), ("w", a, "fwdo", d), dev[d], kind="big")

    def w_last_y(a):
        arr = full[a]
        for blk, nm in ((far["c"], "fwd"), (far["o"], "fwdo")):
            for d, k in (("y+", 0), ("y-", 1)):
                arrived(arr, (blk, pl.ds(*halves[a][k])), ("w", a, nm, d))

    def w_last(a):
        arr = full[a]
        arrived(arr, (left["o"],), ("w", a, "pass", "y+"))
        arrived(arr, (right["o"],), ("w", a, "pass", "y-"))
        arrived(arr, (far["o"],), ("w", a, "far"))

    def ag_own(buf, nm, hh=()):
        own_at = (z, xl, *hh)
        send(buf, own_at, buf, own_at, (nm, "xl", *hh), dev["xl"])
        send(buf, own_at, buf, own_at, (nm, "z+", 1, 0, *hh), dev["z+"])
        send(buf, own_at, buf, own_at, (nm, "z-", 1, 0, *hh), dev["z-"])

    def ag_partner(buf, nm, hh=()):
        at = (z, ol, *hh)
        arrived(buf, at, (nm, "xl", *hh))
        send(buf, at, buf, at, (nm, "z+", 1, 1, *hh), dev["z+"])
        send(buf, at, buf, at, (nm, "z-", 1, 1, *hh), dev["z-"])

    def ag_fwd(buf, nm, k, j, hh=()):
        q = (xl, ol)[j]
        for d, blk in (("z+", zblk[NZ - k]), ("z-", zblk[k])):
            at = (blk, q, *hh)
            arrived(buf, at, (nm, d, k, j, *hh))
            send(buf, at, buf, at, (nm, d, k + 1, j, *hh), dev[d])

    def ag_fwd3(buf, nm, hh=()):
        for d, blk, q in (("z+", zblk[5], 0), ("z-", zblk[3], 1)):
            for j in range(2):
                arrived(buf, (blk, (xl, ol)[j], *hh), (nm, d, 3, j, *hh))
            send(buf, (blk, q, *hh), buf, (blk, q, *hh), (nm, d, 4, *hh), dev[d])

    def ag_last(buf, nm, hh=()):
        arrived(buf, (zblk[4], 0, *hh), (nm, "z+", 4, *hh))
        arrived(buf, (zblk[4], 1, *hh), (nm, "z-", 4, *hh))

    def agz_pair(buf, nm, k, blk):
        send(buf, (blk, xl), buf, (blk, xl), (nm, "pair", k), dev["xl"])

    def agz_own(buf, nm):
        for d in ("z+", "z-"):
            send(buf, (z, xl), buf, (z, xl), (nm, d, 1), dev[d])

    def agz_fwd(buf, nm, k):
        for d, blk in (("z+", zblk[NZ - k]), ("z-", zblk[k])):
            arrived(buf, (blk, xl), (nm, d, k))
            part = () if k < 3 else (pl.ds(0, 80),) if d == "z+" else (pl.ds(80, 80),)
            send(buf, (blk, xl, *part), buf, (blk, xl, *part), (nm, d, k + 1), dev[d])
        agz_pair(buf, nm, NZ - k, zblk[NZ - k])
        agz_pair(buf, nm, k, zblk[k])

    def agz_far(buf, nm):
        for d, lo in (("z+", 0), ("z-", 80)):
            arrived(buf, (zblk[4], xl, pl.ds(lo, 80)), (nm, d, 4))
        agz_pair(buf, nm, 4, zblk[4])

    def agz_last(buf, nm):
        for k in range(NZ):
            arrived(buf, (zblk[k], ol), (nm, "pair", k))

    def act(buf, i):
        return jnp.concatenate([buf[i, :, h].reshape(PW, TH) for h in range(H)], axis=1)

    def pick(i, table):
        v = table[0]
        for k in range(1, len(table)):
            v = jnp.where(i == k, table[k], v)
        return v

    groups = ((0, 1, 7), (2, 6), (3, 5, 4))

    def together(parts):
        return jnp.concatenate(parts, axis=0)

    z_groups = [[zblk[k] for k in g] for g in groups]
    w_groups = [
        [own["c"], left["c"], right["c"], own["o"], left["o"], right["o"]],
        [far["c"], far["o"]],
    ]

    def forward(g, blocks=z_groups):
        blks = blocks[g]
        part = dot(
            together([wgu[b] for b in blks]),
            together([n_all[b].reshape(PW, T) for b in blks]),
            0,
            0,
        )
        gu[...] = part if g == 0 else gu[...] + part

    def dhidden(g):
        blks = [zblk[k] for k in groups[g]]
        dys = [act(dy_all, b) for b in blks]
        dy = together(dys)
        parts = (
            (0, dot(together([wd[b, 0:PW] for b in blks]), dy, 0, 0)),
            (DH, dot(together([wgu[b, :, UW - 128 : UW] for b in blks]), dy, 0, 0)),
        )
        for r, part in parts:
            at = pl.ds(r, part.shape[0])
            dh[at, :] = part if g == 0 else dh[at, :] + part
        part = dot(wd[blks[0], PW:DR, 0:PW], dys[0], 1, 0)
        for b, d in zip(blks[1:], dys[1:]):
            part = part + dot(wd[b, PW:DR, 0:PW], d, 1, 0)
        at = pl.ds(DH + 128, 16)
        dh[at, :] = part if g == 0 else dh[at, :] + part

    def hidden():
        def body(r):
            gate = gu[pl.ds(r, 16), :]
            up = gu[pl.ds(pl.multiple_of(FL + r, 16), 16), :]
            hid[pl.ds(r, 16), :] = (gate * jax.nn.sigmoid(gate) * up).astype(BF16)

        rows(FL, 16, body)
        hid_mid[0:96, :] = jnp.zeros((96, T), BF16)
        hid_mid[96:128, :] = hid[DH : DH + 32, :]
        dgu[GU:UW, :] = jnp.zeros((UW - GU, T), BF16)

    def normalize():
        row_scale = lax.rsqrt(collect(ssq_in, tp_peers, "ssq") / D + EPS)
        scale[...] = row_scale
        u = unit[...] * row_scale
        unit[...] = u
        n_all[z, xl] = (u * gain[:, 0:1]).astype(BF16)

    @pl.when(s == 1)
    def _():
        ctx[0] = 1
        with scope("a_own"):
            ag_own(dy_all, "dy")
            w_own("d", ("y+", "y-", "xh"))
            w_own("u", ("y+", "y-"))
            take_gain()
        with scope("a_norm"):
            normalize()
        with scope("a_nO"):
            ag_own(n_all, "n")
            w_own("u", ("xh",))
        with scope("a_dyP"):
            ag_partner(dy_all, "dy")
        with scope("a_dy10"):
            ag_fwd(dy_all, "dy", 1, 0)
        with scope("a_wfd"):
            w_fwd("d")
        with scope("a_nP"):
            ag_partner(n_all, "n")
        with scope("a_n10"):
            ag_fwd(n_all, "n", 1, 0)
        with scope("a_dy11"):
            ag_fwd(dy_all, "dy", 1, 1)
        with scope("a_wfu"):
            w_fwd("u")
            w_pass("d")
        with scope("a_n11"):
            ag_fwd(n_all, "n", 1, 1)
        with scope("a_wxd"):
            w_far("d")
        with scope("a_dy20"):
            ag_fwd(dy_all, "dy", 2, 0)
        with scope("a_wpu"):
            w_pass("u")
        with scope("a_n20"):
            ag_fwd(n_all, "n", 2, 0)
        with scope("a_wxu"):
            w_far("u")
        with scope("a_n21"):
            ag_fwd(n_all, "n", 2, 1)
        with scope("a_dy21"):
            ag_fwd(dy_all, "dy", 2, 1)
        with scope("a_n3"):
            ag_fwd3(n_all, "n")
            pl.semaphore_signal(go, inc=1, device_id=dev["core"], device_id_type=MESH)
        with scope("a_dy3"):
            ag_fwd3(dy_all, "dy")
            pl.semaphore_signal(go, inc=1, device_id=dev["core"], device_id_type=MESH)
        with scope("a_wl"):
            w_last("d")
            w_last("u")
        with scope("a_h0"):
            dhidden(0)
        with scope("a_f0"):
            forward(0)
        with scope("a_f1"):
            forward(1)
        with scope("a_h1"):
            dhidden(1)
        with scope("a_nl"):
            ag_last(n_all, "n")
        with scope("a_f2"):
            forward(2)
            hidden()
        with scope("a_dyl"):
            ag_last(dy_all, "dy")
        with scope("a_h2"):
            dhidden(2)
        ctx[0] = None

    @pl.when(s == 0)
    def _():
        ctx[0] = 0
        with scope("b_gain"):
            take_gain()
        with scope("b_norm"):
            normalize()
        with scope("b_go"):
            pl.semaphore_wait(go, 1)
        with scope("b_own"):
            agz_pair(n_all, "m", 0, z)
            w_own("d", ("y+", "y-", "xh"))
            w_own("u", ("y+", "y-", "xh"))
        with scope("b_go2"):
            pl.semaphore_wait(go, 1)
            agz_own(n_all, "m")
        with scope("b_wfd"):
            w_fwd("d")
            w_pass("d")
        with scope("b_n1"):
            agz_fwd(n_all, "m", 1)
        with scope("b_wfu"):
            w_fwd("u")
        with scope("b_n2"):
            agz_fwd(n_all, "m", 2)
        with scope("b_wpu"):
            w_pass("u")
        with scope("b_n3"):
            agz_fwd(n_all, "m", 3)
        with scope("b_wod"):
            w_fwd_o("d")
        with scope("b_n4"):
            agz_far(n_all, "m")
        with scope("b_wou"):
            w_fwd_o("u")
        with scope("b_nl"):
            agz_last(n_all, "m")
        with scope("b_f0"):
            forward(0, w_groups)
        with scope("b_wl"):
            w_last_y("d")
            w_last_y("u")
        with scope("b_f1"):
            forward(1, w_groups)
        with scope("b_hid"):
            hidden()
        with scope("b_dyp"):
            for h in range(H):
                ag_partner(dy_all, "e", (h,))
        with scope("b_dy1"):
            for h in range(H):
                for j in range(2):
                    ag_fwd(dy_all, "e", 1, j, (h,))
        with scope("b_dy2"):
            for h in range(H):
                for j in range(2):
                    ag_fwd(dy_all, "e", 2, j, (h,))
        with scope("b_h0"):
            for h in range(H):
                arrived(dy_all, (z, xl, h), ("e", "core", h))
            dhidden(0)
        with scope("b_dy3"):
            for h in range(H):
                ag_fwd3(dy_all, "e", (h,))
        with scope("b_h1"):
            dhidden(1)
        with scope("b_dyl"):
            for h in range(H):
                ag_last(dy_all, "e", (h,))
        with scope("b_h2"):
            dhidden(2)
        ctx[0] = None

    with scope("elem"):
        stat[...] = jnp.zeros_like(stat)

        def elementwise(r):
            gate = gu[pl.ds(r, 16), :]
            up = gu[pl.ds(pl.multiple_of(FL + r, 16), 16), :]
            dd = dh[pl.ds(pl.multiple_of(jnp.where(r < DH, r, r + 96), 16), 16), :]
            sig = jax.nn.sigmoid(gate)
            silu = gate * sig
            d_gate = (dd * up * sig * (1.0 + gate * (1.0 - sig))).astype(BF16)
            d_up = (dd * silu).astype(BF16)
            dgu[pl.ds(r, 16), :] = d_gate
            dgu[pl.ds(pl.multiple_of(FL + r, 16), 16), :] = d_up
            both = d_gate.astype(F32) * gate + d_up.astype(F32) * up
            stat[...] += both[0:8] + both[8:16]

        rows(FL, 16, elementwise)
        stat_in[t] = jnp.sum(stat[...], axis=0, keepdims=True)
        spread(stat_in, t, tp_peers, "stat")

    ways = (("z+", 0), ("z-", 1))

    def rs_first():
        def body(h, c):
            part = dot(wgu[zblk[4], :, 0:GU], dgu[0:GU, :], 1, 0).reshape(NXL, W, T)
            for hh in range(H):
                pdn[0, hh] = part[:, :, hh * TH : (hh + 1) * TH].astype(BF16)
            return c

        lax.fori_loop(0, 1, body, 0)
        for h in range(H):
            for d, w in ways:
                send(pdn, (0, h, w), rdn, (w, 0, h, w), ("rs", d, 1, h), dev[d], q=w)

    def rs_compute(k):
        def body(w, c):
            blk = jnp.where(w == 0, zblk[5 - k], zblk[3 + k])
            part = dot(wgu[blk, :, 0:GU], dgu[0:GU, :], 1, 0).reshape(NXL, W, T)
            for hh in range(H):
                pf[w, hh] = part[:, :, hh * TH : (hh + 1) * TH]
            return c

        lax.fori_loop(0, 2, body, 0)

    def rs_step(k):
        slot = 2 * k - 3
        if k == 2:
            for h in range(H):
                for d, w in ways:
                    q = 1 - w
                    pdn[slot + w, h, q] = pf[w, h, q].astype(BF16)
                    send(pdn, (slot + w, h, q), rdn, (w, k - 1, h, q), ("rs", d, k, h), dev[d], q=q)
        for h in range(H):
            for j in range(2):
                for d, w in ways:
                    if k == 2:
                        q = w
                        if j:
                            continue
                    else:
                        q = (ol, xl)[j]
                    arrived(rdn, (w, k - 2, h, q), ("rs", d, k - 1, h), q=q)
                    pdn[slot + w, h, q] = (pf[w, h, q] + rdn[w, k - 2, h, q].astype(F32)).astype(BF16)
                    send(pdn, (slot + w, h, q), rdn, (w, k - 1, h, q), ("rs", d, k, h), dev[d], q=q)

    def rs_own():
        def body(h, c):
            part = dot(wgu[z, :, 0:GU], dgu[0:GU, :], 1, 0).reshape(NXL, W, T)
            for hh in range(H):
                pown[hh] = part[:, :, hh * TH : (hh + 1) * TH]
            return c

        lax.fori_loop(0, 1, body, 0)

    def rs_last():
        for h in range(H):
            for q in (ol, xl):
                for d, w in ways:
                    arrived(rdn, (w, 3, h, q), ("rs", d, 4, h), q=q)
                if q is ol:
                    xs[h] = (
                        pown[h, q] + rdn[0, 3, h, q].astype(F32) + rdn[1, 3, h, q].astype(F32)
                    ).astype(BF16)
                    send(xs, (h,), xr, (h,), ("rx", h), dev["xl"])

    def dx_part(h, norm_stat):
        arrived(xr, (h,), ("rx", h))
        cols = slice(h * TH, (h + 1) * TH)
        d_normed = (
            pown[h, xl]
            + rdn[0, 3, h, xl].astype(F32)
            + rdn[1, 3, h, xl].astype(F32)
            + xr[h].astype(F32)
        )
        u = unit[:, cols]
        dx = dy_all[z, xl, h].astype(F32) + scale[:, cols] * (
            d_normed * gain[:, 0:1] - u * norm_stat[:, cols]
        )
        dxs[h] = dx.astype(BF16)
        return d_normed * u

    def gain_dx(parts):
        total = dot(
            jnp.ones((8, T), F32), jnp.concatenate(parts, axis=1), 1, 1, lax.Precision.HIGHEST
        )
        gain_in[f] = total
        spread(gain_in, f, fs_peers, "gain")
        for h in range(H):
            dx_ref[h * TH : (h + 1) * TH, :] = dot(dxs[h], eye, 0, 0).astype(BF16)

    sg, rg, fg = {"u": sgu, "d": sgd}, {"u": rgu, "d": rgd}, {"u": fgu, "d": fgd}
    size_of = {"u": (PW, 32), "d": (DR, 48)}

    def wgrad(a, blk, dst, i):
        dy = act(dy_all, blk)
        if a == "u":
            cut = UW - 128
            n = n_all[blk].reshape(PW, T)
            dst[i, :, 0:cut] = dot(n, dgu[0:cut, :], 1, 1).astype(dst.dtype)
            edge = dot(n, dgu[cut:UW, :], 1, 1) + dot(dy, hid_mid[...], 1, 1)
            dst[i, :, cut:UW] = edge.astype(dst.dtype)
        else:
            dst[i, 0:PW, :] = dot(dy, hid[0:DH, :], 1, 1).astype(dst.dtype)
            dst[i, PW:DR, 0:PW] = dot(hid[FL - 16 : FL, :], dy, 1, 1).astype(dst.dtype)

    direct = [far["o"], right["o"], left["o"]]
    kept = [far["c"], own["o"], right["c"], left["c"], own["c"]]

    def g_first(a):
        rm = ident(("g", a, 0), 3)
        sm = [take(sg[a], (0,), "big") for _ in range(3)]

        def body(i, c):
            wgrad(a, pick(i, direct), sg[a], i)
            to = pick(i, [dev[d][1] for d in ("xh", "y+", "y-")])
            copy(sg[a].at[i], rg[a].at[i], pick(i, sm), rm + i, (s, to, t)).start()
            return c

        lax.fori_loop(0, 3, body, 0)

    def g_kept(a, lo, hi):
        def body(i, c):
            wgrad(a, pick(i, kept), fg[a], i)
            return c

        lax.fori_loop(lo, hi, body, 0)

    def g_sum(a, slot, own_i, recv, span=None):
        n, st = size_of[a]
        lo, n = span if span else (0, n)
        st = 16 if span else st

        def body(r):
            r = pl.multiple_of(r + lo, 16)
            v = fg[a][own_i, pl.ds(r, st), :]
            for k in recv:
                v = v + rg[a][k, pl.ds(r, st), :].astype(F32)
            sg[a][slot, pl.ds(r, st), :] = v.astype(BF16)

        rows(n, st, body)

    def g_far(a):
        arrived(rg[a], (0,), ("g", a, 0), q=0)
        g_sum(a, 3, 0, (0,))
        for d, k in (("y+", 0), ("y-", 1)):
            part = pl.ds(*halves[a][k])
            send(sg[a], (3, part), rg[a], (3, part), ("g", a, 3, d), dev[d], kind="big")

    def g_near(a):
        for d, k, slot in (("y+", 0, 4), ("y-", 1, 5)):
            part = pl.ds(*halves[a][k])
            arrived(rg[a], (3, part), ("g", a, 3, d))
            g_sum(a, slot, 2 + k, (3,), halves[a][k])
            g_sum(a, slot, 2 + k, (), halves[a][1 - k])
            send(sg[a], (slot,), rg[a], (slot,), ("g", a, slot), dev[d], kind="big")

    def g_partner(a):
        arrived(rg[a], (1,), ("g", a, 0), q=1)
        arrived(rg[a], (2,), ("g", a, 0), q=2)
        g_sum(a, 6, 1, (1, 2))
        send(sg[a], (6,), rg[a], (6,), ("g", a, 6), dev["xh"], kind="big")

    def g_last(a):
        for k in (4, 5, 6):
            arrived(rg[a], (k,), ("g", a, k))

        def total(at):
            v = fg[a][4, at, :]
            for k in (4, 5, 6):
                v = v + rg[a][k, at, :].astype(F32)
            return v

        def body(r):
            at = pl.ds(r, 32)
            v = total(at)
            if a == "u":
                gg_ref[at, :] = v[:, 0:FL]
                ug_ref[at, :] = v[:, FL:GU]
                dg_ref[at, DH : DH + 32] = v[:, GU:UW]
            else:
                dg_ref[at, 0:DH] = v

        if a == "d":
            rows(PW, 32, body)
            v = total(pl.ds(PW, 16))[:, 0:PW]
            unit16 = (
                lax.broadcasted_iota(jnp.int32, (16, 16), 0)
                == lax.broadcasted_iota(jnp.int32, (16, 16), 1)
            ).astype(F32)
            dg_ref[:, DH + 32 : FL] = dot(v, unit16, 0, 0, lax.Precision.HIGHEST)
            return
        for c in range(2):
            def part(r, c=c):
                body(pl.multiple_of(r + c * 160, 16))

            rows(160, 32, part)
            at = pl.ds(c * 160, 160)

    def finish():
        gn_ref[...] = collect(gain_in, fs_peers, "gain")[0:1]
        left_all()

    @pl.when(s == 1)
    def _():
        ctx[0] = 1
        with scope("c_r1"):
            rs_first()
            rs_compute(2)
        with scope("c_r2"):
            rs_step(2)
            rs_compute(3)
        with scope("c_r3"):
            rs_step(3)
            rs_compute(4)
        with scope("c_r4"):
            rs_step(4)
            rs_own()
        with scope("c_rl"):
            rs_last()
        with scope("c_stat"):
            norm_stat = collect(stat_in, tp_peers, "stat") / D
        with scope("c_dx"):
            parts = []
            for h in range(H):
                parts.append(dx_part(h, norm_stat))
                for d, name in (("xl", ("xl", h)), ("z+", ("z+", 1, 0, h)), ("z-", ("z-", 1, 0, h)), ("core", ("core", h))):
                    send(dxs, (h,), dy_all, (z, xl, h), ("e", *name), across[d])
        with scope("c_g1"):
            left_all("big")
            g_first("u")
            g_first("d")
        with scope("c_gain"):
            gain_dx(parts)
        with scope("c_gk1"):
            g_kept("u", 0, 1)
            g_kept("d", 0, 1)
        with scope("c_gk2"):
            g_kept("u", 1, 5)
        with scope("c_gfu"):
            g_far("u")
        with scope("c_gpu"):
            g_partner("u")
        with scope("c_gk3"):
            g_kept("d", 1, 5)
        with scope("c_gfd"):
            g_far("d")
        with scope("c_gpd"):
            g_partner("d")
        with scope("c_gnu"):
            g_near("u")
        with scope("c_gnd"):
            g_near("d")
        with scope("c_glu"):
            g_last("u")
        with scope("c_gld"):
            g_last("d")
        with scope("c_end"):
            finish()
        ctx[0] = None

    @pl.when(s == 0)
    def _():
        ctx[0] = 0
        with scope("d_r1"):
            rs_first()
        with scope("d_g1"):
            left_all("big")
            g_first("u")
            g_first("d")
        with scope("d_rc2"):
            rs_compute(2)
        with scope("d_r2"):
            rs_step(2)
        with scope("d_gk1"):
            g_kept("u", 0, 2)
            g_kept("d", 0, 2)
        with scope("d_rc3"):
            rs_compute(3)
        with scope("d_gfu"):
            g_far("u")
        with scope("d_gpu"):
            g_partner("u")
        with scope("d_r3"):
            rs_step(3)
        with scope("d_gfd"):
            g_far("d")
        with scope("d_gpd"):
            g_partner("d")
        with scope("d_gk2"):
            g_kept("u", 2, 4)
        with scope("d_rc4"):
            rs_compute(4)
        with scope("d_gnu"):
            g_near("u")
        with scope("d_r4"):
            rs_step(4)
        with scope("d_gk3"):
            g_kept("d", 2, 4)
        with scope("d_gnd"):
            g_near("d")
        with scope("d_gk4"):
            g_kept("u", 4, 5)
            g_kept("d", 4, 5)
            rs_own()
        with scope("d_rl"):
            rs_last()
            norm_stat = collect(stat_in, tp_peers, "stat") / D
        with scope("d_dx"):
            parts = [dx_part(h, norm_stat) for h in range(H)]
            gain_dx(parts)
        with scope("d_glu"):
            g_last("u")
        with scope("d_gld"):
            g_last("d")
        with scope("d_end"):
            finish()
        ctx[0] = None

    spread_left(ssq_in, tp_peers, "ssq")
    spread_left(stat_in, tp_peers, "stat")
    spread_left(gain_in, fs_peers, "gain")


def put_kernel(*refs):
    copies = [pltpu.make_async_copy(refs[k], refs[5 + k], refs[10].at[k]) for k in range(5)]
    for c in copies:
        c.start()
    for c in copies:
        c.wait()


def body(saved_inputs, top_grad, norm_gain, gate_weight, up_weight, down_weight):
    x = saved_inputs.reshape(T, W)
    tg = top_grad.reshape(T, W)
    hbm = pl.BlockSpec(memory_space=pl.ANY)
    outs = (
        jax.ShapeDtypeStruct((T, W), BF16),
        jax.ShapeDtypeStruct((PW, FL), F32),
        jax.ShapeDtypeStruct((PW, FL), F32),
        jax.ShapeDtypeStruct((PW, FL), F32),
        jax.ShapeDtypeStruct((1, W), F32),
    )
    out = pl.pallas_call(
        fused_kernel,
        name="fused",
        out_shape=[pltpu.VMEM(o.shape, o.dtype) for o in outs],
        in_specs=[hbm] * 6,
        out_specs=[pl.BlockSpec(memory_space=pltpu.VMEM)] * 5,
        scratch_shapes=[
            pltpu.VMEM((T, W), BF16),
            pltpu.VMEM((T, W), BF16),
            pltpu.VMEM((1, D), F32),
            pltpu.VMEM((PW, FL), BF16),
            pltpu.VMEM((PW, FL), BF16),
            pltpu.VMEM((PW, FL), BF16),
            pltpu.VMEM((W, 128), F32),
            pltpu.VMEM((NF, PW, UW), BF16),
            pltpu.VMEM((NF, DR, DH), BF16),
            pltpu.VMEM((NZ, NXL, W, T), BF16),
            pltpu.VMEM((NZ, NXL, H, W, TH), BF16),
            pltpu.VMEM((UW, T), F32),
            pltpu.VMEM((DH + 128 + 16, T), F32),
            pltpu.VMEM((UW, T), BF16),
            pltpu.VMEM((FL, T), BF16),
            pltpu.VMEM((128, T), BF16),
            pltpu.VMEM((W, T), F32),
            pltpu.VMEM((1, T), F32),
            pltpu.VMEM((8, T), F32),
            pltpu.VMEM((NT, 1, T), F32),
            pltpu.VMEM((NT, 1, T), F32),
            pltpu.VMEM((NF, 8, W), F32),
            pltpu.VMEM((7, H, NXL, W, TH), BF16),
            pltpu.VMEM((2, 4, H, NXL, W, TH), BF16),
            pltpu.VMEM((2, H, NXL, W, TH), F32),
            pltpu.VMEM((H, NXL, W, TH), F32),
            pltpu.VMEM((H, W, TH), BF16),
            pltpu.VMEM((H, W, TH), BF16),
            pltpu.VMEM((H, W, TH), BF16),
            pltpu.VMEM((7, PW, UW), BF16),
            pltpu.VMEM((7, PW, UW), BF16),
            pltpu.VMEM((5, PW, UW), F32),
            pltpu.VMEM((7, DR, DH), BF16),
            pltpu.VMEM((7, DR, DH), BF16),
            pltpu.VMEM((5, DR, DH), F32),
            pltpu.SemaphoreType.DMA((NBIG + NSMALL + 3,)),
            pltpu.SemaphoreType.DMA((NCOMMON + NEACH,)),
            pltpu.SemaphoreType.DMA((6,)),
            pltpu.SemaphoreType.REGULAR,
        ],
        compiler_params=pltpu.CompilerParams(
            collective_id=0, has_side_effects=True, vmem_limit_bytes=58 * 2**20
        ),
    )(x, tg, norm_gain, gate_weight[0], up_weight[0], down_weight[0].T)
    dx, gg, ug, dg, gn = pl.pallas_call(
        put_kernel,
        name="put",
        out_shape=outs,
        in_specs=[pl.BlockSpec(memory_space=pltpu.VMEM)] * 5,
        out_specs=[hbm] * 5,
        scratch_shapes=[pltpu.SemaphoreType.DMA((5,))],
    )(*[pltpu.with_memory_space_constraint(o, pltpu.VMEM) for o in out])
    return (dx.reshape(1, MICRO, ROWS, W), gg[None], ug[None], dg.T[None], gn)


def solution(mesh):
    return jax.shard_map(
        body,
        mesh=mesh,
        in_specs=(
            P("section", None, "fsdp", "tp"),
            P(None, "fsdp", "tp"),
            P("section", None),
            P("section", "fsdp", "tp"),
            P("section", "fsdp", "tp"),
            P("section", "tp", "fsdp"),
        ),
        out_specs=(
            P("section", None, "fsdp", "tp"),
            P("section", "fsdp", "tp"),
            P("section", "fsdp", "tp"),
            P("section", "tp", "fsdp"),
            P("section", "tp"),
        ),
        check_vma=False,
    )
```

```python
import jax
import jax.numpy as jnp
from jax import lax
from jax.experimental import pallas as pl
from jax.experimental.pallas import tpu as pltpu
from jax.sharding import PartitionSpec as P

EPS = 1e-05
MESH = pl.DeviceIdType.MESH
F32 = jnp.float32
BF16 = jnp.bfloat16

NY, NXH, NZ, NXL = 4, 2, 8, 2
NF, NT = NY * NXH, NZ * NXL
MICRO = 8
ROWS = 64
T = MICRO * ROWS
H = 2
TH = T // H
W = 160
PW = NXL * W
FL = 432
GU = 2 * FL
D = W * NT
UW = 896
DH = 384
DR = PW + 16
NCOMMON = 77
NEACH = 48
NBIG = 20
NSMALL = 27


def dot(a, b, ca, cb, precision=None):
    return lax.dot_general(
        a, b, (((ca,), (cb,)), ((), ())), preferred_element_type=F32, precision=precision
    )


def fused_kernel(
    x_hbm,
    tg_hbm,
    gain_hbm,
    wg_hbm,
    wu_hbm,
    wd_hbm,
    dx_ref,
    gg_ref,
    ug_ref,
    dg_ref,
    gn_ref,
    x_ref,
    tg_ref,
    gain_row,
    wg_ref,
    wu_ref,
    wd_ref,
    gain,
    wgu,
    wd,
    n_all,
    dy_all,
    gu,
    dh,
    dgu,
    hid,
    hid_mid,
    unit,
    scale,
    stat,
    ssq_in,
    stat_in,
    gain_in,
    pdn,
    rdn,
    pf,
    pown,
    xs,
    xr,
    dxs,
    sgu,
    rgu,
    fgu,
    sgd,
    rgd,
    fgd,
    ssem,
    rsem,
    lsem,
    go,
):
    s = lax.axis_index("section")
    f = lax.axis_index("fsdp")
    t = lax.axis_index("tp")
    y, xh = lax.div(f, NXH), lax.rem(f, NXH)
    z, xl = lax.div(t, NXL), lax.rem(t, NXL)
    oh, ol = 1 - xh, 1 - xl

    def at_y(step):
        return (s, lax.rem(y + step + NY, NY) * NXH + xh, t)

    def at_z(step):
        return (s, f, lax.rem(z + step + NZ, NZ) * NXL + xl)

    dev = {
        "y+": at_y(1),
        "y-": at_y(-1),
        "z+": at_z(1),
        "z-": at_z(-1),
        "xh": (s, y * NXH + oh, t),
        "xl": (s, f, z * NXL + ol),
        "core": (1 - s, f, t),
    }
    across = {
        "core": (1 - s, f, t),
        "xl": (1 - s, *dev["xl"][1:]),
        "z+": (1 - s, *dev["z+"][1:]),
        "z-": (1 - s, *dev["z-"][1:]),
    }
    tp_peers = [(s, f, lax.rem(t + k, NT)) for k in range(1, NT)]
    fs_peers = [(s, lax.rem(f + k, NF), t) for k in range(1, NF)]
    zblk = [lax.rem(z + k, NZ) for k in range(NZ)]
    own, left, right, far = (
        {"c": lax.rem(y + k, NY) * NXH + xh, "o": lax.rem(y + k, NY) * NXH + oh} for k in (0, 3, 1, 2)
    )

    ids = {}
    size = {None: 0, 0: 0, 1: 0}
    private = {"dy": 1, "n": 1, "m": 0, "e": 0}
    ctx = [None]

    def ident(name, n=1):
        if name not in ids:
            sec = private.get(name[0])
            ids[name] = size[sec] + (0 if sec is None else NCOMMON)
            size[sec] += n
            assert size[sec] <= (NCOMMON if sec is None else NEACH), size
        return ids[name]

    def copy(src, dst, sm, rm, to):
        return pltpu.make_async_remote_copy(
            src_ref=src,
            dst_ref=dst,
            send_sem=ssem.at[sm],
            recv_sem=rsem.at[rm],
            device_id=to,
            device_id_type=MESH,
        )

    def static(idx):
        return tuple(i if isinstance(i, (int, pl.Slice)) else 0 for i in idx)

    turn = {sec: {"big": 0, "small": 0} for sec in (0, 1)}
    flying = {0: {}, 1: {}}

    def left_all(kind=None):
        mine = flying[ctx[0]]
        for m in sorted(mine):
            if kind is None or (m < NBIG) == (kind == "big"):
                src, si = mine.pop(m)
                r = src.at[si]
                copy(r, r, m, 0, dev["core"]).wait_send()

    def take(src, si, kind):
        mine, sec = flying[ctx[0]], ctx[0]
        base, n = (0, NBIG) if kind == "big" else (NBIG, NSMALL)
        m = base + turn[sec][kind] % n
        turn[sec][kind] += 1
        if m in mine:
            was, wi = mine.pop(m)
            r = was.at[wi]
            copy(r, r, m, 0, dev["core"]).wait_send()
        mine[m] = (src, static(si))
        return m

    def send(src, si, dst, di, name, to, q=None, kind="small"):
        rm = ident(name, 1 if q is None else 2)
        sm = take(src, si, kind)
        copy(src.at[si], dst.at[di], sm, rm if q is None else rm + q, to).start()

    def arrived(dst, di, name, q=None):
        m = ident(name, 1 if q is None else 2)
        r = dst.at[di]
        copy(r, r, 0, m if q is None else m + q, dev["core"]).wait_recv()

    def rows(n, step, fn):
        def body(i, c):
            fn(pl.multiple_of(i * step, step))
            return c

        lax.fori_loop(0, n // step, body, 0)

    barrier = pltpu.get_barrier_semaphore()
    everyone = tp_peers + fs_peers + list(across.values())
    for to in everyone:
        pl.semaphore_signal(barrier, inc=1, device_id=to, device_id_type=MESH)

    loads = [
        pltpu.make_async_copy(src, dst, lsem.at[k])
        for k, (src, dst) in enumerate(
            (
                (x_hbm, x_ref),
                (tg_hbm, tg_ref),
                (gain_hbm, gain_row),
                (wd_hbm, wd_ref),
                (wg_hbm, wg_ref),
                (wu_hbm, wu_ref),
            )
        )
    ]
    for c in loads:
        c.start()
    eye = (
        lax.broadcasted_iota(jnp.int32, (W, W), 0) == lax.broadcasted_iota(jnp.int32, (W, W), 1)
    ).astype(BF16)
    loads[0].wait()
    xt = dot(eye, x_ref[...], 1, 1)
    ssq_in[t] = jnp.sum(xt * xt, axis=0, keepdims=True)
    unit[...] = xt
    loads[1].wait()

    @pl.when(s == 1)
    def _():
        top = dot(eye, tg_ref[...], 1, 1).astype(BF16)
        for h in range(H):
            dy_all[z, xl, h] = top[:, h * TH : (h + 1) * TH]

    def pack_d():
        loads[3].wait()

        def pack(r):
            wd[f, pl.ds(r, 32), :] = wd_ref[pl.ds(r, 32), 0:DH]
            wgu[f, pl.ds(r, 32), GU:UW] = wd_ref[pl.ds(r, 32), DH : DH + 32]

        rows(PW, 32, pack)
        last = (
            lax.broadcasted_iota(jnp.int32, (16, FL), 0) + (FL - 16)
            == lax.broadcasted_iota(jnp.int32, (16, FL), 1)
        ).astype(BF16)
        wd[f, PW:DR, 0:PW] = dot(last, wd_ref[...], 1, 1).astype(BF16)

    def pack_u():
        loads[4].wait()
        loads[5].wait()

        def pack(r):
            wgu[f, pl.ds(r, 32), 0:FL] = wg_ref[pl.ds(r, 32), :]
            wgu[f, pl.ds(r, 32), FL:GU] = wu_ref[pl.ds(r, 32), :]

        rows(PW, 32, pack)

    def take_gain():
        loads[2].wait()

        def gains(r):
            mine = lax.broadcasted_iota(jnp.int32, (32, D), 1) == (
                lax.broadcasted_iota(jnp.int32, (32, D), 0) + (t * W + r)
            )
            row = jnp.broadcast_to(gain_row[...], (32, D))
            gain[pl.ds(r, 32), :] = jnp.broadcast_to(
                jnp.sum(jnp.where(mine, row, 0.0), axis=1, keepdims=True), (32, 128)
            )

        rows(W, 32, gains)

    def spread(buf, me, peers, name):
        m = ident((name,))
        for to in peers:
            copy(buf.at[me], buf.at[me], NBIG + NSMALL + ("ssq", "stat", "gain").index(name), m, to).start()

    def collect(buf, peers, name):
        n = len(peers)
        r = buf.at[pl.ds(0, n)]
        copy(r, r, 0, ident((name,)), dev["core"]).wait_recv()
        total = buf[0]
        for k in range(1, n + 1):
            total = total + buf[k]
        return total

    def spread_left(buf, peers, name):
        r = buf.at[pl.ds(0, len(peers))]
        copy(r, r, NBIG + NSMALL + ("ssq", "stat", "gain").index(name), 0, dev["core"]).wait_send()

    pack_d()
    pack_u()

    pl.semaphore_wait(barrier, len(everyone))
    spread(ssq_in, t, tp_peers, "ssq")

    halves = {"u": ((0, 160), (160, 160)), "d": ((0, 160), (160, 176))}
    full = {"u": wgu, "d": wd}

    def w_own(a, dirs):
        for d in dirs:
            send(full[a], (f,), full[a], (f,), ("w", a, "own", d), dev[d], kind="big")

    def w_fwd(a):
        arr = full[a]
        for d, blk, k in (("y+", left["c"], 0), ("y-", right["c"], 1)):
            arrived(arr, (blk,), ("w", a, "own", d))
            part = pl.ds(*halves[a][k])
            send(arr, (blk, part), arr, (blk, part), ("w", a, "fwd", d), dev[d], kind="big")

    def w_pass(a):
        arr, blk = full[a], own["o"]
        arrived(arr, (blk,), ("w", a, "own", "xh"))
        for d in ("y+", "y-"):
            send(arr, (blk,), arr, (blk,), ("w", a, "pass", d), dev[d], kind="big")

    def w_far(a):
        arr, blk = full[a], far["c"]
        for d, k in (("y+", 0), ("y-", 1)):
            arrived(arr, (blk, pl.ds(*halves[a][k])), ("w", a, "fwd", d))
        send(arr, (blk,), arr, (blk,), ("w", a, "far"), dev["xh"], kind="big")

    def w_fwd_o(a):
        arr = full[a]
        for d, blk, k in (("y+", left["o"], 0), ("y-", right["o"], 1)):
            arrived(arr, (blk,), ("w", a, "pass", d))
            part = pl.ds(*halves[a][k])
            send(arr, (blk, part), arr, (blk, part), ("w", a, "fwdo", d), dev[d], kind="big")

    def w_last_y(a):
        arr = full[a]
        for blk, nm in ((far["c"], "fwd"), (far["o"], "fwdo")):
            for d, k in (("y+", 0), ("y-", 1)):
                arrived(arr, (blk, pl.ds(*halves[a][k])), ("w", a, nm, d))

    def w_last(a):
        arr = full[a]
        arrived(arr, (left["o"],), ("w", a, "pass", "y+"))
        arrived(arr, (right["o"],), ("w", a, "pass", "y-"))
        arrived(arr, (far["o"],), ("w", a, "far"))

    def ag_xl(buf, nm):
        send(buf, (z, xl), buf, (z, xl), (nm, "xl"), dev["xl"])

    def ag_z(buf, nm):
        for d in ("z+", "z-"):
            send(buf, (z, xl), buf, (z, xl), (nm, d, 1, 0), dev[d])

    def ag_own(buf, nm):
        ag_xl(buf, nm)
        ag_z(buf, nm)

    def ag_partner(buf, nm, hh=()):
        at = (z, ol, *hh)
        arrived(buf, at, (nm, "xl", *hh))
        send(buf, at, buf, at, (nm, "z+", 1, 1, *hh), dev["z+"])
        send(buf, at, buf, at, (nm, "z-", 1, 1, *hh), dev["z-"])

    def ag_fwd(buf, nm, k, j, hh=()):
        q = (xl, ol)[j]
        for d, blk in (("z+", zblk[NZ - k]), ("z-", zblk[k])):
            at = (blk, q, *hh)
            arrived(buf, at, (nm, d, k, j, *hh))
            send(buf, at, buf, at, (nm, d, k + 1, j, *hh), dev[d])

    def ag_fwd3(buf, nm, hh=()):
        for d, blk, q in (("z+", zblk[5], 0), ("z-", zblk[3], 1)):
            for j in range(2):
                arrived(buf, (blk, (xl, ol)[j], *hh), (nm, d, 3, j, *hh))
            send(buf, (blk, q, *hh), buf, (blk, q, *hh), (nm, d, 4, *hh), dev[d])

    def ag_last(buf, nm, hh=()):
        arrived(buf, (zblk[4], 0, *hh), (nm, "z+", 4, *hh))
        arrived(buf, (zblk[4], 1, *hh), (nm, "z-", 4, *hh))

    def act(buf, i):
        return jnp.concatenate([buf[i, :, h].reshape(PW, TH) for h in range(H)], axis=1)

    def pick(i, table):
        v = table[0]
        for k in range(1, len(table)):
            v = jnp.where(i == k, table[k], v)
        return v

    def together(parts):
        return jnp.concatenate(parts, axis=0)

    def forward(*ks):
        blks = [zblk[k] for k in ks]
        part = dot(
            together([wgu[b] for b in blks]),
            together([n_all[b].reshape(PW, T) for b in blks]),
            0,
            0,
        )
        gu[...] = part if 0 in ks else gu[...] + part

    def dhidden(*ks):
        blks = [zblk[k] for k in ks]
        dys = [act(dy_all, b) for b in blks]
        dy = together(dys)
        parts = (
            (0, dot(together([wd[b, 0:PW] for b in blks]), dy, 0, 0)),
            (DH, dot(together([wgu[b, :, UW - 128 : UW] for b in blks]), dy, 0, 0)),
        )
        for r, part in parts:
            at = pl.ds(r, part.shape[0])
            dh[at, :] = part if 0 in ks else dh[at, :] + part
        part = dot(wd[blks[0], PW:DR, 0:PW], dys[0], 1, 0)
        for b, d in zip(blks[1:], dys[1:]):
            part = part + dot(wd[b, PW:DR, 0:PW], d, 1, 0)
        at = pl.ds(DH + 128, 16)
        dh[at, :] = part if 0 in ks else dh[at, :] + part

    def hidden():
        def body(r):
            gate = gu[pl.ds(r, 16), :]
            up = gu[pl.ds(pl.multiple_of(FL + r, 16), 16), :]
            hid[pl.ds(r, 16), :] = (gate * jax.nn.sigmoid(gate) * up).astype(BF16)

        rows(FL, 16, body)
        hid_mid[0:96, :] = jnp.zeros((96, T), BF16)
        hid_mid[96:128, :] = hid[DH : DH + 32, :]

    def normalize():
        row_scale = lax.rsqrt(collect(ssq_in, tp_peers, "ssq") / D + EPS)
        scale[...] = row_scale
        u = unit[...] * row_scale
        unit[...] = u
        n_all[z, xl] = (u * gain[:, 0:1]).astype(BF16)

    def cotangents():
        stat[...] = jnp.zeros_like(stat)
        dgu[GU:UW, :] = jnp.zeros((UW - GU, T), BF16)

        def elementwise(r):
            gate = gu[pl.ds(r, 16), :]
            up = gu[pl.ds(pl.multiple_of(FL + r, 16), 16), :]
            dd = dh[pl.ds(pl.multiple_of(jnp.where(r < DH, r, r + 96), 16), 16), :]
            sig = jax.nn.sigmoid(gate)
            silu = gate * sig
            d_gate = (dd * up * sig * (1.0 + gate * (1.0 - sig))).astype(BF16)
            d_up = (dd * silu).astype(BF16)
            dgu[pl.ds(r, 16), :] = d_gate
            dgu[pl.ds(pl.multiple_of(FL + r, 16), 16), :] = d_up
            both = d_gate.astype(F32) * gate + d_up.astype(F32) * up
            stat[...] += both[0:8] + both[8:16]

        rows(FL, 16, elementwise)
        stat_in[t] = jnp.sum(stat[...], axis=0, keepdims=True)
        spread(stat_in, t, tp_peers, "stat")

    ways = (("z+", 0), ("z-", 1))

    def rs_first():
        def body(h, c):
            part = dot(wgu[zblk[4], :, 0:GU], dgu[0:GU, :], 1, 0).reshape(NXL, W, T)
            for hh in range(H):
                pdn[0, hh] = part[:, :, hh * TH : (hh + 1) * TH].astype(BF16)
            return c

        lax.fori_loop(0, 1, body, 0)
        for h in range(H):
            for d, w in ways:
                send(pdn, (0, h, w), rdn, (w, 0, h, w), ("rs", d, 1, h), dev[d], q=w)

    def rs_compute(k):
        def body(w, c):
            blk = jnp.where(w == 0, zblk[5 - k], zblk[3 + k])
            part = dot(wgu[blk, :, 0:GU], dgu[0:GU, :], 1, 0).reshape(NXL, W, T)
            for hh in range(H):
                pf[w, hh] = part[:, :, hh * TH : (hh + 1) * TH]
            return c

        lax.fori_loop(0, 2, body, 0)

    def rs_step(k, hs=range(H)):
        slot = 2 * k - 3
        if k == 2:
            for h in hs:
                for d, w in ways:
                    q = 1 - w
                    pdn[slot + w, h, q] = pf[w, h, q].astype(BF16)
                    send(pdn, (slot + w, h, q), rdn, (w, k - 1, h, q), ("rs", d, k, h), dev[d], q=q)
        for h in hs:
            for j in range(2 if k > 2 else 1):
                for d, w in ways:
                    q = w if k == 2 else (ol, xl)[j]
                    arrived(rdn, (w, k - 2, h, q), ("rs", d, k - 1, h), q=q)
                    pdn[slot + w, h, q] = (pf[w, h, q] + rdn[w, k - 2, h, q].astype(F32)).astype(BF16)
                    send(pdn, (slot + w, h, q), rdn, (w, k - 1, h, q), ("rs", d, k, h), dev[d], q=q)

    def rs_own():
        def body(h, c):
            part = dot(wgu[z, :, 0:GU], dgu[0:GU, :], 1, 0).reshape(NXL, W, T)
            for hh in range(H):
                pown[hh] = part[:, :, hh * TH : (hh + 1) * TH]
            return c

        lax.fori_loop(0, 1, body, 0)

    def rs_last():
        for h in range(H):
            for q in (ol, xl):
                for d, w in ways:
                    arrived(rdn, (w, 3, h, q), ("rs", d, 4, h), q=q)
                if q is ol:
                    xs[h] = (
                        pown[h, q] + rdn[0, 3, h, q].astype(F32) + rdn[1, 3, h, q].astype(F32)
                    ).astype(BF16)
                    send(xs, (h,), xr, (h,), ("rx", h), dev["xl"])

    def dx_part(h, norm_stat):
        arrived(xr, (h,), ("rx", h))
        cols = slice(h * TH, (h + 1) * TH)
        d_normed = (
            pown[h, xl]
            + rdn[0, 3, h, xl].astype(F32)
            + rdn[1, 3, h, xl].astype(F32)
            + xr[h].astype(F32)
        )
        u = unit[:, cols]
        dx = dy_all[z, xl, h].astype(F32) + scale[:, cols] * (
            d_normed * gain[:, 0:1] - u * norm_stat[:, cols]
        )
        dxs[h] = dx.astype(BF16)
        return d_normed * u

    def gain_dx(parts):
        total = dot(
            jnp.ones((8, T), F32), jnp.concatenate(parts, axis=1), 1, 1, lax.Precision.HIGHEST
        )
        gain_in[f] = total
        spread(gain_in, f, fs_peers, "gain")
        for h in range(H):
            dx_ref[h * TH : (h + 1) * TH, :] = dot(dxs[h], eye, 0, 0).astype(BF16)

    sg, rg, fg = {"u": sgu, "d": sgd}, {"u": rgu, "d": rgd}, {"u": fgu, "d": fgd}
    size_of = {"u": (PW, 32), "d": (DR, 48)}

    def wgrad(a, blk, dst, i):
        dy = act(dy_all, blk)
        if a == "u":
            cut = UW - 128
            n = n_all[blk].reshape(PW, T)
            dst[i, :, 0:cut] = dot(n, dgu[0:cut, :], 1, 1).astype(dst.dtype)
            edge = dot(n, dgu[cut:UW, :], 1, 1) + dot(dy, hid_mid[...], 1, 1)
            dst[i, :, cut:UW] = edge.astype(dst.dtype)
        else:
            dst[i, 0:PW, :] = dot(dy, hid[0:DH, :], 1, 1).astype(dst.dtype)
            dst[i, PW:DR, 0:PW] = dot(hid[FL - 16 : FL, :], dy, 1, 1).astype(dst.dtype)

    direct = [far["o"], right["o"], left["o"]]
    kept = [far["c"], own["o"], right["c"], left["c"], own["c"]]

    def g_first(a, lo=0, hi=3):
        rm = ident(("g", a, 0), 3)
        sm = [take(sg[a], (0,), "big") if lo <= i < hi else 0 for i in range(3)]

        def body(i, c):
            wgrad(a, pick(i, direct), sg[a], i)
            to = pick(i, [dev[d][1] for d in ("xh", "y+", "y-")])
            copy(sg[a].at[i], rg[a].at[i], pick(i, sm), rm + i, (s, to, t)).start()
            return c

        lax.fori_loop(lo, hi, body, 0)

    def g_kept(a, lo, hi):
        def body(i, c):
            wgrad(a, pick(i, kept), fg[a], i)
            return c

        lax.fori_loop(lo, hi, body, 0)

    def g_sum(a, slot, own_i, recv, span=None):
        n, st = size_of[a]
        lo, n = span if span else (0, n)
        st = 16 if span else st

        def body(r):
            r = pl.multiple_of(r + lo, 16)
            v = fg[a][own_i, pl.ds(r, st), :]
            for k in recv:
                v = v + rg[a][k, pl.ds(r, st), :].astype(F32)
            sg[a][slot, pl.ds(r, st), :] = v.astype(BF16)

        rows(n, st, body)

    def g_far(a):
        arrived(rg[a], (0,), ("g", a, 0), q=0)
        g_sum(a, 3, 0, (0,))
        for d, k in (("y+", 0), ("y-", 1)):
            part = pl.ds(*halves[a][k])
            send(sg[a], (3, part), rg[a], (3, part), ("g", a, 3, d), dev[d], kind="big")

    def g_near(a, waits):
        for d, k, slot in (("y+", 0, 4), ("y-", 1, 5)):
            half = halves[a][k if waits else 1 - k]
            part = pl.ds(*half)
            if waits:
                arrived(rg[a], (3, part), ("g", a, 3, d))
            g_sum(a, slot, 2 + k, (3,) if waits else (), half)
            send(sg[a], (slot, part), rg[a], (slot, part), ("g", a, slot, waits), dev[d], kind="big")

    def g_partner(a):
        arrived(rg[a], (1,), ("g", a, 0), q=1)
        arrived(rg[a], (2,), ("g", a, 0), q=2)
        g_sum(a, 6, 1, (1, 2))
        send(sg[a], (6,), rg[a], (6,), ("g", a, 6), dev["xh"], kind="big")

    def g_last(a):
        for k in (0, 1):
            for waits in (False, True):
                part = pl.ds(*halves[a][k if waits else 1 - k])
                arrived(rg[a], (4 + k, part), ("g", a, 4 + k, waits))
        arrived(rg[a], (6,), ("g", a, 6))

        def total(at):
            v = fg[a][4, at, :]
            for k in (4, 5, 6):
                v = v + rg[a][k, at, :].astype(F32)
            return v

        def body(r):
            at = pl.ds(r, 32)
            v = total(at)
            if a == "u":
                gg_ref[at, :] = v[:, 0:FL]
                ug_ref[at, :] = v[:, FL:GU]
                dg_ref[at, DH : DH + 32] = v[:, GU:UW]
            else:
                dg_ref[at, 0:DH] = v

        if a == "d":
            rows(PW, 32, body)
            v = total(pl.ds(PW, 16))[:, 0:PW]
            unit16 = (
                lax.broadcasted_iota(jnp.int32, (16, 16), 0)
                == lax.broadcasted_iota(jnp.int32, (16, 16), 1)
            ).astype(F32)
            dg_ref[:, DH + 32 : FL] = dot(v, unit16, 0, 0, lax.Precision.HIGHEST)
            return
        for c in range(2):
            def part(r, c=c):
                body(pl.multiple_of(r + c * 160, 16))

            rows(160, 32, part)
            at = pl.ds(c * 160, 160)

    def finish():
        gn_ref[...] = collect(gain_in, fs_peers, "gain")[0:1]
        left_all()

    @pl.when(s == 1)
    def _():
        ctx[0] = 1
        ag_own(dy_all, "dy")
        w_own("d", ("y+", "y-", "xh"))
        w_own("u", ("y+", "y-"))
        take_gain()
        normalize()
        ag_own(n_all, "n")
        w_own("u", ("xh",))
        ag_partner(dy_all, "dy")
        ag_fwd(dy_all, "dy", 1, 0)
        w_fwd("d")
        ag_partner(n_all, "n")
        ag_fwd(n_all, "n", 1, 0)
        ag_fwd(dy_all, "dy", 1, 1)
        w_fwd("u")
        w_pass("d")
        ag_fwd(n_all, "n", 1, 1)
        w_far("d")
        ag_fwd(dy_all, "dy", 2, 0)
        w_pass("u")
        ag_fwd(n_all, "n", 2, 0)
        w_far("u")
        ag_fwd(n_all, "n", 2, 1)
        ag_fwd(dy_all, "dy", 2, 1)
        ag_fwd3(n_all, "n")
        pl.semaphore_signal(go, inc=1, device_id=dev["core"], device_id_type=MESH)
        ag_fwd3(dy_all, "dy")
        w_last("d")
        w_last("u")
        dhidden(0, 1, 7)
        forward(0, 1, 7)
        forward(2, 6, 3, 5)
        dhidden(2, 6, 3, 5)
        ag_last(n_all, "n")
        forward(4)
        ag_last(dy_all, "dy")
        dhidden(4)
        cotangents()
        rs_first()
        rs_compute(2)
        hidden()
        rs_step(2)
        rs_compute(3)
        rs_step(3)
        rs_compute(4)
        rs_step(4)
        pl.semaphore_signal(go, inc=1, device_id=dev["core"], device_id_type=MESH)
        rs_own()
        left_all("big")
        g_first("u", 1, 3)
        rs_last()
        norm_stat = collect(stat_in, tp_peers, "stat") / D
        parts = []
        for h in range(H):
            parts.append(dx_part(h, norm_stat))
            for d, name in (("xl", ("xl", h)), ("z+", ("z+", 1, 0, h)), ("z-", ("z-", 1, 0, h)), ("core", ("core", h))):
                send(dxs, (h,), dy_all, (z, xl, h), ("e", *name), across[d])
        g_first("u", 0, 1)
        g_kept("u", 2, 4)
        g_near("u", False)
        g_first("d")
        gain_dx(parts)
        g_kept("u", 0, 2)
        g_partner("u")
        g_kept("d", 0, 4)
        g_far("u")
        g_far("d")
        g_partner("d")
        g_near("d", False)
        g_kept("u", 4, 5)
        g_kept("d", 4, 5)
        g_near("u", True)
        g_near("d", True)
        g_last("u")
        g_last("d")
        finish()
        ctx[0] = None

    @pl.when(s == 0)
    def _():
        ctx[0] = 0
        take_gain()
        normalize()
        pl.semaphore_wait(go, 1)
        ag_own(n_all, "m")
        w_own("d", ("y+", "y-", "xh"))
        w_own("u", ("y+", "y-", "xh"))
        ag_partner(n_all, "m")
        ag_fwd(n_all, "m", 1, 0)
        w_fwd("d")
        ag_fwd(n_all, "m", 1, 1)
        w_fwd("u")
        w_pass("d")
        w_far("d")
        w_pass("u")
        w_far("u")
        pl.semaphore_wait(go, 1)
        ag_fwd(n_all, "m", 2, 0)
        ag_fwd(n_all, "m", 2, 1)
        w_last("d")
        w_last("u")
        forward(0, 1, 7)
        for h in range(H):
            ag_partner(dy_all, "e", (h,))
        ag_fwd3(n_all, "m")
        forward(2, 6)
        for h in range(H):
            for j in range(2):
                ag_fwd(dy_all, "e", 1, j, (h,))
        forward(3, 5)
        for h in range(H):
            for j in range(2):
                ag_fwd(dy_all, "e", 2, j, (h,))
        ag_last(n_all, "m")
        forward(4)
        hidden()
        for h in range(H):
            arrived(dy_all, (z, xl, h), ("e", "core", h))
        dhidden(0, 1, 7)
        for h in range(H):
            ag_fwd3(dy_all, "e", (h,))
        dhidden(2, 6, 3, 5)
        for h in range(H):
            ag_last(dy_all, "e", (h,))
        dhidden(4)
        cotangents()
        rs_first()
        left_all("big")
        g_first("u")
        rs_compute(2)
        rs_step(2)
        g_kept("u", 2, 4)
        g_near("u", False)
        g_first("d")
        rs_compute(3)
        rs_step(3, (0,))
        rs_step(3, (1,))
        g_kept("u", 0, 2)
        g_far("u")
        g_partner("u")
        rs_compute(4)
        rs_step(4)
        g_kept("d", 0, 4)
        g_far("d")
        g_near("d", False)
        rs_own()
        rs_last()
        norm_stat = collect(stat_in, tp_peers, "stat") / D
        g_partner("d")
        g_kept("u", 4, 5)
        g_kept("d", 4, 5)
        g_near("u", True)
        parts = [dx_part(h, norm_stat) for h in range(H)]
        gain_dx(parts)
        g_near("d", True)
        g_last("u")
        g_last("d")
        finish()
        ctx[0] = None

    spread_left(ssq_in, tp_peers, "ssq")
    spread_left(stat_in, tp_peers, "stat")
    spread_left(gain_in, fs_peers, "gain")


def put_kernel(*refs):
    copies = [pltpu.make_async_copy(refs[k], refs[5 + k], refs[10].at[k]) for k in range(5)]
    for c in copies:
        c.start()
    for c in copies:
        c.wait()


def body(saved_inputs, top_grad, norm_gain, gate_weight, up_weight, down_weight):
    x = saved_inputs.reshape(T, W)
    tg = top_grad.reshape(T, W)
    hbm = pl.BlockSpec(memory_space=pl.ANY)
    outs = (
        jax.ShapeDtypeStruct((T, W), BF16),
        jax.ShapeDtypeStruct((PW, FL), F32),
        jax.ShapeDtypeStruct((PW, FL), F32),
        jax.ShapeDtypeStruct((PW, FL), F32),
        jax.ShapeDtypeStruct((1, W), F32),
    )
    out = pl.pallas_call(
        fused_kernel,
        name="fused",
        out_shape=[pltpu.VMEM(o.shape, o.dtype) for o in outs],
        in_specs=[hbm] * 6,
        out_specs=[pl.BlockSpec(memory_space=pltpu.VMEM)] * 5,
        scratch_shapes=[
            pltpu.VMEM((T, W), BF16),
            pltpu.VMEM((T, W), BF16),
            pltpu.VMEM((1, D), F32),
            pltpu.VMEM((PW, FL), BF16),
            pltpu.VMEM((PW, FL), BF16),
            pltpu.VMEM((PW, FL), BF16),
            pltpu.VMEM((W, 128), F32),
            pltpu.VMEM((NF, PW, UW), BF16),
            pltpu.VMEM((NF, DR, DH), BF16),
            pltpu.VMEM((NZ, NXL, W, T), BF16),
            pltpu.VMEM((NZ, NXL, H, W, TH), BF16),
            pltpu.VMEM((UW, T), F32),
            pltpu.VMEM((DH + 128 + 16, T), F32),
            pltpu.VMEM((UW, T), BF16),
            pltpu.VMEM((FL, T), BF16),
            pltpu.VMEM((128, T), BF16),
            pltpu.VMEM((W, T), F32),
            pltpu.VMEM((1, T), F32),
            pltpu.VMEM((8, T), F32),
            pltpu.VMEM((NT, 1, T), F32),
            pltpu.VMEM((NT, 1, T), F32),
            pltpu.VMEM((NF, 8, W), F32),
            pltpu.VMEM((7, H, NXL, W, TH), BF16),
            pltpu.VMEM((2, 4, H, NXL, W, TH), BF16),
            pltpu.VMEM((2, H, NXL, W, TH), F32),
            pltpu.VMEM((H, NXL, W, TH), F32),
            pltpu.VMEM((H, W, TH), BF16),
            pltpu.VMEM((H, W, TH), BF16),
            pltpu.VMEM((H, W, TH), BF16),
            pltpu.VMEM((7, PW, UW), BF16),
            pltpu.VMEM((7, PW, UW), BF16),
            pltpu.VMEM((5, PW, UW), F32),
            pltpu.VMEM((7, DR, DH), BF16),
            pltpu.VMEM((7, DR, DH), BF16),
            pltpu.VMEM((5, DR, DH), F32),
            pltpu.SemaphoreType.DMA((NBIG + NSMALL + 3,)),
            pltpu.SemaphoreType.DMA((NCOMMON + NEACH,)),
            pltpu.SemaphoreType.DMA((6,)),
            pltpu.SemaphoreType.REGULAR,
        ],
        compiler_params=pltpu.CompilerParams(
            collective_id=0, has_side_effects=True, vmem_limit_bytes=58 * 2**20
        ),
    )(x, tg, norm_gain, gate_weight[0], up_weight[0], down_weight[0].T)
    dx, gg, ug, dg, gn = pl.pallas_call(
        put_kernel,
        name="put",
        out_shape=outs,
        in_specs=[pl.BlockSpec(memory_space=pltpu.VMEM)] * 5,
        out_specs=[hbm] * 5,
        scratch_shapes=[pltpu.SemaphoreType.DMA((5,))],
    )(*[pltpu.with_memory_space_constraint(o, pltpu.VMEM) for o in out])
    return (dx.reshape(1, MICRO, ROWS, W), gg[None], ug[None], dg.T[None], gn)


def solution(mesh):
    return jax.shard_map(
        body,
        mesh=mesh,
        in_specs=(
            P("section", None, "fsdp", "tp"),
            P(None, "fsdp", "tp"),
            P("section", None),
            P("section", "fsdp", "tp"),
            P("section", "fsdp", "tp"),
            P("section", "tp", "fsdp"),
        ),
        out_specs=(
            P("section", None, "fsdp", "tp"),
            P("section", "fsdp", "tp"),
            P("section", "fsdp", "tp"),
            P("section", "tp", "fsdp"),
            P("section", "tp"),
        ),
        check_vma=False,
    )
```

```python
import jax
import jax.numpy as jnp
from jax import lax
from jax.experimental import pallas as pl
from jax.experimental.pallas import tpu as pltpu
from jax.sharding import PartitionSpec as P

EPS = 1e-05
MESH = pl.DeviceIdType.MESH
F32 = jnp.float32
BF16 = jnp.bfloat16

NY, NXH, NZ, NXL = 4, 2, 8, 2
NF, NT = NY * NXH, NZ * NXL
MICRO = 8
ROWS = 64
T = MICRO * ROWS
H = 2
TH = T // H
W = 160
PW = NXL * W
FL = 432
GU = 2 * FL
D = W * NT
UW = 896
DH = 384
DR = PW + 16
NCOMMON = 79
NEACH = 48
NBIG = 20
NSMALL = 27


def dot(a, b, ca, cb, precision=None):
    return lax.dot_general(
        a, b, (((ca,), (cb,)), ((), ())), preferred_element_type=F32, precision=precision
    )


def fused_kernel(
    x_hbm,
    tg_hbm,
    gain_hbm,
    wg_hbm,
    wu_hbm,
    wd_hbm,
    dx_ref,
    gg_ref,
    ug_ref,
    dg_ref,
    gn_ref,
    x_ref,
    tg_ref,
    gain_row,
    wg_ref,
    wu_ref,
    wd_ref,
    gain,
    gain_sq,
    gain_all,
    x_all,
    wgu,
    wd,
    n_all,
    dy_all,
    gu,
    dh,
    dgu,
    hid,
    hid_mid,
    unit,
    scale,
    stat,
    ssq_in,
    stat_in,
    gain_in,
    pdn,
    rdn,
    pf,
    pown,
    gx,
    nstat,
    xs,
    xr,
    dxs,
    sgu,
    rgu,
    fgu,
    sgd,
    rgd,
    fgd,
    ssem,
    rsem,
    lsem,
    go,
):
    s = lax.axis_index("section")
    f = lax.axis_index("fsdp")
    t = lax.axis_index("tp")
    y, xh = lax.div(f, NXH), lax.rem(f, NXH)
    z, xl = lax.div(t, NXL), lax.rem(t, NXL)
    oh, ol = 1 - xh, 1 - xl

    def at_y(step):
        return (s, lax.rem(y + step + NY, NY) * NXH + xh, t)

    def at_z(step):
        return (s, f, lax.rem(z + step + NZ, NZ) * NXL + xl)

    dev = {
        "y+": at_y(1),
        "y-": at_y(-1),
        "z+": at_z(1),
        "z-": at_z(-1),
        "xh": (s, y * NXH + oh, t),
        "xl": (s, f, z * NXL + ol),
        "core": (1 - s, f, t),
    }
    across = {
        "core": (1 - s, f, t),
        "xl": (1 - s, *dev["xl"][1:]),
        "z+": (1 - s, *dev["z+"][1:]),
        "z-": (1 - s, *dev["z-"][1:]),
    }
    tp_peers = [(s, f, lax.rem(t + k, NT)) for k in range(1, NT)]
    fs_peers = [(s, lax.rem(f + k, NF), t) for k in range(1, NF)]
    zblk = [lax.rem(z + k, NZ) for k in range(NZ)]
    own, left, right, far = (
        {"c": lax.rem(y + k, NY) * NXH + xh, "o": lax.rem(y + k, NY) * NXH + oh} for k in (0, 3, 1, 2)
    )

    ids = {}
    size = {None: 0, 0: 0, 1: 0}
    private = {"dy": 1, "n": 1, "m": 0, "e": 0}
    ctx = [None]

    def ident(name, n=1):
        if name not in ids:
            sec = private.get(name[0])
            ids[name] = size[sec] + (0 if sec is None else NCOMMON)
            size[sec] += n
            assert size[sec] <= (NCOMMON if sec is None else NEACH), size
        return ids[name]

    def copy(src, dst, sm, rm, to):
        return pltpu.make_async_remote_copy(
            src_ref=src,
            dst_ref=dst,
            send_sem=ssem.at[sm],
            recv_sem=rsem.at[rm],
            device_id=to,
            device_id_type=MESH,
        )

    def static(idx):
        return tuple(i if isinstance(i, (int, pl.Slice)) else 0 for i in idx)

    turn = {sec: {"big": 0, "small": 0} for sec in (0, 1)}
    flying = {0: {}, 1: {}}

    def left_all(kind=None):
        mine = flying[ctx[0]]
        for m in sorted(mine):
            if kind is None or (m < NBIG) == (kind == "big"):
                src, si = mine.pop(m)
                r = src.at[si]
                copy(r, r, m, 0, dev["core"]).wait_send()

    def take(src, si, kind):
        mine, sec = flying[ctx[0]], ctx[0]
        base, n = (0, NBIG) if kind == "big" else (NBIG, NSMALL)
        m = base + turn[sec][kind] % n
        turn[sec][kind] += 1
        if m in mine:
            was, wi = mine.pop(m)
            r = was.at[wi]
            copy(r, r, m, 0, dev["core"]).wait_send()
        mine[m] = (src, static(si))
        return m

    def send(src, si, dst, di, name, to, q=None, kind="small"):
        rm = ident(name, 1 if q is None else 2)
        sm = take(src, si, kind)
        copy(src.at[si], dst.at[di], sm, rm if q is None else rm + q, to).start()

    def arrived(dst, di, name, q=None):
        m = ident(name, 1 if q is None else 2)
        r = dst.at[di]
        copy(r, r, 0, m if q is None else m + q, dev["core"]).wait_recv()

    def rows(n, step, fn):
        def body(i, c):
            fn(pl.multiple_of(i * step, step))
            return c

        lax.fori_loop(0, n // step, body, 0)

    barrier = pltpu.get_barrier_semaphore()
    everyone = tp_peers + fs_peers + list(across.values())
    for to in everyone:
        pl.semaphore_signal(barrier, inc=1, device_id=to, device_id_type=MESH)

    loads = [
        pltpu.make_async_copy(src, dst, lsem.at[k])
        for k, (src, dst) in enumerate(
            (
                (x_hbm, x_ref),
                (tg_hbm, tg_ref),
                (gain_hbm, gain_row),
                (wd_hbm, wd_ref),
                (wg_hbm, wg_ref),
                (wu_hbm, wu_ref),
            )
        )
    ]
    for c in loads:
        c.start()
    eye = (
        lax.broadcasted_iota(jnp.int32, (W, W), 0) == lax.broadcasted_iota(jnp.int32, (W, W), 1)
    ).astype(BF16)
    loads[0].wait()
    xt = dot(eye, x_ref[...], 1, 1)
    ssq_in[t] = jnp.sum(xt * xt, axis=0, keepdims=True)
    unit[...] = xt
    loads[1].wait()

    @pl.when(s == 1)
    def _():
        x_all[z, xl] = xt.astype(BF16)
        top = dot(eye, tg_ref[...], 1, 1).astype(BF16)
        for h in range(H):
            dy_all[z, xl, h] = top[:, h * TH : (h + 1) * TH]

    def pack_d():
        loads[3].wait()

        def pack(r):
            wd[f, pl.ds(r, 32), :] = wd_ref[pl.ds(r, 32), 0:DH]
            wgu[f, pl.ds(r, 32), GU:UW] = wd_ref[pl.ds(r, 32), DH : DH + 32]

        rows(PW, 32, pack)
        last = (
            lax.broadcasted_iota(jnp.int32, (16, FL), 0) + (FL - 16)
            == lax.broadcasted_iota(jnp.int32, (16, FL), 1)
        ).astype(BF16)
        wd[f, PW:DR, 0:PW] = dot(last, wd_ref[...], 1, 1).astype(BF16)

    def pack_u():
        loads[4].wait()
        loads[5].wait()

        def pack(r):
            wgu[f, pl.ds(r, 32), 0:FL] = wg_ref[pl.ds(r, 32), :]
            wgu[f, pl.ds(r, 32), FL:GU] = wu_ref[pl.ds(r, 32), :]

        rows(PW, 32, pack)

    def take_gain():
        loads[2].wait()
        gain_sq[...] = jnp.zeros_like(gain_sq)
        for c in range(D // 128):
            gain_sq[c : c + 1, :] = gain_row[:, c * 128 : (c + 1) * 128]
        cols = gain_sq[...].T
        for c in range(D // 128):
            gain_all[c * 128 : (c + 1) * 128, :] = jnp.broadcast_to(cols[:, c : c + 1], (128, 128))
        gain[...] = gain_all[pl.ds(pl.multiple_of(t * W, 8), W), :]

    def spread(buf, me, peers, name):
        m = ident((name,))
        for to in peers:
            copy(buf.at[me], buf.at[me], NBIG + NSMALL + ("ssq", "stat", "gain").index(name), m, to).start()

    def collect(buf, peers, name):
        n = len(peers)
        r = buf.at[pl.ds(0, n)]
        copy(r, r, 0, ident((name,)), dev["core"]).wait_recv()
        total = buf[0]
        for k in range(1, n + 1):
            total = total + buf[k]
        return total

    def spread_left(buf, peers, name):
        r = buf.at[pl.ds(0, len(peers))]
        copy(r, r, NBIG + NSMALL + ("ssq", "stat", "gain").index(name), 0, dev["core"]).wait_send()

    pack_d()
    pack_u()

    pl.semaphore_wait(barrier, len(everyone))
    spread(ssq_in, t, tp_peers, "ssq")

    halves = {"u": ((0, 160), (160, 160)), "d": ((0, 160), (160, 176))}
    full = {"u": wgu, "d": wd}

    def w_own(a, dirs):
        for d in dirs:
            if d == "xh":
                send(full[a], (f,), full[a], (f,), ("w", a, "own", d), dev[d], kind="big")
        for i in range(2):
            for d, k in (("y+", i), ("y-", 1 - i)):
                if d in dirs:
                    at = (f, pl.ds(*halves[a][k]))
                    send(full[a], at, full[a], at, ("w", a, "own", d, i), dev[d], kind="big")

    def w_fwd(a):
        arr = full[a]
        for d, blk, k in (("y+", left["c"], 0), ("y-", right["c"], 1)):
            at = (blk, pl.ds(*halves[a][k]))
            arrived(arr, at, ("w", a, "own", d, 0))
            send(arr, at, arr, at, ("w", a, "fwd", d), dev[d], kind="big")

    def w_pass(a):
        arr, blk = full[a], own["o"]
        arrived(arr, (blk,), ("w", a, "own", "xh"))
        for d in ("y+", "y-"):
            send(arr, (blk,), arr, (blk,), ("w", a, "pass", d), dev[d], kind="big")

    def w_far(a):
        arr, blk = full[a], far["c"]
        for d, k in (("y+", 0), ("y-", 1)):
            arrived(arr, (blk, pl.ds(*halves[a][k])), ("w", a, "fwd", d))
        send(arr, (blk,), arr, (blk,), ("w", a, "far"), dev["xh"], kind="big")

    def w_last(a):
        arr = full[a]
        arrived(arr, (left["o"],), ("w", a, "pass", "y+"))
        arrived(arr, (right["o"],), ("w", a, "pass", "y-"))
        arrived(arr, (far["o"],), ("w", a, "far"))
        for d, blk, k in (("y+", left["c"], 1), ("y-", right["c"], 0)):
            arrived(arr, (blk, pl.ds(*halves[a][k])), ("w", a, "own", d, 1))

    def ag_xl(buf, nm):
        send(buf, (z, xl), buf, (z, xl), (nm, "xl"), dev["xl"])

    def ag_z(buf, nm):
        for d in ("z+", "z-"):
            send(buf, (z, xl), buf, (z, xl), (nm, d, 1, 0), dev[d])

    def ag_own(buf, nm):
        ag_xl(buf, nm)
        ag_z(buf, nm)

    def ag_partner(buf, nm, hh=()):
        at = (z, ol, *hh)
        arrived(buf, at, (nm, "xl", *hh))
        send(buf, at, buf, at, (nm, "z+", 1, 1, *hh), dev["z+"])
        send(buf, at, buf, at, (nm, "z-", 1, 1, *hh), dev["z-"])

    def ag_fwd(buf, nm, k, j, hh=()):
        q = (xl, ol)[j]
        for d, blk in (("z+", zblk[NZ - k]), ("z-", zblk[k])):
            at = (blk, q, *hh)
            arrived(buf, at, (nm, d, k, j, *hh))
            send(buf, at, buf, at, (nm, d, k + 1, j, *hh), dev[d])

    def ag_fwd3(buf, nm, hh=()):
        for d, blk, q in (("z+", zblk[5], 0), ("z-", zblk[3], 1)):
            for j in range(2):
                arrived(buf, (blk, (xl, ol)[j], *hh), (nm, d, 3, j, *hh))
            send(buf, (blk, q, *hh), buf, (blk, q, *hh), (nm, d, 4, *hh), dev[d])

    def ag_last(buf, nm, hh=()):
        arrived(buf, (zblk[4], 0, *hh), (nm, "z+", 4, *hh))
        arrived(buf, (zblk[4], 1, *hh), (nm, "z-", 4, *hh))

    def pair_send(buf, nm, *ks):
        for k in ks:
            at = (zblk[k], xl)
            send(buf, at, buf, at, (nm, "pair", k), dev["xl"])

    def pair_wait(buf, nm, *ks):
        for k in ks:
            arrived(buf, (zblk[k], ol), (nm, "pair", k))

    def own_wait(buf, nm, k):
        for d, b in (("z+", zblk[NZ - k]), ("z-", zblk[k])):
            arrived(buf, (b, xl), (nm, d, k, 0))

    def z_send(buf, nm, k, j):
        for d, b in (("z+", zblk[NZ - k]), ("z-", zblk[k])):
            at = (b, (xl, ol)[j])
            send(buf, at, buf, at, (nm, d, k + 1, j), dev[d])

    def act(buf, i):
        return jnp.concatenate([buf[i, :, h].reshape(PW, TH) for h in range(H)], axis=1)

    def pick(i, table):
        v = table[0]
        for k in range(1, len(table)):
            v = jnp.where(i == k, table[k], v)
        return v

    def together(parts):
        return jnp.concatenate(parts, axis=0)

    def forward(*ks):
        blks = [zblk[k] for k in ks]
        part = dot(
            together([wgu[b] for b in blks]),
            together([n_all[b].reshape(PW, T) for b in blks]),
            0,
            0,
        )
        gu[...] = part if 0 in ks else gu[...] + part

    def dhidden(*ks):
        blks = [zblk[k] for k in ks]
        dys = [act(dy_all, b) for b in blks]
        dy = together(dys)
        parts = (
            (0, dot(together([wd[b, 0:PW] for b in blks]), dy, 0, 0)),
        )
        for r, part in parts:
            at = pl.ds(r, part.shape[0])
            dh[at, :] = part if 0 in ks else dh[at, :] + part
        part = dot(wd[blks[0], PW:DR, 0:PW], dys[0], 1, 0)
        for b, d in zip(blks[1:], dys[1:]):
            part = part + dot(wd[b, PW:DR, 0:PW], d, 1, 0)
        at = pl.ds(DH + 128, 16)
        dh[at, :] = part if 0 in ks else dh[at, :] + part

    def dhidden_mid():
        lhs = together([wgu[b, :, UW - 128 : UW] for b in range(NF)])
        dh[DH : DH + 128, :] = dot(lhs, together([act(dy_all, b) for b in range(NF)]), 0, 0)

    def hidden():
        def body(r):
            gate = gu[pl.ds(r, 16), :]
            up = gu[pl.ds(pl.multiple_of(FL + r, 16), 16), :]
            hid[pl.ds(r, 16), :] = (gate * jax.nn.sigmoid(gate) * up).astype(BF16)

        rows(FL, 48, lambda r: [body(pl.multiple_of(r + k, 16)) for k in (0, 16, 32)])
        hid_mid[0:96, :] = jnp.zeros((96, T), BF16)
        hid_mid[96:128, :] = hid[DH : DH + 32, :]

    def normalize():
        row_scale = lax.rsqrt(collect(ssq_in, tp_peers, "ssq") / D + EPS)
        scale[...] = row_scale
        unit[...] = unit[...] * row_scale

    def norm_own():
        n_all[z, xl] = (unit[...] * gain[:, 0:1]).astype(BF16)

    def norm_blocks(*ks):
        for k in ks:
            b = zblk[k]
            for q in range(NXL):
                g = gain_all[pl.ds(pl.multiple_of(b * PW + q * W, 8), W), :]
                for c in range(T // 128):
                    at = slice(c * 128, (c + 1) * 128)
                    n_all[b, q, :, at] = (
                        x_all[b, q, :, at].astype(F32) * scale[:, at] * g
                    ).astype(BF16)

    def cotangents():
        stat[...] = jnp.zeros_like(stat)
        dgu[GU:UW, :] = jnp.zeros((UW - GU, T), BF16)

        def elementwise(r):
            gate = gu[pl.ds(r, 16), :]
            up = gu[pl.ds(pl.multiple_of(FL + r, 16), 16), :]
            dd = dh[pl.ds(pl.multiple_of(jnp.where(r < DH, r, r + 96), 16), 16), :]
            sig = jax.nn.sigmoid(gate)
            silu = gate * sig
            d_gate = (dd * up * sig * (1.0 + gate * (1.0 - sig))).astype(BF16)
            d_up = (dd * silu).astype(BF16)
            dgu[pl.ds(r, 16), :] = d_gate
            dgu[pl.ds(pl.multiple_of(FL + r, 16), 16), :] = d_up
            both = d_gate.astype(F32) * gate + d_up.astype(F32) * up
            stat[...] += both[0:8] + both[8:16]

        rows(FL, 48, lambda r: [elementwise(pl.multiple_of(r + k, 16)) for k in (0, 16, 32)])
        stat_in[t] = jnp.sum(stat[...], axis=0, keepdims=True)
        spread(stat_in, t, tp_peers, "stat")

    ways = (("z+", 0), ("z-", 1))

    def rs_first():
        def body(h, c):
            part = dot(wgu[zblk[4], :, 0:GU], dgu[0:GU, :], 1, 0).reshape(NXL, W, T)
            for hh in range(H):
                pdn[0, hh] = part[:, :, hh * TH : (hh + 1) * TH].astype(BF16)
            return c

        lax.fori_loop(0, 1, body, 0)
        for h in range(H):
            for d, w in ways:
                send(pdn, (0, h, w), rdn, (w, 0, h, w), ("rs", d, 1, h), dev[d], q=w)

    def rs_compute(k):
        def body(w, c):
            blk = jnp.where(w == 0, zblk[5 - k], zblk[3 + k])
            part = dot(wgu[blk, :, 0:GU], dgu[0:GU, :], 1, 0).reshape(NXL, W, T)
            for hh in range(H):
                pf[k - 2, w, hh] = part[:, :, hh * TH : (hh + 1) * TH]
            return c

        lax.fori_loop(0, 2, body, 0)

    def rs_free():
        for h in range(H):
            for d, w in ways:
                q = 1 - w
                pdn[1 + w, h, q] = pf[0, w, h, q].astype(BF16)
                send(pdn, (1 + w, h, q), rdn, (w, 1, h, q), ("rs", d, 2, h), dev[d], q=q)

    def rs_step(k, ahead=(True, False), hs=range(H)):
        slot = 2 * k - 3
        for first in ahead:
            for h in hs:
                for d, w in ways:
                    q = 1 - w if first else w
                    arrived(rdn, (w, k - 2, h, q), ("rs", d, k - 1, h), q=q)
                    pdn[slot + w, h, q] = (
                        pf[k - 2, w, h, q] + rdn[w, k - 2, h, q].astype(F32)
                    ).astype(BF16)
                    send(pdn, (slot + w, h, q), rdn, (w, k - 1, h, q), ("rs", d, k, h), dev[d], q=q)

    def rs_own():
        def body(h, c):
            part = dot(wgu[z, :, 0:GU], dgu[0:GU, :], 1, 0).reshape(NXL, W, T)
            for hh in range(H):
                pown[hh] = part[:, :, hh * TH : (hh + 1) * TH]
            return c

        lax.fori_loop(0, 1, body, 0)

    def rs_last(h):
        for q in (ol, xl):
            for d, w in ways:
                arrived(rdn, (w, 3, h, q), ("rs", d, 4, h), q=q)
            if q is ol:
                xs[h] = (
                    pown[h, q] + rdn[0, 3, h, q].astype(F32) + rdn[1, 3, h, q].astype(F32)
                ).astype(BF16)
                send(xs, (h,), xr, (h,), ("rx", h), dev["xl"])

    def take_stat():
        nstat[...] = collect(stat_in, tp_peers, "stat") / D

    def dx_part(h):
        arrived(xr, (h,), ("rx", h))
        cols = slice(h * TH, (h + 1) * TH)
        d_normed = (
            pown[h, xl]
            + rdn[0, 3, h, xl].astype(F32)
            + rdn[1, 3, h, xl].astype(F32)
            + xr[h].astype(F32)
        )
        u = unit[:, cols]
        dx = dy_all[z, xl, h].astype(F32) + scale[:, cols] * (
            d_normed * gain[:, 0:1] - u * nstat[:, cols]
        )
        dxs[h] = dx.astype(BF16)
        gx[h] = d_normed * u

    def dx_send(h):
        dx_part(h)
        for d, name in (
            ("xl", ("xl", h)),
            ("z+", ("z+", 1, 0, h)),
            ("z-", ("z-", 1, 0, h)),
            ("core", ("core", h)),
        ):
            send(dxs, (h,), dy_all, (z, xl, h), ("e", *name), across[d])

    def gain_dx():
        total = dot(
            jnp.ones((8, T), F32),
            jnp.concatenate([gx[h] for h in range(H)], axis=1),
            1,
            1,
            lax.Precision.HIGHEST,
        )
        gain_in[f] = total
        spread(gain_in, f, fs_peers, "gain")
        for h in range(H):
            dx_ref[h * TH : (h + 1) * TH, :] = dot(dxs[h], eye, 0, 0).astype(BF16)

    sg, rg, fg = {"u": sgu, "d": sgd}, {"u": rgu, "d": rgd}, {"u": fgu, "d": fgd}
    size_of = {"u": (PW, 32), "d": (DR, 48)}

    def wgrad(a, blk, dst, i):
        dy = act(dy_all, blk)
        if a == "u":
            cut = UW - 128
            n = n_all[blk].reshape(PW, T)
            dst[i, :, 0:cut] = dot(n, dgu[0:cut, :], 1, 1).astype(dst.dtype)
            edge = dot(n, dgu[cut:UW, :], 1, 1) + dot(dy, hid_mid[...], 1, 1)
            dst[i, :, cut:UW] = edge.astype(dst.dtype)
        else:
            dst[i, 0:PW, :] = dot(dy, hid[0:DH, :], 1, 1).astype(dst.dtype)
            dst[i, PW:DR, 0:PW] = dot(hid[FL - 16 : FL, :], dy, 1, 1).astype(dst.dtype)

    direct = [right["o"], left["o"], far["o"]]
    kept = [far["c"], own["o"], right["c"], left["c"], own["c"]]

    def g_first(a, lo=0, hi=3):
        rm = ident(("g", a, 0), 3)
        sm = [take(sg[a], (0,), "big") if lo <= i < hi else 0 for i in range(3)]

        def body(i, c):
            wgrad(a, pick(i, direct), sg[a], i)
            to = pick(i, [dev[d][1] for d in ("y+", "y-", "xh")])
            copy(sg[a].at[i], rg[a].at[i], pick(i, sm), rm + i, (s, to, t)).start()
            return c

        lax.fori_loop(lo, hi, body, 0)

    def g_kept(a, lo, hi):
        def body(i, c):
            wgrad(a, pick(i, kept), fg[a], i)
            return c

        lax.fori_loop(lo, hi, body, 0)

    def g_sum(a, slot, own_i, recv, span=None):
        n, st = size_of[a]
        lo, n = span if span else (0, n)
        st = 16 if span else st

        def body(r):
            r = pl.multiple_of(r + lo, 16)
            v = fg[a][own_i, pl.ds(r, st), :]
            for k in recv:
                v = v + rg[a][k, pl.ds(r, st), :].astype(F32)
            sg[a][slot, pl.ds(r, st), :] = v.astype(BF16)

        rows(n, st, body)

    def g_far(a):
        arrived(rg[a], (2,), ("g", a, 0), q=2)
        g_sum(a, 3, 0, (2,))
        for d, k in (("y+", 0), ("y-", 1)):
            part = pl.ds(*halves[a][k])
            send(sg[a], (3, part), rg[a], (3, part), ("g", a, 3, d), dev[d], kind="big")

    def g_near(a, waits):
        for d, k, slot in (("y+", 0, 4), ("y-", 1, 5)):
            half = halves[a][k if waits else 1 - k]
            part = pl.ds(*half)
            if waits:
                arrived(rg[a], (3, part), ("g", a, 3, d))
            g_sum(a, slot, 2 + k, (3,) if waits else (), half)
            send(sg[a], (slot, part), rg[a], (slot, part), ("g", a, slot, waits), dev[d], kind="big")

    def g_partner(a):
        arrived(rg[a], (0,), ("g", a, 0), q=0)
        arrived(rg[a], (1,), ("g", a, 0), q=1)
        g_sum(a, 6, 1, (0, 1))
        send(sg[a], (6,), rg[a], (6,), ("g", a, 6), dev["xh"], kind="big")

    def g_most(a):
        for k in (0, 1):
            part = pl.ds(*halves[a][1 - k])
            arrived(rg[a], (4 + k, part), ("g", a, 4 + k, False))
        arrived(rg[a], (6,), ("g", a, 6))
        for k in (0, 1):
            lo, n = halves[a][1 - k]

            def body(r, k=k, lo=lo):
                at = pl.ds(pl.multiple_of(r + lo, 16), 16)
                fg[a][4, at, :] += rg[a][4 + k, at, :].astype(F32) + rg[a][6, at, :].astype(F32)

            rows(n, 16, body)

    def g_last(a):
        for k in (0, 1):
            lo, n = halves[a][k]
            arrived(rg[a], (4 + k, pl.ds(lo, n)), ("g", a, 4 + k, True))

            def total(at, k=k):
                return fg[a][4, at, :] + rg[a][4 + k, at, :].astype(F32)

            def body(r, total=total, lo=lo):
                at = pl.ds(pl.multiple_of(r + lo, 16), 32)
                v = total(at)
                if a == "u":
                    gg_ref[at, :] = v[:, 0:FL]
                    ug_ref[at, :] = v[:, FL:GU]
                    dg_ref[at, DH : DH + 32] = v[:, GU:UW]
                else:
                    dg_ref[at, 0:DH] = v

            rows(160, 32, body)
            if n > 160:
                v = total(pl.ds(PW, 16))[:, 0:PW]
                unit16 = (
                    lax.broadcasted_iota(jnp.int32, (16, 16), 0)
                    == lax.broadcasted_iota(jnp.int32, (16, 16), 1)
                ).astype(F32)
                dg_ref[:, DH + 32 : FL] = dot(v, unit16, 0, 0, lax.Precision.HIGHEST)

    def finish():
        gn_ref[...] = collect(gain_in, fs_peers, "gain")[0:1]
        left_all()

    @pl.when(s == 1)
    def _():
        ctx[0] = 1
        ag_own(dy_all, "dy")
        ag_own(x_all, "n")
        w_own("d", ("y+", "y-", "xh"))
        w_own("u", ("y+", "y-", "xh"))
        take_gain()
        ag_partner(dy_all, "dy")
        ag_fwd(dy_all, "dy", 1, 0)
        normalize()
        ag_partner(x_all, "n")
        ag_fwd(x_all, "n", 1, 0)
        w_fwd("d")
        ag_fwd(dy_all, "dy", 1, 1)
        ag_fwd(dy_all, "dy", 2, 0)
        w_fwd("u")
        w_pass("d")
        ag_fwd(x_all, "n", 1, 1)
        ag_fwd(x_all, "n", 2, 0)
        w_far("d")
        norm_blocks(0, 1, 7)
        ag_fwd(dy_all, "dy", 2, 1)
        w_pass("u")
        w_far("u")
        ag_fwd(x_all, "n", 2, 1)
        norm_blocks(2, 6)
        ag_fwd3(dy_all, "dy")
        w_last("d")
        dhidden(0, 1, 7)
        ag_fwd3(x_all, "n")
        pl.semaphore_signal(go, inc=1, device_id=dev["core"], device_id_type=MESH)
        norm_blocks(3, 5)
        dhidden(2, 6, 3, 5)
        w_last("u")
        forward(0, 1, 7)
        pl.semaphore_signal(go, inc=1, device_id=dev["core"], device_id_type=MESH)
        ag_last(dy_all, "dy")
        dhidden(4)
        dhidden_mid()
        ag_last(x_all, "n")
        norm_blocks(4)
        forward(2, 6, 3, 5, 4)
        cotangents()
        rs_first()
        rs_compute(2)
        rs_free()
        rs_step(2, (False,), (0,))
        hidden()
        rs_compute(3)
        rs_step(2, (False,), (1,))
        left_all("big")
        g_first("u", 0, 1)
        rs_step(3, (True,), (0,))
        rs_step(3, (True,), (1,))
        rs_step(3, (False,), (0,))
        rs_compute(4)
        rs_step(3, (False,), (1,))
        g_first("u", 1, 2)
        rs_step(4, (True,), (0,))
        rs_own()
        rs_step(4, (False,), (0,))
        rs_step(4, (False,), (1,))
        g_kept("d", 0, 1)
        rs_step(4, (True,), (1,))
        rs_last(0)
        g_first("d", 1, 2)
        g_kept("d", 1, 2)
        rs_last(1)
        pl.semaphore_signal(go, inc=1, device_id=dev["core"], device_id_type=MESH)
        g_first("d", 0, 1)
        take_stat()
        dx_send(0)
        dx_send(1)
        g_first("u", 2, 3)
        g_kept("u", 1, 2)
        g_kept("u", 0, 1)
        g_first("d", 2, 3)
        g_kept("u", 2, 4)
        g_near("u", False)
        gain_dx()
        g_partner("u")
        g_kept("d", 4, 5)
        g_kept("d", 2, 4)
        g_near("d", False)
        g_far("u")
        g_partner("d")
        g_kept("u", 4, 5)
        g_far("d")
        g_near("u", True)
        g_near("d", True)
        g_most("u")
        g_last("u")
        g_most("d")
        g_last("d")
        finish()
        ctx[0] = None

    @pl.when(s == 0)
    def _():
        ctx[0] = 0
        take_gain()
        normalize()
        norm_own()
        pl.semaphore_wait(go, 1)
        ag_xl(n_all, "m")
        w_own("d", ("y+", "y-", "xh"))
        w_own("u", ("y+", "y-", "xh"))
        pl.semaphore_wait(go, 1)
        ag_z(n_all, "m")
        ag_partner(n_all, "m")
        w_fwd("d")
        own_wait(n_all, "m", 1)
        z_send(n_all, "m", 1, 0)
        w_fwd("u")
        w_pass("d")
        own_wait(n_all, "m", 2)
        pair_send(n_all, "m", 2, 6)
        w_far("d")
        w_pass("u")
        w_far("u")
        pl.semaphore_wait(go, 1)
        z_send(n_all, "m", 2, 0)
        pair_wait(n_all, "m", 2, 6)
        z_send(n_all, "m", 2, 1)
        for h in range(H):
            ag_partner(dy_all, "e", (h,))
        ag_fwd3(n_all, "m")
        for h in range(H):
            for j in range(2):
                ag_fwd(dy_all, "e", 1, j, (h,))
        w_last("d")
        w_last("u")
        arrived(n_all, (zblk[7], ol), ("m", "z+", 1, 1))
        arrived(n_all, (zblk[1], ol), ("m", "z-", 1, 1))
        forward(0, 1, 7)
        for h in range(H):
            for j in range(2):
                ag_fwd(dy_all, "e", 2, j, (h,))
        forward(2, 6, 3, 5)
        for h in range(H):
            arrived(dy_all, (z, xl, h), ("e", "core", h))
        dhidden(0, 1, 7)
        for h in range(H):
            ag_fwd3(dy_all, "e", (h,))
        ag_last(n_all, "m")
        forward(4)
        hidden()
        dhidden(2, 6, 3, 5)
        for h in range(H):
            ag_last(dy_all, "e", (h,))
        dhidden(4)
        dhidden_mid()
        cotangents()
        left_all("big")
        g_first("u", 0, 2)
        rs_first()
        g_first("u", 2, 3)
        rs_compute(2)
        rs_free()
        g_kept("u", 2, 4)
        g_near("u", False)
        g_first("d", 1, 2)
        rs_step(2, (False,), (0,))
        g_kept("u", 1, 2)
        rs_step(2, (False,), (1,))
        rs_compute(3)
        rs_step(3, (True,), (0,))
        g_first("d", 2, 3)
        g_first("d", 0, 1)
        rs_step(3, (True,), (1,))
        rs_compute(4)
        rs_step(3, (False,), (0,))
        rs_own()
        rs_step(3, (False,), (1,))
        g_partner("u")
        rs_step(4, (True,), (0,))
        g_kept("u", 0, 1)
        g_far("u")
        rs_step(4, (True,), (1,))
        g_kept("d", 0, 1)
        rs_step(4, (False,), (0,))
        g_kept("d", 4, 5)
        g_far("d")
        rs_step(4, (False,), (1,))
        g_kept("d", 1, 2)
        g_kept("d", 2, 4)
        g_near("d", False)
        rs_last(0)
        rs_last(1)
        g_partner("d")
        g_kept("u", 4, 5)
        g_near("u", True)
        g_near("d", True)
        take_stat()
        dx_part(0)
        g_most("u")
        dx_part(1)
        gain_dx()
        g_last("u")
        g_most("d")
        g_last("d")
        finish()
        ctx[0] = None

    spread_left(ssq_in, tp_peers, "ssq")
    spread_left(stat_in, tp_peers, "stat")
    spread_left(gain_in, fs_peers, "gain")


def put_kernel(*refs):
    copies = [pltpu.make_async_copy(refs[k], refs[5 + k], refs[10].at[k]) for k in range(5)]
    for c in copies:
        c.start()
    for c in copies:
        c.wait()


def body(saved_inputs, top_grad, norm_gain, gate_weight, up_weight, down_weight):
    x = saved_inputs.reshape(T, W)
    tg = top_grad.reshape(T, W)
    hbm = pl.BlockSpec(memory_space=pl.ANY)
    outs = (
        jax.ShapeDtypeStruct((T, W), BF16),
        jax.ShapeDtypeStruct((PW, FL), F32),
        jax.ShapeDtypeStruct((PW, FL), F32),
        jax.ShapeDtypeStruct((PW, FL), F32),
        jax.ShapeDtypeStruct((1, W), F32),
    )
    out = pl.pallas_call(
        fused_kernel,
        name="fused",
        out_shape=[pltpu.VMEM(o.shape, o.dtype) for o in outs],
        in_specs=[hbm] * 6,
        out_specs=[pl.BlockSpec(memory_space=pltpu.VMEM)] * 5,
        scratch_shapes=[
            pltpu.VMEM((T, W), BF16),
            pltpu.VMEM((T, W), BF16),
            pltpu.VMEM((1, D), F32),
            pltpu.VMEM((PW, FL), BF16),
            pltpu.VMEM((PW, FL), BF16),
            pltpu.VMEM((PW, FL), BF16),
            pltpu.VMEM((W, 128), F32),
            pltpu.VMEM((128, 128), F32),
            pltpu.VMEM((D, 128), F32),
            pltpu.VMEM((NZ, NXL, W, T), BF16),
            pltpu.VMEM((NF, PW, UW), BF16),
            pltpu.VMEM((NF, DR, DH), BF16),
            pltpu.VMEM((NZ, NXL, W, T), BF16),
            pltpu.VMEM((NZ, NXL, H, W, TH), BF16),
            pltpu.VMEM((UW, T), F32),
            pltpu.VMEM((DH + 128 + 16, T), F32),
            pltpu.VMEM((UW, T), BF16),
            pltpu.VMEM((FL, T), BF16),
            pltpu.VMEM((128, T), BF16),
            pltpu.VMEM((W, T), F32),
            pltpu.VMEM((1, T), F32),
            pltpu.VMEM((8, T), F32),
            pltpu.VMEM((NT, 1, T), F32),
            pltpu.VMEM((NT, 1, T), F32),
            pltpu.VMEM((NF, 8, W), F32),
            pltpu.VMEM((7, H, NXL, W, TH), BF16),
            pltpu.VMEM((2, 4, H, NXL, W, TH), BF16),
            pltpu.VMEM((3, 2, H, NXL, W, TH), F32),
            pltpu.VMEM((H, NXL, W, TH), F32),
            pltpu.VMEM((H, W, TH), F32),
            pltpu.VMEM((1, T), F32),
            pltpu.VMEM((H, W, TH), BF16),
            pltpu.VMEM((H, W, TH), BF16),
            pltpu.VMEM((H, W, TH), BF16),
            pltpu.VMEM((7, PW, UW), BF16),
            pltpu.VMEM((7, PW, UW), BF16),
            pltpu.VMEM((5, PW, UW), F32),
            pltpu.VMEM((7, DR, DH), BF16),
            pltpu.VMEM((7, DR, DH), BF16),
            pltpu.VMEM((5, DR, DH), F32),
            pltpu.SemaphoreType.DMA((NBIG + NSMALL + 3,)),
            pltpu.SemaphoreType.DMA((NCOMMON + NEACH,)),
            pltpu.SemaphoreType.DMA((6,)),
            pltpu.SemaphoreType.REGULAR,
        ],
        compiler_params=pltpu.CompilerParams(
            collective_id=0, has_side_effects=True, vmem_limit_bytes=58 * 2**20
        ),
    )(x, tg, norm_gain, gate_weight[0], up_weight[0], down_weight[0].T)
    dx, gg, ug, dg, gn = pl.pallas_call(
        put_kernel,
        name="put",
        out_shape=outs,
        in_specs=[pl.BlockSpec(memory_space=pltpu.VMEM)] * 5,
        out_specs=[hbm] * 5,
        scratch_shapes=[pltpu.SemaphoreType.DMA((5,))],
    )(*[pltpu.with_memory_space_constraint(o, pltpu.VMEM) for o in out])
    return (dx.reshape(1, MICRO, ROWS, W), gg[None], ug[None], dg.T[None], gn)


def solution(mesh):
    return jax.shard_map(
        body,
        mesh=mesh,
        in_specs=(
            P("section", None, "fsdp", "tp"),
            P(None, "fsdp", "tp"),
            P("section", None),
            P("section", "fsdp", "tp"),
            P("section", "fsdp", "tp"),
            P("section", "tp", "fsdp"),
        ),
        out_specs=(
            P("section", None, "fsdp", "tp"),
            P("section", "fsdp", "tp"),
            P("section", "fsdp", "tp"),
            P("section", "tp", "fsdp"),
            P("section", "tp"),
        ),
        check_vma=False,
    )
```

```python
import jax
import jax.numpy as jnp
from jax import lax
from jax.experimental import pallas as pl
from jax.experimental.pallas import tpu as pltpu
from jax.sharding import PartitionSpec as P

EPS = 1e-05
MESH = pl.DeviceIdType.MESH
F32 = jnp.float32
BF16 = jnp.bfloat16

NY, NXH, NZ, NXL = 4, 2, 8, 2
NF, NT = NY * NXH, NZ * NXL
MICRO = 8
ROWS = 64
T = MICRO * ROWS
H = 2
TH = T // H
W = 160
PW = NXL * W
FL = 432
GU = 2 * FL
D = W * NT
UW = 896
DH = 384
DR = PW + 16
NCOMMON = 79
NEACH = 48
NBIG = 16
NSMALL = 20


def dot(a, b, ca, cb, precision=None):
    return lax.dot_general(
        a, b, (((ca,), (cb,)), ((), ())), preferred_element_type=F32, precision=precision
    )


def fused_kernel(
    x_hbm,
    tg_hbm,
    gain_hbm,
    wg_hbm,
    wu_hbm,
    wd_hbm,
    dx_ref,
    gg_ref,
    ug_ref,
    dg_ref,
    gn_ref,
    x_ref,
    tg_ref,
    gain_row,
    wg_ref,
    wu_ref,
    wd_ref,
    gain,
    gain_sq,
    gain_all,
    x_all,
    wgu,
    wd,
    n_all,
    dy_all,
    gu,
    dh,
    dgu,
    hid,
    hid_mid,
    unit,
    scale,
    stat,
    ssq_in,
    stat_in,
    gain_in,
    pdn,
    rdn,
    pf,
    pown,
    gx,
    nstat,
    xs,
    xr,
    dxs,
    sgu,
    rgu,
    fgu,
    sgd,
    rgd,
    fgd,
    ssem,
    rsem,
    lsem,
    go,
):
    s = lax.axis_index("section")
    f = lax.axis_index("fsdp")
    t = lax.axis_index("tp")
    y, xh = lax.div(f, NXH), lax.rem(f, NXH)
    z, xl = lax.div(t, NXL), lax.rem(t, NXL)
    oh, ol = 1 - xh, 1 - xl

    def at_y(step):
        return (s, lax.rem(y + step + NY, NY) * NXH + xh, t)

    def at_z(step):
        return (s, f, lax.rem(z + step + NZ, NZ) * NXL + xl)

    dev = {
        "y+": at_y(1),
        "y-": at_y(-1),
        "z+": at_z(1),
        "z-": at_z(-1),
        "xh": (s, y * NXH + oh, t),
        "xl": (s, f, z * NXL + ol),
        "core": (1 - s, f, t),
    }
    across = {
        "core": (1 - s, f, t),
        "xl": (1 - s, *dev["xl"][1:]),
        "z+": (1 - s, *dev["z+"][1:]),
        "z-": (1 - s, *dev["z-"][1:]),
    }
    tp_peers = [(s, f, lax.rem(t + k, NT)) for k in range(1, NT)]
    fs_peers = [(s, lax.rem(f + k, NF), t) for k in range(1, NF)]
    zblk = [lax.rem(z + k, NZ) for k in range(NZ)]
    own, left, right, far = (
        {"c": lax.rem(y + k, NY) * NXH + xh, "o": lax.rem(y + k, NY) * NXH + oh} for k in (0, 3, 1, 2)
    )

    ids = {}
    size = {None: 0, 0: 0, 1: 0}
    private = {"dy": 1, "n": 1, "m": 0, "e": 0}
    ctx = [None]

    def ident(name, n=1):
        if name not in ids:
            sec = private.get(name[0])
            ids[name] = size[sec] + (0 if sec is None else NCOMMON)
            size[sec] += n
            assert size[sec] <= (NCOMMON if sec is None else NEACH), size
        return ids[name]

    def copy(src, dst, sm, rm, to):
        return pltpu.make_async_remote_copy(
            src_ref=src,
            dst_ref=dst,
            send_sem=ssem.at[sm],
            recv_sem=rsem.at[rm],
            device_id=to,
            device_id_type=MESH,
        )

    def static(idx):
        return tuple(i if isinstance(i, (int, pl.Slice)) else 0 for i in idx)

    turn = {sec: {"big": 0, "small": 0} for sec in (0, 1)}
    flying = {0: {}, 1: {}}

    def left_all(kind=None):
        mine = flying[ctx[0]]
        for m in sorted(mine):
            if kind is None or (m < NBIG) == (kind == "big"):
                src, si = mine.pop(m)
                r = src.at[si]
                copy(r, r, m, 0, dev["core"]).wait_send()

    def take(src, si, kind):
        mine, sec = flying[ctx[0]], ctx[0]
        base, n = (0, NBIG) if kind == "big" else (NBIG, NSMALL)
        m = base + turn[sec][kind] % n
        turn[sec][kind] += 1
        if m in mine:
            was, wi = mine.pop(m)
            r = was.at[wi]
            copy(r, r, m, 0, dev["core"]).wait_send()
        mine[m] = (src, static(si))
        return m

    def send(src, si, dst, di, name, to, q=None, kind="small"):
        rm = ident(name, 1 if q is None else 2)
        sm = take(src, si, kind)
        copy(src.at[si], dst.at[di], sm, rm if q is None else rm + q, to).start()

    def arrived(dst, di, name, q=None):
        m = ident(name, 1 if q is None else 2)
        r = dst.at[di]
        copy(r, r, 0, m if q is None else m + q, dev["core"]).wait_recv()

    def rows(n, step, fn):
        def body(i, c):
            fn(pl.multiple_of(i * step, step))
            return c

        lax.fori_loop(0, n // step, body, 0)

    barrier = pltpu.get_barrier_semaphore()
    everyone = tp_peers[4:11] + tp_peers[:4] + tp_peers[11:] + fs_peers + list(across.values())
    for to in everyone:
        pl.semaphore_signal(barrier, inc=1, device_id=to, device_id_type=MESH)

    loads = [
        pltpu.make_async_copy(src, dst, lsem.at[k])
        for k, (src, dst) in enumerate(
            (
                (x_hbm, x_ref),
                (tg_hbm, tg_ref),
                (gain_hbm, gain_row),
                (wd_hbm, wd_ref),
                (wg_hbm, wg_ref),
                (wu_hbm, wu_ref),
            )
        )
    ]
    for c in loads:
        c.start()
    eye = (
        lax.broadcasted_iota(jnp.int32, (W, W), 0) == lax.broadcasted_iota(jnp.int32, (W, W), 1)
    ).astype(BF16)
    loads[0].wait()
    xt = dot(eye, x_ref[...], 1, 1)
    ssq_in[t] = jnp.sum(xt * xt, axis=0, keepdims=True)
    unit[...] = xt
    loads[1].wait()

    @pl.when(s == 1)
    def _():
        x_all[z, xl] = xt.astype(BF16)
        top = dot(eye, tg_ref[...], 1, 1).astype(BF16)
        for h in range(H):
            dy_all[z, xl, h] = top[:, h * TH : (h + 1) * TH]

    def pack_d():
        loads[3].wait()

        def pack(r):
            wd[f, pl.ds(r, 32), :] = wd_ref[pl.ds(r, 32), 0:DH]
            wgu[f, pl.ds(r, 32), GU:UW] = wd_ref[pl.ds(r, 32), DH : DH + 32]

        rows(PW, 32, pack)
        last = (
            lax.broadcasted_iota(jnp.int32, (16, FL), 0) + (FL - 16)
            == lax.broadcasted_iota(jnp.int32, (16, FL), 1)
        ).astype(BF16)
        wd[f, PW:DR, 0:PW] = dot(last, wd_ref[...], 1, 1).astype(BF16)

    def pack_u():
        loads[4].wait()
        loads[5].wait()

        def pack(r):
            wgu[f, pl.ds(r, 32), 0:FL] = wg_ref[pl.ds(r, 32), :]
            wgu[f, pl.ds(r, 32), FL:GU] = wu_ref[pl.ds(r, 32), :]

        rows(PW, 32, pack)

    def take_gain():
        loads[2].wait()
        gain_sq[...] = jnp.zeros_like(gain_sq)
        for c in range(D // 128):
            gain_sq[c : c + 1, :] = gain_row[:, c * 128 : (c + 1) * 128]
        cols = gain_sq[...].T
        for c in range(D // 128):
            gain_all[c * 128 : (c + 1) * 128, :] = jnp.broadcast_to(cols[:, c : c + 1], (128, 128))
        gain[...] = gain_all[pl.ds(pl.multiple_of(t * W, 8), W), :]

    def spread(buf, me, peers, name):
        m = ident((name,))
        for to in peers:
            copy(buf.at[me], buf.at[me], NBIG + NSMALL + ("ssq", "stat", "gain").index(name), m, to).start()

    def collect(buf, peers, name):
        n = len(peers)
        r = buf.at[pl.ds(0, n)]
        copy(r, r, 0, ident((name,)), dev["core"]).wait_recv()
        total = buf[0]
        for k in range(1, n + 1):
            total = total + buf[k]
        return total

    def spread_left(buf, peers, name):
        r = buf.at[pl.ds(0, len(peers))]
        copy(r, r, NBIG + NSMALL + ("ssq", "stat", "gain").index(name), 0, dev["core"]).wait_send()

    pack_d()
    pack_u()

    pl.semaphore_wait(barrier, len(everyone))
    spread(ssq_in, t, tp_peers, "ssq")

    halves = {"u": ((0, 160), (160, 160)), "d": ((0, 160), (160, 176))}
    full = {"u": wgu, "d": wd}

    def w_own_x(a):
        send(full[a], (f,), full[a], (f,), ("w", a, "own", "xh"), dev["xh"], kind="big")

    def w_own_y(a, *parts):
        for i in parts:
            for d, k in (("y+", i), ("y-", 1 - i)):
                at = (f, pl.ds(*halves[a][k]))
                send(full[a], at, full[a], at, ("w", a, "own", d, i), dev[d], kind="big")

    def w_fwd(a):
        arr = full[a]
        for d, blk, k in (("y+", left["c"], 0), ("y-", right["c"], 1)):
            at = (blk, pl.ds(*halves[a][k]))
            arrived(arr, at, ("w", a, "own", d, 0))
            send(arr, at, arr, at, ("w", a, "fwd", d), dev[d], kind="big")

    def w_pass(a):
        arr, blk = full[a], own["o"]
        arrived(arr, (blk,), ("w", a, "own", "xh"))
        for d in ("y+", "y-"):
            send(arr, (blk,), arr, (blk,), ("w", a, "pass", d), dev[d], kind="big")

    def w_far(a):
        arr, blk = full[a], far["c"]
        for d, k in (("y+", 0), ("y-", 1)):
            arrived(arr, (blk, pl.ds(*halves[a][k])), ("w", a, "fwd", d))
        send(arr, (blk,), arr, (blk,), ("w", a, "far"), dev["xh"], kind="big")

    def w_last(a):
        arr = full[a]
        arrived(arr, (left["o"],), ("w", a, "pass", "y+"))
        arrived(arr, (right["o"],), ("w", a, "pass", "y-"))
        arrived(arr, (far["o"],), ("w", a, "far"))
        for d, blk, k in (("y+", left["c"], 1), ("y-", right["c"], 0)):
            arrived(arr, (blk, pl.ds(*halves[a][k])), ("w", a, "own", d, 1))

    def ag_xl(buf, nm):
        send(buf, (z, xl), buf, (z, xl), (nm, "xl"), dev["xl"])

    def ag_z(buf, nm):
        for d in ("z+", "z-"):
            send(buf, (z, xl), buf, (z, xl), (nm, d, 1, 0), dev[d])

    def ag_own(buf, nm):
        ag_xl(buf, nm)
        ag_z(buf, nm)

    def ag_partner(buf, nm, hh=()):
        at = (z, ol, *hh)
        arrived(buf, at, (nm, "xl", *hh))
        send(buf, at, buf, at, (nm, "z+", 1, 1, *hh), dev["z+"])
        send(buf, at, buf, at, (nm, "z-", 1, 1, *hh), dev["z-"])

    def ag_fwd(buf, nm, k, j, hh=()):
        q = (xl, ol)[j]
        for d, blk in (("z+", zblk[NZ - k]), ("z-", zblk[k])):
            at = (blk, q, *hh)
            arrived(buf, at, (nm, d, k, j, *hh))
            send(buf, at, buf, at, (nm, d, k + 1, j, *hh), dev[d])

    def ag_fwd3(buf, nm, hh=()):
        for d, blk, q in (("z+", zblk[5], 0), ("z-", zblk[3], 1)):
            for j in range(2):
                arrived(buf, (blk, (xl, ol)[j], *hh), (nm, d, 3, j, *hh))
            send(buf, (blk, q, *hh), buf, (blk, q, *hh), (nm, d, 4, *hh), dev[d])

    def ag_last(buf, nm, hh=()):
        arrived(buf, (zblk[4], 0, *hh), (nm, "z+", 4, *hh))
        arrived(buf, (zblk[4], 1, *hh), (nm, "z-", 4, *hh))

    def pair_send(buf, nm, *ks):
        for k in ks:
            at = (zblk[k], xl)
            send(buf, at, buf, at, (nm, "pair", k), dev["xl"])

    def pair_wait(buf, nm, *ks):
        for k in ks:
            arrived(buf, (zblk[k], ol), (nm, "pair", k))

    def own_wait(buf, nm, k):
        for d, b in (("z+", zblk[NZ - k]), ("z-", zblk[k])):
            arrived(buf, (b, xl), (nm, d, k, 0))

    def z_send(buf, nm, k, j):
        for d, b in (("z+", zblk[NZ - k]), ("z-", zblk[k])):
            at = (b, (xl, ol)[j])
            send(buf, at, buf, at, (nm, d, k + 1, j), dev[d])

    def act(buf, i):
        return jnp.concatenate([buf[i, :, h].reshape(PW, TH) for h in range(H)], axis=1)

    def pick(i, table):
        v = table[0]
        for k in range(1, len(table)):
            v = jnp.where(i == k, table[k], v)
        return v

    def together(parts):
        return jnp.concatenate(parts, axis=0)

    def forward(*ks):
        blks = [zblk[k] for k in ks]
        part = dot(
            together([wgu[b] for b in blks]),
            together([n_all[b].reshape(PW, T) for b in blks]),
            0,
            0,
        )
        gu[...] = part if 0 in ks else gu[...] + part

    def dhidden(*ks):
        blks = [zblk[k] for k in ks]
        dys = [act(dy_all, b) for b in blks]
        dy = together(dys)
        parts = (
            (0, dot(together([wd[b, 0:PW] for b in blks]), dy, 0, 0)),
        )
        for r, part in parts:
            at = pl.ds(r, part.shape[0])
            dh[at, :] = part if 0 in ks else dh[at, :] + part
        part = dot(wd[blks[0], PW:DR, 0:PW], dys[0], 1, 0)
        for b, d in zip(blks[1:], dys[1:]):
            part = part + dot(wd[b, PW:DR, 0:PW], d, 1, 0)
        at = pl.ds(DH + 128, 16)
        dh[at, :] = part if 0 in ks else dh[at, :] + part

    def dhidden_mid():
        lhs = together([wgu[b, :, UW - 128 : UW] for b in range(NF)])
        dh[DH : DH + 128, :] = dot(lhs, together([act(dy_all, b) for b in range(NF)]), 0, 0)

    def hidden():
        def body(r):
            gate = gu[pl.ds(r, 16), :]
            up = gu[pl.ds(pl.multiple_of(FL + r, 16), 16), :]
            hid[pl.ds(r, 16), :] = (gate * jax.nn.sigmoid(gate) * up).astype(BF16)

        rows(FL, 48, lambda r: [body(pl.multiple_of(r + k, 16)) for k in (0, 16, 32)])
        hid_mid[0:96, :] = jnp.zeros((96, T), BF16)
        hid_mid[96:128, :] = hid[DH : DH + 32, :]

    def normalize():
        row_scale = lax.rsqrt(collect(ssq_in, tp_peers, "ssq") / D + EPS)
        scale[...] = row_scale
        unit[...] = unit[...] * row_scale

    def norm_own():
        n_all[z, xl] = (unit[...] * gain[:, 0:1]).astype(BF16)

    def norm_blocks(*ks):
        for k in ks:
            b = zblk[k]
            for q in range(NXL):
                g = gain_all[pl.ds(pl.multiple_of(b * PW + q * W, 8), W), :]
                for c in range(T // 128):
                    at = slice(c * 128, (c + 1) * 128)
                    n_all[b, q, :, at] = (
                        x_all[b, q, :, at].astype(F32) * scale[:, at] * g
                    ).astype(BF16)

    def cotangents():
        stat[...] = jnp.zeros_like(stat)
        dgu[GU:UW, :] = jnp.zeros((UW - GU, T), BF16)

        def elementwise(r):
            gate = gu[pl.ds(r, 16), :]
            up = gu[pl.ds(pl.multiple_of(FL + r, 16), 16), :]
            dd = dh[pl.ds(pl.multiple_of(jnp.where(r < DH, r, r + 96), 16), 16), :]
            sig = jax.nn.sigmoid(gate)
            silu = gate * sig
            d_gate = (dd * up * sig * (1.0 + gate * (1.0 - sig))).astype(BF16)
            d_up = (dd * silu).astype(BF16)
            dgu[pl.ds(r, 16), :] = d_gate
            dgu[pl.ds(pl.multiple_of(FL + r, 16), 16), :] = d_up
            both = d_gate.astype(F32) * gate + d_up.astype(F32) * up
            stat[...] += both[0:8] + both[8:16]

        rows(FL, 48, lambda r: [elementwise(pl.multiple_of(r + k, 16)) for k in (0, 16, 32)])
        stat_in[t] = jnp.sum(stat[...], axis=0, keepdims=True)
        spread(stat_in, t, tp_peers, "stat")

    ways = (("z+", 0), ("z-", 1))

    def rs_first():
        def body(h, c):
            part = dot(wgu[zblk[4], :, 0:GU], dgu[0:GU, :], 1, 0).reshape(NXL, W, T)
            for hh in range(H):
                pdn[0, hh] = part[:, :, hh * TH : (hh + 1) * TH].astype(BF16)
            return c

        lax.fori_loop(0, 1, body, 0)
        for h in range(H):
            for d, w in ways:
                send(pdn, (0, h, w), rdn, (w, 0, h, w), ("rs", d, 1, h), dev[d], q=w)

    def rs_compute(k):
        def body(w, c):
            blk = jnp.where(w == 0, zblk[5 - k], zblk[3 + k])
            part = dot(wgu[blk, :, 0:GU], dgu[0:GU, :], 1, 0).reshape(NXL, W, T)
            for hh in range(H):
                pf[k - 2, w, hh] = part[:, :, hh * TH : (hh + 1) * TH]
            return c

        lax.fori_loop(0, 2, body, 0)

    def rs_free():
        for h in range(H):
            for d, w in ways:
                q = 1 - w
                pdn[1 + w, h, q] = pf[0, w, h, q].astype(BF16)
                send(pdn, (1 + w, h, q), rdn, (w, 1, h, q), ("rs", d, 2, h), dev[d], q=q)

    def rs_step(k, ahead=(True, False), hs=range(H)):
        slot = 2 * k - 3
        for first in ahead:
            for h in hs:
                for d, w in ways:
                    q = 1 - w if first else w
                    arrived(rdn, (w, k - 2, h, q), ("rs", d, k - 1, h), q=q)
                    pdn[slot + w, h, q] = (
                        pf[k - 2, w, h, q] + rdn[w, k - 2, h, q].astype(F32)
                    ).astype(BF16)
                    send(pdn, (slot + w, h, q), rdn, (w, k - 1, h, q), ("rs", d, k, h), dev[d], q=q)

    def rs_own():
        def body(h, c):
            part = dot(wgu[z, :, 0:GU], dgu[0:GU, :], 1, 0).reshape(NXL, W, T)
            for hh in range(H):
                pown[hh] = part[:, :, hh * TH : (hh + 1) * TH]
            return c

        lax.fori_loop(0, 1, body, 0)

    def rs_last(h):
        for q in (ol, xl):
            for d, w in ways:
                arrived(rdn, (w, 3, h, q), ("rs", d, 4, h), q=q)
            if q is ol:
                xs[h] = (
                    pown[h, q] + rdn[0, 3, h, q].astype(F32) + rdn[1, 3, h, q].astype(F32)
                ).astype(BF16)
                send(xs, (h,), xr, (h,), ("rx", h), dev["xl"])

    def take_stat():
        nstat[...] = collect(stat_in, tp_peers, "stat") / D

    def dx_part(h):
        arrived(xr, (h,), ("rx", h))
        cols = slice(h * TH, (h + 1) * TH)
        d_normed = (
            pown[h, xl]
            + rdn[0, 3, h, xl].astype(F32)
            + rdn[1, 3, h, xl].astype(F32)
            + xr[h].astype(F32)
        )
        u = unit[:, cols]
        dx = dy_all[z, xl, h].astype(F32) + scale[:, cols] * (
            d_normed * gain[:, 0:1] - u * nstat[:, cols]
        )
        dxs[h] = dx.astype(BF16)
        gx[h] = d_normed * u

    def dx_send(h):
        dx_part(h)
        for d, name in (
            ("xl", ("xl", h)),
            ("z+", ("z+", 1, 0, h)),
            ("z-", ("z-", 1, 0, h)),
            ("core", ("core", h)),
        ):
            send(dxs, (h,), dy_all, (z, xl, h), ("e", *name), across[d])

    def gain_dx():
        total = dot(
            jnp.ones((8, T), F32),
            jnp.concatenate([gx[h] for h in range(H)], axis=1),
            1,
            1,
            lax.Precision.HIGHEST,
        )
        gain_in[f] = total
        spread(gain_in, f, fs_peers, "gain")
        for h in range(H):
            dx_ref[h * TH : (h + 1) * TH, :] = dot(dxs[h], eye, 0, 0).astype(BF16)

    sg, rg, fg = {"u": sgu, "d": sgd}, {"u": rgu, "d": rgd}, {"u": fgu, "d": fgd}
    size_of = {"u": (PW, 32), "d": (DR, 48)}

    def wgrad(a, blk, dst, i):
        dy = act(dy_all, blk)
        if a == "u":
            cut = UW - 128
            n = n_all[blk].reshape(PW, T)
            dst[i, :, 0:cut] = dot(n, dgu[0:cut, :], 1, 1).astype(dst.dtype)
            edge = dot(n, dgu[cut:UW, :], 1, 1) + dot(dy, hid_mid[...], 1, 1)
            dst[i, :, cut:UW] = edge.astype(dst.dtype)
        else:
            dst[i, 0:PW, :] = dot(dy, hid[0:DH, :], 1, 1).astype(dst.dtype)
            dst[i, PW:DR, 0:PW] = dot(hid[FL - 16 : FL, :], dy, 1, 1).astype(dst.dtype)

    direct = [right["o"], left["o"], far["o"]]
    kept = [far["c"], own["o"], right["c"], left["c"], own["c"]]

    def g_first(a, lo=0, hi=3):
        rm = ident(("g", a, 0), 3)
        sm = [take(sg[a], (0,), "big") if lo <= i < hi else 0 for i in range(3)]

        def body(i, c):
            wgrad(a, pick(i, direct), sg[a], i)
            to = pick(i, [dev[d][1] for d in ("y+", "y-", "xh")])
            copy(sg[a].at[i], rg[a].at[i], pick(i, sm), rm + i, (s, to, t)).start()
            return c

        lax.fori_loop(lo, hi, body, 0)

    def g_kept(a, lo, hi):
        def body(i, c):
            wgrad(a, pick(i, kept), fg[a], i)
            return c

        lax.fori_loop(lo, hi, body, 0)

    def g_sum(a, slot, own_i, recv, span=None):
        n, st = size_of[a]
        lo, n = span if span else (0, n)
        st = 16 if span else st

        def body(r):
            r = pl.multiple_of(r + lo, 16)
            v = fg[a][own_i, pl.ds(r, st), :]
            for k in recv:
                v = v + rg[a][k, pl.ds(r, st), :].astype(F32)
            sg[a][slot, pl.ds(r, st), :] = v.astype(BF16)

        rows(n, st, body)

    def g_far(a):
        arrived(rg[a], (2,), ("g", a, 0), q=2)
        g_sum(a, 3, 0, (2,))
        for d, k in (("y+", 0), ("y-", 1)):
            part = pl.ds(*halves[a][k])
            send(sg[a], (3, part), rg[a], (3, part), ("g", a, 3, d), dev[d], kind="big")

    def g_near(a, waits):
        for d, k, slot in (("y+", 0, 4), ("y-", 1, 5)):
            half = halves[a][k if waits else 1 - k]
            part = pl.ds(*half)
            if waits:
                arrived(rg[a], (3, part), ("g", a, 3, d))
            g_sum(a, slot, 2 + k, (3,) if waits else (), half)
            send(sg[a], (slot, part), rg[a], (slot, part), ("g", a, slot, waits), dev[d], kind="big")

    def g_partner(a):
        arrived(rg[a], (0,), ("g", a, 0), q=0)
        arrived(rg[a], (1,), ("g", a, 0), q=1)
        g_sum(a, 6, 1, (0, 1))
        send(sg[a], (6,), rg[a], (6,), ("g", a, 6), dev["xh"], kind="big")

    def g_most(a):
        for k in (0, 1):
            part = pl.ds(*halves[a][1 - k])
            arrived(rg[a], (4 + k, part), ("g", a, 4 + k, False))
        arrived(rg[a], (6,), ("g", a, 6))
        for k in (0, 1):
            lo, n = halves[a][1 - k]

            def body(r, k=k, lo=lo):
                at = pl.ds(pl.multiple_of(r + lo, 16), 16)
                fg[a][4, at, :] += rg[a][4 + k, at, :].astype(F32) + rg[a][6, at, :].astype(F32)

            rows(n, 16, body)

    def g_last(a):
        for k in (0, 1):
            lo, n = halves[a][k]
            arrived(rg[a], (4 + k, pl.ds(lo, n)), ("g", a, 4 + k, True))

            def total(at, k=k):
                return fg[a][4, at, :] + rg[a][4 + k, at, :].astype(F32)

            def body(r, total=total, lo=lo):
                at = pl.ds(pl.multiple_of(r + lo, 16), 32)
                v = total(at)
                if a == "u":
                    gg_ref[at, :] = v[:, 0:FL]
                    ug_ref[at, :] = v[:, FL:GU]
                    dg_ref[at, DH : DH + 32] = v[:, GU:UW]
                else:
                    dg_ref[at, 0:DH] = v

            rows(160, 32, body)
            if n > 160:
                v = total(pl.ds(PW, 16))[:, 0:PW]
                unit16 = (
                    lax.broadcasted_iota(jnp.int32, (16, 16), 0)
                    == lax.broadcasted_iota(jnp.int32, (16, 16), 1)
                ).astype(F32)
                dg_ref[:, DH + 32 : FL] = dot(v, unit16, 0, 0, lax.Precision.HIGHEST)

    def finish():
        gn_ref[...] = collect(gain_in, fs_peers, "gain")[0:1]
        left_all()

    @pl.when(s == 1)
    def _():
        ctx[0] = 1
        ag_own(dy_all, "dy")
        ag_own(x_all, "n")
        w_own_x("d")
        w_own_y("d", 0, 1)
        w_own_y("u", 0, 1)
        w_own_x("u")
        take_gain()
        ag_partner(dy_all, "dy")
        ag_fwd(dy_all, "dy", 1, 0)
        normalize()
        ag_partner(x_all, "n")
        ag_fwd(x_all, "n", 1, 0)
        w_fwd("d")
        ag_fwd(dy_all, "dy", 1, 1)
        ag_fwd(dy_all, "dy", 2, 0)
        w_fwd("u")
        w_pass("d")
        ag_fwd(x_all, "n", 1, 1)
        ag_fwd(x_all, "n", 2, 0)
        w_far("d")
        norm_blocks(0, 1, 7)
        ag_fwd(dy_all, "dy", 2, 1)
        w_pass("u")
        w_far("u")
        ag_fwd(x_all, "n", 2, 1)
        norm_blocks(2, 6)
        ag_fwd3(dy_all, "dy")
        w_last("d")
        dhidden(0, 1, 7)
        ag_fwd3(x_all, "n")
        pl.semaphore_signal(go, inc=1, device_id=dev["core"], device_id_type=MESH)
        norm_blocks(3, 5)
        dhidden(2, 6, 3, 5)
        w_last("u")
        forward(0, 1, 7)
        pl.semaphore_signal(go, inc=1, device_id=dev["core"], device_id_type=MESH)
        forward(2, 6, 3, 5)
        ag_last(x_all, "n")
        norm_blocks(4)
        forward(4)
        ag_last(dy_all, "dy")
        dhidden(4)
        dhidden_mid()
        cotangents()
        rs_first()
        rs_compute(2)
        rs_free()
        rs_step(2, (False,), (0,))
        hidden()
        rs_compute(3)
        rs_step(2, (False,), (1,))
        left_all("big")
        g_first("u", 0, 1)
        rs_step(3, (True,), (0,))
        rs_step(3, (True,), (1,))
        rs_step(3, (False,), (0,))
        rs_compute(4)
        rs_step(3, (False,), (1,))
        g_first("u", 1, 2)
        rs_step(4, (True,), (0,))
        rs_own()
        rs_step(4, (False,), (0,))
        rs_step(4, (False,), (1,))
        g_kept("d", 0, 1)
        rs_step(4, (True,), (1,))
        rs_last(0)
        g_first("d", 1, 2)
        g_kept("d", 1, 2)
        rs_last(1)
        pl.semaphore_signal(go, inc=1, device_id=dev["core"], device_id_type=MESH)
        g_first("d", 0, 1)
        take_stat()
        dx_send(0)
        dx_send(1)
        g_first("u", 2, 3)
        g_kept("u", 1, 2)
        g_kept("u", 0, 1)
        g_first("d", 2, 3)
        g_kept("u", 2, 4)
        g_near("u", False)
        gain_dx()
        g_partner("u")
        g_kept("d", 4, 5)
        g_kept("d", 2, 4)
        g_near("d", False)
        g_far("u")
        g_partner("d")
        g_kept("u", 4, 5)
        g_far("d")
        g_near("u", True)
        g_near("d", True)
        g_most("u")
        g_last("u")
        g_most("d")
        g_last("d")
        finish()
        ctx[0] = None

    @pl.when(s == 0)
    def _():
        ctx[0] = 0
        take_gain()
        normalize()
        norm_own()
        ag_xl(n_all, "m")
        pl.semaphore_wait(go, 1)
        w_own_x("d")
        w_own_y("d", 0, 1)
        w_own_y("u", 0)
        w_own_x("u")
        pl.semaphore_wait(go, 1)
        ag_z(n_all, "m")
        ag_partner(n_all, "m")
        w_fwd("d")
        w_own_y("u", 1)
        w_fwd("u")
        w_pass("d")
        own_wait(n_all, "m", 1)
        z_send(n_all, "m", 1, 0)
        w_far("d")
        own_wait(n_all, "m", 2)
        pair_send(n_all, "m", 2, 6)
        w_pass("u")
        w_far("u")
        pl.semaphore_wait(go, 1)
        z_send(n_all, "m", 2, 0)
        pair_wait(n_all, "m", 2, 6)
        z_send(n_all, "m", 2, 1)
        ag_partner(dy_all, "e", (0,))
        ag_partner(dy_all, "e", (1,))
        ag_fwd(dy_all, "e", 1, 0, (1,))
        ag_fwd(dy_all, "e", 1, 1, (0,))
        ag_fwd(dy_all, "e", 1, 0, (0,))
        w_last("d")
        w_last("u")
        arrived(n_all, (zblk[7], ol), ("m", "z+", 1, 1))
        arrived(n_all, (zblk[1], ol), ("m", "z-", 1, 1))
        forward(0, 1, 7)
        ag_fwd(dy_all, "e", 1, 1, (1,))
        ag_fwd(dy_all, "e", 2, 0, (1,))
        ag_fwd(dy_all, "e", 2, 1, (0,))
        ag_fwd(dy_all, "e", 2, 0, (0,))
        ag_fwd(dy_all, "e", 2, 1, (1,))
        ag_fwd3(n_all, "m")
        forward(2, 6, 3, 5)
        ag_fwd3(dy_all, "e", (0,))
        for h in range(H):
            arrived(dy_all, (z, xl, h), ("e", "core", h))
        dhidden(0, 1, 7)
        ag_fwd3(dy_all, "e", (1,))
        dhidden(2, 6, 3, 5)
        ag_last(n_all, "m")
        forward(4)
        hidden()
        ag_last(dy_all, "e", (0,))
        ag_last(dy_all, "e", (1,))
        dhidden(4)
        dhidden_mid()
        cotangents()
        left_all("big")
        g_first("u", 0, 2)
        rs_first()
        g_first("u", 2, 3)
        rs_compute(2)
        rs_free()
        g_kept("u", 2, 4)
        g_near("u", False)
        g_first("d", 1, 2)
        rs_step(2, (False,), (0,))
        g_kept("u", 1, 2)
        rs_step(2, (False,), (1,))
        rs_compute(3)
        rs_step(3, (True,), (0,))
        g_first("d", 2, 3)
        g_first("d", 0, 1)
        rs_step(3, (True,), (1,))
        rs_compute(4)
        rs_step(3, (False,), (0,))
        rs_own()
        rs_step(3, (False,), (1,))
        g_partner("u")
        rs_step(4, (True,), (0,))
        g_kept("u", 0, 1)
        g_far("u")
        rs_step(4, (True,), (1,))
        g_kept("d", 0, 1)
        rs_step(4, (False,), (0,))
        g_kept("d", 4, 5)
        g_far("d")
        rs_step(4, (False,), (1,))
        g_kept("d", 1, 2)
        g_kept("d", 2, 4)
        g_near("d", False)
        rs_last(0)
        rs_last(1)
        g_partner("d")
        g_kept("u", 4, 5)
        g_near("u", True)
        g_near("d", True)
        take_stat()
        dx_part(0)
        g_most("u")
        dx_part(1)
        gain_dx()
        g_last("u")
        g_most("d")
        g_last("d")
        finish()
        ctx[0] = None

    spread_left(ssq_in, tp_peers, "ssq")
    spread_left(stat_in, tp_peers, "stat")
    spread_left(gain_in, fs_peers, "gain")


def put_kernel(*refs):
    copies = [pltpu.make_async_copy(refs[k], refs[5 + k], refs[10].at[k]) for k in range(5)]
    for c in copies:
        c.start()
    for c in copies:
        c.wait()


def body(saved_inputs, top_grad, norm_gain, gate_weight, up_weight, down_weight):
    x = saved_inputs.reshape(T, W)
    tg = top_grad.reshape(T, W)
    hbm = pl.BlockSpec(memory_space=pl.ANY)
    outs = (
        jax.ShapeDtypeStruct((T, W), BF16),
        jax.ShapeDtypeStruct((PW, FL), F32),
        jax.ShapeDtypeStruct((PW, FL), F32),
        jax.ShapeDtypeStruct((PW, FL), F32),
        jax.ShapeDtypeStruct((1, W), F32),
    )
    out = pl.pallas_call(
        fused_kernel,
        name="fused",
        out_shape=[pltpu.VMEM(o.shape, o.dtype) for o in outs],
        in_specs=[hbm] * 6,
        out_specs=[pl.BlockSpec(memory_space=pltpu.VMEM)] * 5,
        scratch_shapes=[
            pltpu.VMEM((T, W), BF16),
            pltpu.VMEM((T, W), BF16),
            pltpu.VMEM((1, D), F32),
            pltpu.VMEM((PW, FL), BF16),
            pltpu.VMEM((PW, FL), BF16),
            pltpu.VMEM((PW, FL), BF16),
            pltpu.VMEM((W, 128), F32),
            pltpu.VMEM((128, 128), F32),
            pltpu.VMEM((D, 128), F32),
            pltpu.VMEM((NZ, NXL, W, T), BF16),
            pltpu.VMEM((NF, PW, UW), BF16),
            pltpu.VMEM((NF, DR, DH), BF16),
            pltpu.VMEM((NZ, NXL, W, T), BF16),
            pltpu.VMEM((NZ, NXL, H, W, TH), BF16),
            pltpu.VMEM((UW, T), F32),
            pltpu.VMEM((DH + 128 + 16, T), F32),
            pltpu.VMEM((UW, T), BF16),
            pltpu.VMEM((FL, T), BF16),
            pltpu.VMEM((128, T), BF16),
            pltpu.VMEM((W, T), F32),
            pltpu.VMEM((1, T), F32),
            pltpu.VMEM((8, T), F32),
            pltpu.VMEM((NT, 1, T), F32),
            pltpu.VMEM((NT, 1, T), F32),
            pltpu.VMEM((NF, 8, W), F32),
            pltpu.VMEM((7, H, NXL, W, TH), BF16),
            pltpu.VMEM((2, 4, H, NXL, W, TH), BF16),
            pltpu.VMEM((3, 2, H, NXL, W, TH), F32),
            pltpu.VMEM((H, NXL, W, TH), F32),
            pltpu.VMEM((H, W, TH), F32),
            pltpu.VMEM((1, T), F32),
            pltpu.VMEM((H, W, TH), BF16),
            pltpu.VMEM((H, W, TH), BF16),
            pltpu.VMEM((H, W, TH), BF16),
            pltpu.VMEM((7, PW, UW), BF16),
            pltpu.VMEM((7, PW, UW), BF16),
            pltpu.VMEM((5, PW, UW), F32),
            pltpu.VMEM((7, DR, DH), BF16),
            pltpu.VMEM((7, DR, DH), BF16),
            pltpu.VMEM((5, DR, DH), F32),
            pltpu.SemaphoreType.DMA((NBIG + NSMALL + 3,)),
            pltpu.SemaphoreType.DMA((NCOMMON + NEACH,)),
            pltpu.SemaphoreType.DMA((6,)),
            pltpu.SemaphoreType.REGULAR,
        ],
        compiler_params=pltpu.CompilerParams(
            collective_id=0, has_side_effects=True, vmem_limit_bytes=58 * 2**20
        ),
    )(x, tg, norm_gain, gate_weight[0], up_weight[0], down_weight[0].T)
    dx, gg, ug, dg, gn = pl.pallas_call(
        put_kernel,
        name="put",
        out_shape=outs,
        in_specs=[pl.BlockSpec(memory_space=pltpu.VMEM)] * 5,
        out_specs=[hbm] * 5,
        scratch_shapes=[pltpu.SemaphoreType.DMA((5,))],
    )(*[pltpu.with_memory_space_constraint(o, pltpu.VMEM) for o in out])
    return (dx.reshape(1, MICRO, ROWS, W), gg[None], ug[None], dg.T[None], gn)


def solution(mesh):
    return jax.shard_map(
        body,
        mesh=mesh,
        in_specs=(
            P("section", None, "fsdp", "tp"),
            P(None, "fsdp", "tp"),
            P("section", None),
            P("section", "fsdp", "tp"),
            P("section", "fsdp", "tp"),
            P("section", "tp", "fsdp"),
        ),
        out_specs=(
            P("section", None, "fsdp", "tp"),
            P("section", "fsdp", "tp"),
            P("section", "fsdp", "tp"),
            P("section", "tp", "fsdp"),
            P("section", "tp"),
        ),
        check_vma=False,
    )
```

```python
import jax
import jax.numpy as jnp
from jax import lax
from jax.experimental import pallas as pl
from jax.experimental.pallas import tpu as pltpu
from jax.sharding import PartitionSpec as P

EPS = 1e-05
MESH = pl.DeviceIdType.MESH
F32 = jnp.float32
BF16 = jnp.bfloat16

NY, NXH, NZ, NXL = 4, 2, 8, 2
NF, NT = NY * NXH, NZ * NXL
MICRO = 8
ROWS = 64
T = MICRO * ROWS
H = 2
TH = T // H
W = 160
PW = NXL * W
FL = 432
GU = 2 * FL
D = W * NT
UW = 896
DH = 384
DR = PW + 16
NCOMMON = 79
NEACH = 48
NBIG = 16
NSMALL = 20


def dot(a, b, ca, cb, precision=None):
    return lax.dot_general(
        a, b, (((ca,), (cb,)), ((), ())), preferred_element_type=F32, precision=precision
    )


def fused_kernel(
    x_hbm,
    tg_hbm,
    gain_hbm,
    wg_hbm,
    wu_hbm,
    wd_hbm,
    dx_ref,
    gg_ref,
    ug_ref,
    dg_ref,
    gn_ref,
    x_ref,
    tg_ref,
    gain_row,
    wg_ref,
    wu_ref,
    wd_ref,
    gain,
    gain_sq,
    gain_all,
    x_all,
    wgu,
    wd,
    n_all,
    dy_all,
    gu,
    dh,
    dgu,
    hid,
    hid_mid,
    unit,
    scale,
    stat,
    ssq_in,
    stat_in,
    gain_in,
    pdn,
    rdn,
    pf,
    pown,
    gx,
    nstat,
    xs,
    xr,
    dxs,
    sgu,
    rgu,
    fgu,
    sgd,
    rgd,
    fgd,
    ssem,
    rsem,
    lsem,
    go,
):
    s = lax.axis_index("section")
    f = lax.axis_index("fsdp")
    t = lax.axis_index("tp")
    y, xh = lax.div(f, NXH), lax.rem(f, NXH)
    z, xl = lax.div(t, NXL), lax.rem(t, NXL)
    oh, ol = 1 - xh, 1 - xl

    def at_y(step):
        return (s, lax.rem(y + step + NY, NY) * NXH + xh, t)

    def at_z(step):
        return (s, f, lax.rem(z + step + NZ, NZ) * NXL + xl)

    dev = {
        "y+": at_y(1),
        "y-": at_y(-1),
        "z+": at_z(1),
        "z-": at_z(-1),
        "xh": (s, y * NXH + oh, t),
        "xl": (s, f, z * NXL + ol),
        "core": (1 - s, f, t),
    }
    across = {
        "core": (1 - s, f, t),
        "xl": (1 - s, *dev["xl"][1:]),
        "z+": (1 - s, *dev["z+"][1:]),
        "z-": (1 - s, *dev["z-"][1:]),
    }
    tp_peers = [(s, f, lax.rem(t + k, NT)) for k in range(1, NT)]
    fs_peers = [(s, lax.rem(f + k, NF), t) for k in range(1, NF)]
    zblk = [lax.rem(z + k, NZ) for k in range(NZ)]
    own, left, right, far = (
        {"c": lax.rem(y + k, NY) * NXH + xh, "o": lax.rem(y + k, NY) * NXH + oh} for k in (0, 3, 1, 2)
    )

    ids = {}
    size = {None: 0, 0: 0, 1: 0}
    private = {"dy": 1, "n": 1, "m": 0, "e": 0}
    ctx = [None]

    def ident(name, n=1):
        if name not in ids:
            sec = private.get(name[0])
            ids[name] = size[sec] + (0 if sec is None else NCOMMON)
            size[sec] += n
            assert size[sec] <= (NCOMMON if sec is None else NEACH), size
        return ids[name]

    def copy(src, dst, sm, rm, to):
        return pltpu.make_async_remote_copy(
            src_ref=src,
            dst_ref=dst,
            send_sem=ssem.at[sm],
            recv_sem=rsem.at[rm],
            device_id=to,
            device_id_type=MESH,
        )

    def static(idx):
        return tuple(i if isinstance(i, (int, pl.Slice)) else 0 for i in idx)

    turn = {sec: {"big": 0, "small": 0} for sec in (0, 1)}
    flying = {0: {}, 1: {}}

    def left_all(kind=None):
        mine = flying[ctx[0]]
        for m in sorted(mine):
            if kind is None or (m < NBIG) == (kind == "big"):
                src, si = mine.pop(m)
                r = src.at[si]
                copy(r, r, m, 0, dev["core"]).wait_send()

    def take(src, si, kind):
        mine, sec = flying[ctx[0]], ctx[0]
        base, n = (0, NBIG) if kind == "big" else (NBIG, NSMALL)
        m = base + turn[sec][kind] % n
        turn[sec][kind] += 1
        if m in mine:
            was, wi = mine.pop(m)
            r = was.at[wi]
            copy(r, r, m, 0, dev["core"]).wait_send()
        mine[m] = (src, static(si))
        return m

    def send(src, si, dst, di, name, to, q=None, kind="small"):
        rm = ident(name, 1 if q is None else 2)
        sm = take(src, si, kind)
        copy(src.at[si], dst.at[di], sm, rm if q is None else rm + q, to).start()

    def arrived(dst, di, name, q=None):
        m = ident(name, 1 if q is None else 2)
        r = dst.at[di]
        copy(r, r, 0, m if q is None else m + q, dev["core"]).wait_recv()

    def rows(n, step, fn):
        def body(i, c):
            fn(pl.multiple_of(i * step, step))
            return c

        lax.fori_loop(0, n // step, body, 0)

    barrier = pltpu.get_barrier_semaphore()
    everyone = tp_peers[4:11] + tp_peers[:4] + tp_peers[11:] + fs_peers + list(across.values())
    for to in everyone:
        pl.semaphore_signal(barrier, inc=1, device_id=to, device_id_type=MESH)

    loads = [
        pltpu.make_async_copy(src, dst, lsem.at[k])
        for k, (src, dst) in enumerate(
            (
                (x_hbm, x_ref),
                (tg_hbm, tg_ref),
                (gain_hbm, gain_row),
                (wd_hbm, wd_ref),
                (wg_hbm, wg_ref),
                (wu_hbm, wu_ref),
            )
        )
    ]
    for c in loads:
        c.start()
    eye = (
        lax.broadcasted_iota(jnp.int32, (W, W), 0) == lax.broadcasted_iota(jnp.int32, (W, W), 1)
    ).astype(BF16)
    loads[0].wait()
    xt = dot(eye, x_ref[...], 1, 1)
    ssq_in[t] = jnp.sum(xt * xt, axis=0, keepdims=True)
    unit[...] = xt
    loads[1].wait()

    @pl.when(s == 1)
    def _():
        x_all[z, xl] = xt.astype(BF16)
        top = dot(eye, tg_ref[...], 1, 1).astype(BF16)
        for h in range(H):
            dy_all[z, xl, h] = top[:, h * TH : (h + 1) * TH]

    def pack_d():
        loads[3].wait()

        def pack(r):
            wd[f, pl.ds(r, 32), :] = wd_ref[pl.ds(r, 32), 0:DH]
            wgu[f, pl.ds(r, 32), GU:UW] = wd_ref[pl.ds(r, 32), DH : DH + 32]

        rows(PW, 32, pack)
        last = (
            lax.broadcasted_iota(jnp.int32, (16, FL), 0) + (FL - 16)
            == lax.broadcasted_iota(jnp.int32, (16, FL), 1)
        ).astype(BF16)
        wd[f, PW:DR, 0:PW] = dot(last, wd_ref[...], 1, 1).astype(BF16)

    def pack_u():
        loads[4].wait()
        loads[5].wait()

        def pack(r):
            wgu[f, pl.ds(r, 32), 0:FL] = wg_ref[pl.ds(r, 32), :]
            wgu[f, pl.ds(r, 32), FL:GU] = wu_ref[pl.ds(r, 32), :]

        rows(PW, 32, pack)

    def take_gain():
        loads[2].wait()
        gain_sq[...] = jnp.zeros_like(gain_sq)
        for c in range(D // 128):
            gain_sq[c : c + 1, :] = gain_row[:, c * 128 : (c + 1) * 128]
        cols = gain_sq[...].T
        for c in range(D // 128):
            gain_all[c * 128 : (c + 1) * 128, :] = jnp.broadcast_to(cols[:, c : c + 1], (128, 128))
        gain[...] = gain_all[pl.ds(pl.multiple_of(t * W, 8), W), :]

    def spread(buf, me, peers, name):
        m = ident((name,))
        for to in peers:
            copy(buf.at[me], buf.at[me], NBIG + NSMALL + ("ssq", "stat", "gain").index(name), m, to).start()

    def collect(buf, peers, name):
        n = len(peers)
        r = buf.at[pl.ds(0, n)]
        copy(r, r, 0, ident((name,)), dev["core"]).wait_recv()
        total = buf[0]
        for k in range(1, n + 1):
            total = total + buf[k]
        return total

    def spread_left(buf, peers, name):
        r = buf.at[pl.ds(0, len(peers))]
        copy(r, r, NBIG + NSMALL + ("ssq", "stat", "gain").index(name), 0, dev["core"]).wait_send()

    pack_d()
    pack_u()

    pl.semaphore_wait(barrier, len(everyone))
    spread(ssq_in, t, tp_peers, "ssq")

    halves = {"u": ((0, 160), (160, 160)), "d": ((0, 160), (160, 176))}
    full = {"u": wgu, "d": wd}

    def w_own_x(a):
        send(full[a], (f,), full[a], (f,), ("w", a, "own", "xh"), dev["xh"], kind="big")

    def w_own_y(a, *parts):
        for i in parts:
            for d, k in (("y+", i), ("y-", 1 - i)):
                at = (f, pl.ds(*halves[a][k]))
                send(full[a], at, full[a], at, ("w", a, "own", d, i), dev[d], kind="big")

    def w_fwd(a):
        arr = full[a]
        for d, blk, k in (("y+", left["c"], 0), ("y-", right["c"], 1)):
            at = (blk, pl.ds(*halves[a][k]))
            arrived(arr, at, ("w", a, "own", d, 0))
            send(arr, at, arr, at, ("w", a, "fwd", d), dev[d], kind="big")

    def w_pass(a):
        arr, blk = full[a], own["o"]
        arrived(arr, (blk,), ("w", a, "own", "xh"))
        for d in ("y+", "y-"):
            send(arr, (blk,), arr, (blk,), ("w", a, "pass", d), dev[d], kind="big")

    def w_far(a):
        arr, blk = full[a], far["c"]
        for d, k in (("y+", 0), ("y-", 1)):
            arrived(arr, (blk, pl.ds(*halves[a][k])), ("w", a, "fwd", d))
        send(arr, (blk,), arr, (blk,), ("w", a, "far"), dev["xh"], kind="big")

    def w_last(a):
        arr = full[a]
        arrived(arr, (left["o"],), ("w", a, "pass", "y+"))
        arrived(arr, (right["o"],), ("w", a, "pass", "y-"))
        arrived(arr, (far["o"],), ("w", a, "far"))
        for d, blk, k in (("y+", left["c"], 1), ("y-", right["c"], 0)):
            arrived(arr, (blk, pl.ds(*halves[a][k])), ("w", a, "own", d, 1))

    def ag_xl(buf, nm):
        send(buf, (z, xl), buf, (z, xl), (nm, "xl"), dev["xl"])

    def ag_z(buf, nm):
        for d in ("z+", "z-"):
            send(buf, (z, xl), buf, (z, xl), (nm, d, 1, 0), dev[d])

    def ag_own(buf, nm):
        ag_xl(buf, nm)
        ag_z(buf, nm)

    def ag_partner(buf, nm, hh=()):
        at = (z, ol, *hh)
        arrived(buf, at, (nm, "xl", *hh))
        send(buf, at, buf, at, (nm, "z+", 1, 1, *hh), dev["z+"])
        send(buf, at, buf, at, (nm, "z-", 1, 1, *hh), dev["z-"])

    def ag_fwd(buf, nm, k, j, hh=()):
        q = (xl, ol)[j]
        for d, blk in (("z+", zblk[NZ - k]), ("z-", zblk[k])):
            at = (blk, q, *hh)
            arrived(buf, at, (nm, d, k, j, *hh))
            send(buf, at, buf, at, (nm, d, k + 1, j, *hh), dev[d])

    def ag_fwd3(buf, nm, hh=()):
        for d, blk, q in (("z+", zblk[5], 0), ("z-", zblk[3], 1)):
            for j in range(2):
                arrived(buf, (blk, (xl, ol)[j], *hh), (nm, d, 3, j, *hh))
            send(buf, (blk, q, *hh), buf, (blk, q, *hh), (nm, d, 4, *hh), dev[d])

    def ag_last(buf, nm, hh=()):
        arrived(buf, (zblk[4], 0, *hh), (nm, "z+", 4, *hh))
        arrived(buf, (zblk[4], 1, *hh), (nm, "z-", 4, *hh))

    def pair_send(buf, nm, *ks):
        for k in ks:
            at = (zblk[k], xl)
            send(buf, at, buf, at, (nm, "pair", k), dev["xl"])

    def pair_wait(buf, nm, *ks):
        for k in ks:
            arrived(buf, (zblk[k], ol), (nm, "pair", k))

    def own_wait(buf, nm, k):
        for d, b in (("z+", zblk[NZ - k]), ("z-", zblk[k])):
            arrived(buf, (b, xl), (nm, d, k, 0))

    def z_send(buf, nm, k, j):
        for d, b in (("z+", zblk[NZ - k]), ("z-", zblk[k])):
            at = (b, (xl, ol)[j])
            send(buf, at, buf, at, (nm, d, k + 1, j), dev[d])

    def act(buf, i):
        return jnp.concatenate([buf[i, :, h].reshape(PW, TH) for h in range(H)], axis=1)

    def pick(i, table):
        v = table[0]
        for k in range(1, len(table)):
            v = jnp.where(i == k, table[k], v)
        return v

    def together(parts):
        return jnp.concatenate(parts, axis=0)

    def forward(*ks):
        blks = [zblk[k] for k in ks]
        part = dot(
            together([wgu[b] for b in blks]),
            together([n_all[b].reshape(PW, T) for b in blks]),
            0,
            0,
        )
        gu[...] = part if 0 in ks else gu[...] + part

    def dhidden(*ks):
        blks = [zblk[k] for k in ks]
        dys = [act(dy_all, b) for b in blks]
        dy = together(dys)
        parts = (
            (0, dot(together([wd[b, 0:PW] for b in blks]), dy, 0, 0)),
        )
        for r, part in parts:
            at = pl.ds(r, part.shape[0])
            dh[at, :] = part if 0 in ks else dh[at, :] + part
        part = dot(wd[blks[0], PW:DR, 0:PW], dys[0], 1, 0)
        for b, d in zip(blks[1:], dys[1:]):
            part = part + dot(wd[b, PW:DR, 0:PW], d, 1, 0)
        at = pl.ds(DH + 128, 16)
        dh[at, :] = part if 0 in ks else dh[at, :] + part

    def dhidden_mid():
        lhs = together([wgu[b, :, UW - 128 : UW] for b in range(NF)])
        dh[DH : DH + 128, :] = dot(lhs, together([act(dy_all, b) for b in range(NF)]), 0, 0)

    def hidden():
        def body(r):
            gate = gu[pl.ds(r, 16), :]
            up = gu[pl.ds(pl.multiple_of(FL + r, 16), 16), :]
            hid[pl.ds(r, 16), :] = (gate * jax.nn.sigmoid(gate) * up).astype(BF16)

        rows(FL, 48, lambda r: [body(pl.multiple_of(r + k, 16)) for k in (0, 16, 32)])
        hid_mid[0:96, :] = jnp.zeros((96, T), BF16)
        hid_mid[96:128, :] = hid[DH : DH + 32, :]

    def normalize():
        row_scale = lax.rsqrt(collect(ssq_in, tp_peers, "ssq") / D + EPS)
        scale[...] = row_scale
        unit[...] = unit[...] * row_scale

    def norm_own():
        n_all[z, xl] = (unit[...] * gain[:, 0:1]).astype(BF16)

    def norm_blocks(*ks):
        for k in ks:
            b = zblk[k]
            for q in range(NXL):
                g = gain_all[pl.ds(pl.multiple_of(b * PW + q * W, 8), W), :]
                for c in range(T // 128):
                    at = slice(c * 128, (c + 1) * 128)
                    n_all[b, q, :, at] = (
                        x_all[b, q, :, at].astype(F32) * scale[:, at] * g
                    ).astype(BF16)

    def cotangents():
        stat[...] = jnp.zeros_like(stat)
        dgu[GU:UW, :] = jnp.zeros((UW - GU, T), BF16)

        def elementwise(r):
            gate = gu[pl.ds(r, 16), :]
            up = gu[pl.ds(pl.multiple_of(FL + r, 16), 16), :]
            dd = dh[pl.ds(pl.multiple_of(jnp.where(r < DH, r, r + 96), 16), 16), :]
            sig = jax.nn.sigmoid(gate)
            silu = gate * sig
            d_gate = (dd * up * sig * (1.0 + gate * (1.0 - sig))).astype(BF16)
            d_up = (dd * silu).astype(BF16)
            dgu[pl.ds(r, 16), :] = d_gate
            dgu[pl.ds(pl.multiple_of(FL + r, 16), 16), :] = d_up
            both = d_gate.astype(F32) * gate + d_up.astype(F32) * up
            stat[...] += both[0:8] + both[8:16]

        rows(FL, 48, lambda r: [elementwise(pl.multiple_of(r + k, 16)) for k in (0, 16, 32)])
        stat_in[t] = jnp.sum(stat[...], axis=0, keepdims=True)
        spread(stat_in, t, tp_peers, "stat")

    ways = (("z+", 0), ("z-", 1))

    def rs_first():
        def body(h, c):
            part = dot(wgu[zblk[4], :, 0:GU], dgu[0:GU, :], 1, 0).reshape(NXL, W, T)
            for hh in range(H):
                pdn[0, hh] = part[:, :, hh * TH : (hh + 1) * TH].astype(BF16)
            return c

        lax.fori_loop(0, 1, body, 0)
        for h in range(H):
            for d, w in ways:
                send(pdn, (0, h, w), rdn, (w, 0, h, w), ("rs", d, 1, h), dev[d], q=w)

    def rs_compute(k):
        def body(w, c):
            blk = jnp.where(w == 0, zblk[5 - k], zblk[3 + k])
            part = dot(wgu[blk, :, 0:GU], dgu[0:GU, :], 1, 0).reshape(NXL, W, T)
            for hh in range(H):
                pf[k - 2, w, hh] = part[:, :, hh * TH : (hh + 1) * TH]
            return c

        lax.fori_loop(0, 2, body, 0)

    def rs_free():
        for h in range(H):
            for d, w in ways:
                q = 1 - w
                pdn[1 + w, h, q] = pf[0, w, h, q].astype(BF16)
                send(pdn, (1 + w, h, q), rdn, (w, 1, h, q), ("rs", d, 2, h), dev[d], q=q)

    def rs_step(k, ahead=(True, False), hs=range(H)):
        slot = 2 * k - 3
        for first in ahead:
            for h in hs:
                for d, w in ways:
                    q = 1 - w if first else w
                    arrived(rdn, (w, k - 2, h, q), ("rs", d, k - 1, h), q=q)
                    pdn[slot + w, h, q] = (
                        pf[k - 2, w, h, q] + rdn[w, k - 2, h, q].astype(F32)
                    ).astype(BF16)
                    send(pdn, (slot + w, h, q), rdn, (w, k - 1, h, q), ("rs", d, k, h), dev[d], q=q)

    def rs_own():
        def body(h, c):
            part = dot(wgu[z, :, 0:GU], dgu[0:GU, :], 1, 0).reshape(NXL, W, T)
            for hh in range(H):
                pown[hh] = part[:, :, hh * TH : (hh + 1) * TH]
            return c

        lax.fori_loop(0, 1, body, 0)

    def rs_last(h):
        for q in (ol, xl):
            for d, w in ways:
                arrived(rdn, (w, 3, h, q), ("rs", d, 4, h), q=q)
            if q is ol:
                xs[h] = (
                    pown[h, q] + rdn[0, 3, h, q].astype(F32) + rdn[1, 3, h, q].astype(F32)
                ).astype(BF16)
                send(xs, (h,), xr, (h,), ("rx", h), dev["xl"])

    def take_stat():
        nstat[...] = collect(stat_in, tp_peers, "stat") / D

    def dx_part(h):
        arrived(xr, (h,), ("rx", h))
        cols = slice(h * TH, (h + 1) * TH)
        d_normed = (
            pown[h, xl]
            + rdn[0, 3, h, xl].astype(F32)
            + rdn[1, 3, h, xl].astype(F32)
            + xr[h].astype(F32)
        )
        u = unit[:, cols]
        dx = dy_all[z, xl, h].astype(F32) + scale[:, cols] * (
            d_normed * gain[:, 0:1] - u * nstat[:, cols]
        )
        dxs[h] = dx.astype(BF16)
        gx[h] = d_normed * u

    def dx_send(h):
        dx_part(h)
        for d, name in (
            ("xl", ("xl", h)),
            ("z+", ("z+", 1, 0, h)),
            ("z-", ("z-", 1, 0, h)),
            ("core", ("core", h)),
        ):
            send(dxs, (h,), dy_all, (z, xl, h), ("e", *name), across[d])

    def gain_dx():
        total = dot(
            jnp.ones((8, T), F32),
            jnp.concatenate([gx[h] for h in range(H)], axis=1),
            1,
            1,
            lax.Precision.HIGHEST,
        )
        gain_in[f] = total
        spread(gain_in, f, fs_peers, "gain")
        for h in range(H):
            dx_ref[h * TH : (h + 1) * TH, :] = dot(dxs[h], eye, 0, 0).astype(BF16)

    sg, rg, fg = {"u": sgu, "d": sgd}, {"u": rgu, "d": rgd}, {"u": fgu, "d": fgd}
    size_of = {"u": (PW, 32), "d": (DR, 48)}

    def wgrad(a, blk, dst, i):
        dy = act(dy_all, blk)
        if a == "u":
            cut = UW - 128
            n = n_all[blk].reshape(PW, T)
            dst[i, :, 0:cut] = dot(n, dgu[0:cut, :], 1, 1).astype(dst.dtype)
            edge = dot(n, dgu[cut:UW, :], 1, 1) + dot(dy, hid_mid[...], 1, 1)
            dst[i, :, cut:UW] = edge.astype(dst.dtype)
        else:
            dst[i, 0:PW, :] = dot(dy, hid[0:DH, :], 1, 1).astype(dst.dtype)
            dst[i, PW:DR, 0:PW] = dot(hid[FL - 16 : FL, :], dy, 1, 1).astype(dst.dtype)

    direct = [right["o"], left["o"], far["o"]]
    kept = [far["c"], own["o"], right["c"], left["c"], own["c"]]

    def g_first(a, lo=0, hi=3):
        rm = ident(("g", a, 0), 3)
        sm = [take(sg[a], (0,), "big") if lo <= i < hi else 0 for i in range(3)]

        def body(i, c):
            wgrad(a, pick(i, direct), sg[a], i)
            to = pick(i, [dev[d][1] for d in ("y+", "y-", "xh")])
            copy(sg[a].at[i], rg[a].at[i], pick(i, sm), rm + i, (s, to, t)).start()
            return c

        lax.fori_loop(lo, hi, body, 0)

    def g_kept(a, lo, hi):
        def body(i, c):
            wgrad(a, pick(i, kept), fg[a], i)
            return c

        lax.fori_loop(lo, hi, body, 0)

    def g_sum(a, slot, own_i, recv, span=None):
        n, st = size_of[a]
        lo, n = span if span else (0, n)
        st = 16 if span else st

        def body(r):
            r = pl.multiple_of(r + lo, 16)
            v = fg[a][own_i, pl.ds(r, st), :]
            for k in recv:
                v = v + rg[a][k, pl.ds(r, st), :].astype(F32)
            sg[a][slot, pl.ds(r, st), :] = v.astype(BF16)

        rows(n, st, body)

    def g_far(a):
        arrived(rg[a], (2,), ("g", a, 0), q=2)
        g_sum(a, 3, 0, (2,))
        for d, k in (("y+", 0), ("y-", 1)):
            part = pl.ds(*halves[a][k])
            send(sg[a], (3, part), rg[a], (3, part), ("g", a, 3, d), dev[d], kind="big")

    def g_near(a, waits):
        for d, k, slot in (("y+", 0, 4), ("y-", 1, 5)):
            half = halves[a][k if waits else 1 - k]
            part = pl.ds(*half)
            if waits:
                arrived(rg[a], (3, part), ("g", a, 3, d))
            g_sum(a, slot, 2 + k, (3,) if waits else (), half)
            send(sg[a], (slot, part), rg[a], (slot, part), ("g", a, slot, waits), dev[d], kind="big")

    def g_partner(a):
        arrived(rg[a], (0,), ("g", a, 0), q=0)
        arrived(rg[a], (1,), ("g", a, 0), q=1)
        g_sum(a, 6, 1, (0, 1))
        send(sg[a], (6,), rg[a], (6,), ("g", a, 6), dev["xh"], kind="big")

    def g_most(a):
        for k in (0, 1):
            part = pl.ds(*halves[a][1 - k])
            arrived(rg[a], (4 + k, part), ("g", a, 4 + k, False))
        arrived(rg[a], (6,), ("g", a, 6))
        for k in (0, 1):
            lo, n = halves[a][1 - k]

            def body(r, k=k, lo=lo):
                at = pl.ds(pl.multiple_of(r + lo, 16), 16)
                fg[a][4, at, :] += rg[a][4 + k, at, :].astype(F32) + rg[a][6, at, :].astype(F32)

            rows(n, 16, body)

    def g_last(a):
        for k in (0, 1):
            lo, n = halves[a][k]
            arrived(rg[a], (4 + k, pl.ds(lo, n)), ("g", a, 4 + k, True))

            def total(at, k=k):
                return fg[a][4, at, :] + rg[a][4 + k, at, :].astype(F32)

            def body(r, total=total, lo=lo):
                at = pl.ds(pl.multiple_of(r + lo, 16), 32)
                v = total(at)
                if a == "u":
                    gg_ref[at, :] = v[:, 0:FL]
                    ug_ref[at, :] = v[:, FL:GU]
                    dg_ref[at, DH : DH + 32] = v[:, GU:UW]
                else:
                    dg_ref[at, 0:DH] = v

            rows(160, 32, body)
            if n > 160:
                v = total(pl.ds(PW, 16))[:, 0:PW]
                unit16 = (
                    lax.broadcasted_iota(jnp.int32, (16, 16), 0)
                    == lax.broadcasted_iota(jnp.int32, (16, 16), 1)
                ).astype(F32)
                dg_ref[:, DH + 32 : FL] = dot(v, unit16, 0, 0, lax.Precision.HIGHEST)

    def finish():
        gn_ref[...] = collect(gain_in, fs_peers, "gain")[0:1]
        left_all()

    @pl.when(s == 1)
    def _():
        ctx[0] = 1
        ag_own(dy_all, "dy")
        ag_own(x_all, "n")
        w_own_x("d")
        w_own_y("d", 0, 1)
        w_own_y("u", 0, 1)
        w_own_x("u")
        take_gain()
        ag_partner(dy_all, "dy")
        ag_fwd(dy_all, "dy", 1, 0)
        normalize()
        ag_partner(x_all, "n")
        ag_fwd(x_all, "n", 1, 0)
        w_fwd("d")
        ag_fwd(dy_all, "dy", 1, 1)
        ag_fwd(dy_all, "dy", 2, 0)
        w_fwd("u")
        w_pass("d")
        ag_fwd(x_all, "n", 1, 1)
        ag_fwd(x_all, "n", 2, 0)
        w_far("d")
        norm_blocks(0, 1, 7)
        ag_fwd(dy_all, "dy", 2, 1)
        w_pass("u")
        w_far("u")
        ag_fwd(x_all, "n", 2, 1)
        norm_blocks(2, 6)
        ag_fwd3(dy_all, "dy")
        w_last("d")
        dhidden(0, 1, 7)
        ag_fwd3(x_all, "n")
        pl.semaphore_signal(go, inc=1, device_id=dev["core"], device_id_type=MESH)
        norm_blocks(3, 5)
        dhidden(2, 6, 3, 5)
        pl.semaphore_signal(go, inc=1, device_id=dev["core"], device_id_type=MESH)
        w_last("u")
        forward(0, 1, 7)
        forward(2, 6, 3, 5)
        ag_last(x_all, "n")
        norm_blocks(4)
        forward(4)
        ag_last(dy_all, "dy")
        dhidden(4)
        dhidden_mid()
        cotangents()
        rs_first()
        rs_compute(2)
        rs_free()
        rs_step(2, (False,), (0,))
        hidden()
        rs_compute(3)
        rs_step(2, (False,), (1,))
        left_all("big")
        g_first("u", 0, 1)
        rs_step(3, (True,), (0,))
        rs_step(3, (True,), (1,))
        rs_step(3, (False,), (0,))
        rs_compute(4)
        rs_step(3, (False,), (1,))
        g_first("u", 1, 2)
        rs_step(4, (True,), (0,))
        rs_own()
        rs_step(4, (False,), (0,))
        rs_step(4, (False,), (1,))
        g_kept("d", 0, 1)
        rs_step(4, (True,), (1,))
        rs_last(0)
        g_first("d", 1, 2)
        g_kept("d", 1, 2)
        rs_last(1)
        pl.semaphore_signal(go, inc=1, device_id=dev["core"], device_id_type=MESH)
        g_first("d", 0, 1)
        take_stat()
        dx_send(0)
        dx_send(1)
        g_first("u", 2, 3)
        g_kept("u", 1, 2)
        g_kept("u", 0, 1)
        g_first("d", 2, 3)
        g_kept("u", 2, 4)
        g_near("u", False)
        gain_dx()
        g_partner("u")
        g_kept("d", 4, 5)
        g_kept("d", 2, 4)
        g_near("d", False)
        g_far("u")
        g_partner("d")
        g_kept("u", 4, 5)
        g_far("d")
        g_near("u", True)
        g_near("d", True)
        g_most("u")
        g_last("u")
        g_most("d")
        g_last("d")
        finish()
        ctx[0] = None

    @pl.when(s == 0)
    def _():
        ctx[0] = 0
        take_gain()
        normalize()
        norm_own()
        ag_xl(n_all, "m")
        pl.semaphore_wait(go, 1)
        w_own_x("d")
        w_own_y("d", 0, 1)
        w_own_y("u", 0)
        w_own_x("u")
        pl.semaphore_wait(go, 1)
        ag_z(n_all, "m")
        ag_partner(n_all, "m")
        w_fwd("d")
        w_own_y("u", 1)
        own_wait(n_all, "m", 1)
        z_send(n_all, "m", 1, 0)
        w_fwd("u")
        w_pass("d")
        w_far("d")
        own_wait(n_all, "m", 2)
        pair_send(n_all, "m", 2, 6)
        w_pass("u")
        w_far("u")
        pl.semaphore_wait(go, 1)
        z_send(n_all, "m", 2, 0)
        pair_wait(n_all, "m", 2, 6)
        z_send(n_all, "m", 2, 1)
        ag_partner(dy_all, "e", (0,))
        ag_partner(dy_all, "e", (1,))
        ag_fwd(dy_all, "e", 1, 0, (1,))
        ag_fwd(dy_all, "e", 1, 1, (0,))
        ag_fwd(dy_all, "e", 1, 0, (0,))
        w_last("d")
        w_last("u")
        arrived(n_all, (zblk[7], ol), ("m", "z+", 1, 1))
        arrived(n_all, (zblk[1], ol), ("m", "z-", 1, 1))
        forward(0, 1, 7)
        ag_fwd(dy_all, "e", 1, 1, (1,))
        ag_fwd(dy_all, "e", 2, 0, (1,))
        ag_fwd(dy_all, "e", 2, 1, (0,))
        ag_fwd(dy_all, "e", 2, 0, (0,))
        ag_fwd(dy_all, "e", 2, 1, (1,))
        ag_fwd3(n_all, "m")
        forward(2, 6, 3, 5)
        ag_fwd3(dy_all, "e", (0,))
        for h in range(H):
            arrived(dy_all, (z, xl, h), ("e", "core", h))
        dhidden(0, 1, 7)
        ag_fwd3(dy_all, "e", (1,))
        dhidden(2, 6, 3, 5)
        ag_last(n_all, "m")
        forward(4)
        hidden()
        ag_last(dy_all, "e", (0,))
        ag_last(dy_all, "e", (1,))
        dhidden(4)
        dhidden_mid()
        cotangents()
        left_all("big")
        g_first("u", 0, 2)
        rs_first()
        g_first("u", 2, 3)
        rs_compute(2)
        rs_free()
        g_kept("u", 2, 4)
        g_near("u", False)
        g_first("d", 1, 2)
        rs_step(2, (False,), (0,))
        g_kept("u", 1, 2)
        rs_step(2, (False,), (1,))
        rs_compute(3)
        rs_step(3, (True,), (0,))
        g_first("d", 2, 3)
        g_first("d", 0, 1)
        rs_step(3, (True,), (1,))
        rs_compute(4)
        rs_step(3, (False,), (0,))
        rs_own()
        rs_step(3, (False,), (1,))
        g_partner("u")
        rs_step(4, (True,), (0,))
        g_kept("u", 0, 1)
        g_far("u")
        rs_step(4, (True,), (1,))
        g_kept("d", 0, 1)
        rs_step(4, (False,), (0,))
        g_kept("d", 4, 5)
        g_far("d")
        rs_step(4, (False,), (1,))
        g_kept("d", 1, 2)
        g_kept("d", 2, 4)
        g_near("d", False)
        rs_last(0)
        rs_last(1)
        g_near("u", True)
        g_partner("d")
        g_kept("u", 4, 5)
        g_near("d", True)
        take_stat()
        dx_part(0)
        g_most("u")
        dx_part(1)
        gain_dx()
        g_last("u")
        g_most("d")
        g_last("d")
        finish()
        ctx[0] = None

    spread_left(ssq_in, tp_peers, "ssq")
    spread_left(stat_in, tp_peers, "stat")
    spread_left(gain_in, fs_peers, "gain")


def put_kernel(*refs):
    copies = [pltpu.make_async_copy(refs[k], refs[5 + k], refs[10].at[k]) for k in range(5)]
    for c in copies:
        c.start()
    for c in copies:
        c.wait()


def body(saved_inputs, top_grad, norm_gain, gate_weight, up_weight, down_weight):
    x = saved_inputs.reshape(T, W)
    tg = top_grad.reshape(T, W)
    hbm = pl.BlockSpec(memory_space=pl.ANY)
    outs = (
        jax.ShapeDtypeStruct((T, W), BF16),
        jax.ShapeDtypeStruct((PW, FL), F32),
        jax.ShapeDtypeStruct((PW, FL), F32),
        jax.ShapeDtypeStruct((PW, FL), F32),
        jax.ShapeDtypeStruct((1, W), F32),
    )
    out = pl.pallas_call(
        fused_kernel,
        name="fused",
        out_shape=[pltpu.VMEM(o.shape, o.dtype) for o in outs],
        in_specs=[hbm] * 6,
        out_specs=[pl.BlockSpec(memory_space=pltpu.VMEM)] * 5,
        scratch_shapes=[
            pltpu.VMEM((T, W), BF16),
            pltpu.VMEM((T, W), BF16),
            pltpu.VMEM((1, D), F32),
            pltpu.VMEM((PW, FL), BF16),
            pltpu.VMEM((PW, FL), BF16),
            pltpu.VMEM((PW, FL), BF16),
            pltpu.VMEM((W, 128), F32),
            pltpu.VMEM((128, 128), F32),
            pltpu.VMEM((D, 128), F32),
            pltpu.VMEM((NZ, NXL, W, T), BF16),
            pltpu.VMEM((NF, PW, UW), BF16),
            pltpu.VMEM((NF, DR, DH), BF16),
            pltpu.VMEM((NZ, NXL, W, T), BF16),
            pltpu.VMEM((NZ, NXL, H, W, TH), BF16),
            pltpu.VMEM((UW, T), F32),
            pltpu.VMEM((DH + 128 + 16, T), F32),
            pltpu.VMEM((UW, T), BF16),
            pltpu.VMEM((FL, T), BF16),
            pltpu.VMEM((128, T), BF16),
            pltpu.VMEM((W, T), F32),
            pltpu.VMEM((1, T), F32),
            pltpu.VMEM((8, T), F32),
            pltpu.VMEM((NT, 1, T), F32),
            pltpu.VMEM((NT, 1, T), F32),
            pltpu.VMEM((NF, 8, W), F32),
            pltpu.VMEM((7, H, NXL, W, TH), BF16),
            pltpu.VMEM((2, 4, H, NXL, W, TH), BF16),
            pltpu.VMEM((3, 2, H, NXL, W, TH), F32),
            pltpu.VMEM((H, NXL, W, TH), F32),
            pltpu.VMEM((H, W, TH), F32),
            pltpu.VMEM((1, T), F32),
            pltpu.VMEM((H, W, TH), BF16),
            pltpu.VMEM((H, W, TH), BF16),
            pltpu.VMEM((H, W, TH), BF16),
            pltpu.VMEM((7, PW, UW), BF16),
            pltpu.VMEM((7, PW, UW), BF16),
            pltpu.VMEM((5, PW, UW), F32),
            pltpu.VMEM((7, DR, DH), BF16),
            pltpu.VMEM((7, DR, DH), BF16),
            pltpu.VMEM((5, DR, DH), F32),
            pltpu.SemaphoreType.DMA((NBIG + NSMALL + 3,)),
            pltpu.SemaphoreType.DMA((NCOMMON + NEACH,)),
            pltpu.SemaphoreType.DMA((6,)),
            pltpu.SemaphoreType.REGULAR,
        ],
        compiler_params=pltpu.CompilerParams(
            collective_id=0, has_side_effects=True, vmem_limit_bytes=58 * 2**20
        ),
    )(x, tg, norm_gain, gate_weight[0], up_weight[0], down_weight[0].T)
    dx, gg, ug, dg, gn = pl.pallas_call(
        put_kernel,
        name="put",
        out_shape=outs,
        in_specs=[pl.BlockSpec(memory_space=pltpu.VMEM)] * 5,
        out_specs=[hbm] * 5,
        scratch_shapes=[pltpu.SemaphoreType.DMA((5,))],
    )(*[pltpu.with_memory_space_constraint(o, pltpu.VMEM) for o in out])
    return (dx.reshape(1, MICRO, ROWS, W), gg[None], ug[None], dg.T[None], gn)


def solution(mesh):
    return jax.shard_map(
        body,
        mesh=mesh,
        in_specs=(
            P("section", None, "fsdp", "tp"),
            P(None, "fsdp", "tp"),
            P("section", None),
            P("section", "fsdp", "tp"),
            P("section", "fsdp", "tp"),
            P("section", "tp", "fsdp"),
        ),
        out_specs=(
            P("section", None, "fsdp", "tp"),
            P("section", "fsdp", "tp"),
            P("section", "fsdp", "tp"),
            P("section", "tp", "fsdp"),
            P("section", "tp"),
        ),
        check_vma=False,
    )
```

```python
import jax
import jax.numpy as jnp
from jax import lax
from jax.experimental import pallas as pl
from jax.experimental.pallas import tpu as pltpu
from jax.sharding import PartitionSpec as P

EPS = 1e-05
MESH = pl.DeviceIdType.MESH
F32 = jnp.float32
BF16 = jnp.bfloat16

NY, NXH, NZ, NXL = 4, 2, 8, 2
NF, NT = NY * NXH, NZ * NXL
MICRO = 8
ROWS = 64
T = MICRO * ROWS
H = 2
TH = T // H
W = 160
PW = NXL * W
FL = 432
GU = 2 * FL
D = W * NT
UW = 896
DH = 384
DR = PW + 16
NCOMMON = 79
NEACH = 48
NBIG = 16
NSMALL = 20


def dot(a, b, ca, cb, precision=None):
    return lax.dot_general(
        a, b, (((ca,), (cb,)), ((), ())), preferred_element_type=F32, precision=precision
    )


def fused_kernel(
    x_hbm,
    tg_hbm,
    gain_hbm,
    wg_hbm,
    wu_hbm,
    wd_hbm,
    dx_ref,
    gg_ref,
    ug_ref,
    dg_ref,
    gn_ref,
    x_ref,
    tg_ref,
    gain_row,
    wg_ref,
    wu_ref,
    wd_ref,
    gain,
    gain_sq,
    gain_all,
    x_all,
    wgu,
    wd,
    n_all,
    dy_all,
    gu,
    dh,
    dgu,
    hid,
    hid_mid,
    unit,
    scale,
    stat,
    ssq_in,
    stat_in,
    gain_in,
    pdn,
    rdn,
    pf,
    pown,
    gx,
    nstat,
    xs,
    xr,
    dxs,
    sgu,
    rgu,
    fgu,
    sgd,
    rgd,
    fgd,
    ssem,
    rsem,
    lsem,
    go,
):
    s = lax.axis_index("section")
    f = lax.axis_index("fsdp")
    t = lax.axis_index("tp")
    y, xh = lax.div(f, NXH), lax.rem(f, NXH)
    z, xl = lax.div(t, NXL), lax.rem(t, NXL)
    oh, ol = 1 - xh, 1 - xl

    def at_y(step):
        return (s, lax.rem(y + step + NY, NY) * NXH + xh, t)

    def at_z(step):
        return (s, f, lax.rem(z + step + NZ, NZ) * NXL + xl)

    dev = {
        "y+": at_y(1),
        "y-": at_y(-1),
        "z+": at_z(1),
        "z-": at_z(-1),
        "xh": (s, y * NXH + oh, t),
        "xl": (s, f, z * NXL + ol),
        "core": (1 - s, f, t),
    }
    across = {
        "core": (1 - s, f, t),
        "xl": (1 - s, *dev["xl"][1:]),
        "z+": (1 - s, *dev["z+"][1:]),
        "z-": (1 - s, *dev["z-"][1:]),
    }
    tp_peers = [(s, f, lax.rem(t + k, NT)) for k in range(1, NT)]
    fs_peers = [(s, lax.rem(f + k, NF), t) for k in range(1, NF)]
    zblk = [lax.rem(z + k, NZ) for k in range(NZ)]
    own, left, right, far = (
        {"c": lax.rem(y + k, NY) * NXH + xh, "o": lax.rem(y + k, NY) * NXH + oh} for k in (0, 3, 1, 2)
    )

    ids = {}
    size = {None: 0, 0: 0, 1: 0}
    private = {"dy": 1, "n": 1, "m": 0, "e": 0}
    ctx = [None]

    def ident(name, n=1):
        if name not in ids:
            sec = private.get(name[0])
            ids[name] = size[sec] + (0 if sec is None else NCOMMON)
            size[sec] += n
            assert size[sec] <= (NCOMMON if sec is None else NEACH), size
        return ids[name]

    def copy(src, dst, sm, rm, to):
        return pltpu.make_async_remote_copy(
            src_ref=src,
            dst_ref=dst,
            send_sem=ssem.at[sm],
            recv_sem=rsem.at[rm],
            device_id=to,
            device_id_type=MESH,
        )

    def static(idx):
        return tuple(i if isinstance(i, (int, pl.Slice)) else 0 for i in idx)

    turn = {sec: {"big": 0, "small": 0} for sec in (0, 1)}
    flying = {0: {}, 1: {}}

    def left_all(kind=None):
        mine = flying[ctx[0]]
        for m in sorted(mine):
            if kind is None or (m < NBIG) == (kind == "big"):
                src, si = mine.pop(m)
                r = src.at[si]
                copy(r, r, m, 0, dev["core"]).wait_send()

    def take(src, si, kind):
        mine, sec = flying[ctx[0]], ctx[0]
        base, n = (0, NBIG) if kind == "big" else (NBIG, NSMALL)
        m = base + turn[sec][kind] % n
        turn[sec][kind] += 1
        if m in mine:
            was, wi = mine.pop(m)
            r = was.at[wi]
            copy(r, r, m, 0, dev["core"]).wait_send()
        mine[m] = (src, static(si))
        return m

    def send(src, si, dst, di, name, to, q=None, kind="small"):
        rm = ident(name, 1 if q is None else 2)
        sm = take(src, si, kind)
        copy(src.at[si], dst.at[di], sm, rm if q is None else rm + q, to).start()

    def arrived(dst, di, name, q=None):
        m = ident(name, 1 if q is None else 2)
        r = dst.at[di]
        copy(r, r, 0, m if q is None else m + q, dev["core"]).wait_recv()

    def rows(n, step, fn):
        def body(i, c):
            fn(pl.multiple_of(i * step, step))
            return c

        lax.fori_loop(0, n // step, body, 0)

    barrier = pltpu.get_barrier_semaphore()
    everyone = tp_peers[4:11] + tp_peers[:4] + tp_peers[11:] + fs_peers + list(across.values())
    for to in everyone:
        pl.semaphore_signal(barrier, inc=1, device_id=to, device_id_type=MESH)

    loads = [
        pltpu.make_async_copy(src, dst, lsem.at[k])
        for k, (src, dst) in enumerate(
            (
                (x_hbm, x_ref),
                (tg_hbm, tg_ref),
                (gain_hbm, gain_row),
                (wd_hbm, wd_ref),
                (wg_hbm, wg_ref),
                (wu_hbm, wu_ref),
            )
        )
    ]
    for c in loads:
        c.start()
    eye = (
        lax.broadcasted_iota(jnp.int32, (W, W), 0) == lax.broadcasted_iota(jnp.int32, (W, W), 1)
    ).astype(BF16)
    loads[0].wait()
    xt = dot(eye, x_ref[...], 1, 1)
    ssq_in[t] = jnp.sum(xt * xt, axis=0, keepdims=True)
    unit[...] = xt
    loads[1].wait()

    @pl.when(s == 1)
    def _():
        x_all[z, xl] = xt.astype(BF16)
        top = dot(eye, tg_ref[...], 1, 1).astype(BF16)
        for h in range(H):
            dy_all[z, xl, h] = top[:, h * TH : (h + 1) * TH]

    def pack_d():
        loads[3].wait()

        def pack(r):
            wd[f, pl.ds(r, 32), :] = wd_ref[pl.ds(r, 32), 0:DH]
            wgu[f, pl.ds(r, 32), GU:UW] = wd_ref[pl.ds(r, 32), DH : DH + 32]

        rows(PW, 32, pack)
        last = (
            lax.broadcasted_iota(jnp.int32, (16, FL), 0) + (FL - 16)
            == lax.broadcasted_iota(jnp.int32, (16, FL), 1)
        ).astype(BF16)
        wd[f, PW:DR, 0:PW] = dot(last, wd_ref[...], 1, 1).astype(BF16)

    def pack_u():
        loads[4].wait()
        loads[5].wait()

        def pack(r):
            wgu[f, pl.ds(r, 32), 0:FL] = wg_ref[pl.ds(r, 32), :]
            wgu[f, pl.ds(r, 32), FL:GU] = wu_ref[pl.ds(r, 32), :]

        rows(PW, 32, pack)

    def take_gain():
        loads[2].wait()
        gain_sq[...] = jnp.zeros_like(gain_sq)
        for c in range(D // 128):
            gain_sq[c : c + 1, :] = gain_row[:, c * 128 : (c + 1) * 128]
        cols = gain_sq[...].T
        for c in range(D // 128):
            gain_all[c * 128 : (c + 1) * 128, :] = jnp.broadcast_to(cols[:, c : c + 1], (128, 128))
        gain[...] = gain_all[pl.ds(pl.multiple_of(t * W, 8), W), :]

    def spread(buf, me, peers, name):
        m = ident((name,))
        for to in peers:
            copy(buf.at[me], buf.at[me], NBIG + NSMALL + ("ssq", "stat", "gain").index(name), m, to).start()

    def collect(buf, peers, name):
        n = len(peers)
        r = buf.at[pl.ds(0, n)]
        copy(r, r, 0, ident((name,)), dev["core"]).wait_recv()
        total = buf[0]
        for k in range(1, n + 1):
            total = total + buf[k]
        return total

    def spread_left(buf, peers, name):
        r = buf.at[pl.ds(0, len(peers))]
        copy(r, r, NBIG + NSMALL + ("ssq", "stat", "gain").index(name), 0, dev["core"]).wait_send()

    pack_d()
    pack_u()

    pl.semaphore_wait(barrier, len(everyone))
    spread(ssq_in, t, tp_peers, "ssq")

    halves = {"u": ((0, 160), (160, 160)), "d": ((0, 160), (160, 176))}
    full = {"u": wgu, "d": wd}

    def w_own_x(a):
        send(full[a], (f,), full[a], (f,), ("w", a, "own", "xh"), dev["xh"], kind="big")

    def w_own_y(a, *parts):
        for i in parts:
            for d, k in (("y+", i), ("y-", 1 - i)):
                at = (f, pl.ds(*halves[a][k]))
                send(full[a], at, full[a], at, ("w", a, "own", d, i), dev[d], kind="big")

    def w_fwd(a):
        arr = full[a]
        for d, blk, k in (("y+", left["c"], 0), ("y-", right["c"], 1)):
            at = (blk, pl.ds(*halves[a][k]))
            arrived(arr, at, ("w", a, "own", d, 0))
            send(arr, at, arr, at, ("w", a, "fwd", d), dev[d], kind="big")

    def w_pass(a):
        arr, blk = full[a], own["o"]
        arrived(arr, (blk,), ("w", a, "own", "xh"))
        for d in ("y+", "y-"):
            send(arr, (blk,), arr, (blk,), ("w", a, "pass", d), dev[d], kind="big")

    def w_far(a):
        arr, blk = full[a], far["c"]
        for d, k in (("y+", 0), ("y-", 1)):
            arrived(arr, (blk, pl.ds(*halves[a][k])), ("w", a, "fwd", d))
        send(arr, (blk,), arr, (blk,), ("w", a, "far"), dev["xh"], kind="big")

    def w_last(a):
        arr = full[a]
        arrived(arr, (left["o"],), ("w", a, "pass", "y+"))
        arrived(arr, (right["o"],), ("w", a, "pass", "y-"))
        arrived(arr, (far["o"],), ("w", a, "far"))
        for d, blk, k in (("y+", left["c"], 1), ("y-", right["c"], 0)):
            arrived(arr, (blk, pl.ds(*halves[a][k])), ("w", a, "own", d, 1))

    def ag_xl(buf, nm):
        send(buf, (z, xl), buf, (z, xl), (nm, "xl"), dev["xl"])

    def ag_z(buf, nm):
        for d in ("z+", "z-"):
            send(buf, (z, xl), buf, (z, xl), (nm, d, 1, 0), dev[d])

    def ag_own(buf, nm):
        ag_xl(buf, nm)
        ag_z(buf, nm)

    def ag_partner(buf, nm, hh=()):
        at = (z, ol, *hh)
        arrived(buf, at, (nm, "xl", *hh))
        send(buf, at, buf, at, (nm, "z+", 1, 1, *hh), dev["z+"])
        send(buf, at, buf, at, (nm, "z-", 1, 1, *hh), dev["z-"])

    def ag_fwd(buf, nm, k, j, hh=()):
        q = (xl, ol)[j]
        for d, blk in (("z+", zblk[NZ - k]), ("z-", zblk[k])):
            at = (blk, q, *hh)
            arrived(buf, at, (nm, d, k, j, *hh))
            send(buf, at, buf, at, (nm, d, k + 1, j, *hh), dev[d])

    def ag_fwd3(buf, nm, hh=()):
        for d, blk, q in (("z+", zblk[5], 0), ("z-", zblk[3], 1)):
            for j in range(2):
                arrived(buf, (blk, (xl, ol)[j], *hh), (nm, d, 3, j, *hh))
            send(buf, (blk, q, *hh), buf, (blk, q, *hh), (nm, d, 4, *hh), dev[d])

    def ag_last(buf, nm, hh=()):
        arrived(buf, (zblk[4], 0, *hh), (nm, "z+", 4, *hh))
        arrived(buf, (zblk[4], 1, *hh), (nm, "z-", 4, *hh))

    def pair_send(buf, nm, *ks):
        for k in ks:
            at = (zblk[k], xl)
            send(buf, at, buf, at, (nm, "pair", k), dev["xl"])

    def pair_wait(buf, nm, *ks):
        for k in ks:
            arrived(buf, (zblk[k], ol), (nm, "pair", k))

    def own_wait(buf, nm, k):
        for d, b in (("z+", zblk[NZ - k]), ("z-", zblk[k])):
            arrived(buf, (b, xl), (nm, d, k, 0))

    def z_send(buf, nm, k, j):
        for d, b in (("z+", zblk[NZ - k]), ("z-", zblk[k])):
            at = (b, (xl, ol)[j])
            send(buf, at, buf, at, (nm, d, k + 1, j), dev[d])

    def act(buf, i):
        return jnp.concatenate([buf[i, :, h].reshape(PW, TH) for h in range(H)], axis=1)

    def pick(i, table):
        v = table[0]
        for k in range(1, len(table)):
            v = jnp.where(i == k, table[k], v)
        return v

    def together(parts):
        return jnp.concatenate(parts, axis=0)

    def forward(*ks):
        blks = [zblk[k] for k in ks]
        part = dot(
            together([wgu[b] for b in blks]),
            together([n_all[b].reshape(PW, T) for b in blks]),
            0,
            0,
        )
        gu[...] = part if 0 in ks else gu[...] + part

    def dhidden(*ks):
        blks = [zblk[k] for k in ks]
        dys = [act(dy_all, b) for b in blks]
        dy = together(dys)
        parts = (
            (0, dot(together([wd[b, 0:PW] for b in blks]), dy, 0, 0)),
        )
        for r, part in parts:
            at = pl.ds(r, part.shape[0])
            dh[at, :] = part if 0 in ks else dh[at, :] + part
        part = dot(wd[blks[0], PW:DR, 0:PW], dys[0], 1, 0)
        for b, d in zip(blks[1:], dys[1:]):
            part = part + dot(wd[b, PW:DR, 0:PW], d, 1, 0)
        at = pl.ds(DH + 128, 16)
        dh[at, :] = part if 0 in ks else dh[at, :] + part

    def dhidden_mid():
        lhs = together([wgu[b, :, UW - 128 : UW] for b in range(NF)])
        dh[DH : DH + 128, :] = dot(lhs, together([act(dy_all, b) for b in range(NF)]), 0, 0)

    def hidden():
        def body(r):
            gate = gu[pl.ds(r, 16), :]
            up = gu[pl.ds(pl.multiple_of(FL + r, 16), 16), :]
            hid[pl.ds(r, 16), :] = (gate * jax.nn.sigmoid(gate) * up).astype(BF16)

        rows(FL, 48, lambda r: [body(pl.multiple_of(r + k, 16)) for k in (0, 16, 32)])
        hid_mid[0:96, :] = jnp.zeros((96, T), BF16)
        hid_mid[96:128, :] = hid[DH : DH + 32, :]

    def normalize():
        row_scale = lax.rsqrt(collect(ssq_in, tp_peers, "ssq") / D + EPS)
        scale[...] = row_scale
        unit[...] = unit[...] * row_scale

    def norm_own():
        n_all[z, xl] = (unit[...] * gain[:, 0:1]).astype(BF16)

    def norm_blocks(*ks):
        for k in ks:
            b = zblk[k]
            for q in range(NXL):
                g = gain_all[pl.ds(pl.multiple_of(b * PW + q * W, 8), W), :]
                for c in range(T // 128):
                    at = slice(c * 128, (c + 1) * 128)
                    n_all[b, q, :, at] = (
                        x_all[b, q, :, at].astype(F32) * scale[:, at] * g
                    ).astype(BF16)

    def cotangents():
        stat[...] = jnp.zeros_like(stat)
        dgu[GU:UW, :] = jnp.zeros((UW - GU, T), BF16)

        def elementwise(r):
            gate = gu[pl.ds(r, 16), :]
            up = gu[pl.ds(pl.multiple_of(FL + r, 16), 16), :]
            dd = dh[pl.ds(pl.multiple_of(jnp.where(r < DH, r, r + 96), 16), 16), :]
            sig = jax.nn.sigmoid(gate)
            silu = gate * sig
            d_gate = (dd * up * sig * (1.0 + gate * (1.0 - sig))).astype(BF16)
            d_up = (dd * silu).astype(BF16)
            dgu[pl.ds(r, 16), :] = d_gate
            dgu[pl.ds(pl.multiple_of(FL + r, 16), 16), :] = d_up
            both = d_gate.astype(F32) * gate + d_up.astype(F32) * up
            stat[...] += both[0:8] + both[8:16]

        rows(FL, 48, lambda r: [elementwise(pl.multiple_of(r + k, 16)) for k in (0, 16, 32)])
        stat_in[t] = jnp.sum(stat[...], axis=0, keepdims=True)
        spread(stat_in, t, tp_peers, "stat")

    ways = (("z+", 0), ("z-", 1))

    def rs_first():
        def body(h, c):
            part = dot(wgu[zblk[4], :, 0:GU], dgu[0:GU, :], 1, 0).reshape(NXL, W, T)
            for hh in range(H):
                pdn[0, hh] = part[:, :, hh * TH : (hh + 1) * TH].astype(BF16)
            return c

        lax.fori_loop(0, 1, body, 0)
        for h in range(H):
            for d, w in ways:
                send(pdn, (0, h, w), rdn, (w, 0, h, w), ("rs", d, 1, h), dev[d], q=w)

    def rs_compute(k):
        def body(w, c):
            blk = jnp.where(w == 0, zblk[5 - k], zblk[3 + k])
            part = dot(wgu[blk, :, 0:GU], dgu[0:GU, :], 1, 0).reshape(NXL, W, T)
            for hh in range(H):
                pf[k - 2, w, hh] = part[:, :, hh * TH : (hh + 1) * TH]
            return c

        lax.fori_loop(0, 2, body, 0)

    def rs_free():
        for h in range(H):
            for d, w in ways:
                q = 1 - w
                pdn[1 + w, h, q] = pf[0, w, h, q].astype(BF16)
                send(pdn, (1 + w, h, q), rdn, (w, 1, h, q), ("rs", d, 2, h), dev[d], q=q)

    def rs_step(k, ahead=(True, False), hs=range(H)):
        slot = 2 * k - 3
        for first in ahead:
            for h in hs:
                for d, w in ways:
                    q = 1 - w if first else w
                    arrived(rdn, (w, k - 2, h, q), ("rs", d, k - 1, h), q=q)
                    pdn[slot + w, h, q] = (
                        pf[k - 2, w, h, q] + rdn[w, k - 2, h, q].astype(F32)
                    ).astype(BF16)
                    send(pdn, (slot + w, h, q), rdn, (w, k - 1, h, q), ("rs", d, k, h), dev[d], q=q)

    def rs_own():
        def body(h, c):
            part = dot(wgu[z, :, 0:GU], dgu[0:GU, :], 1, 0).reshape(NXL, W, T)
            for hh in range(H):
                pown[hh] = part[:, :, hh * TH : (hh + 1) * TH]
            return c

        lax.fori_loop(0, 1, body, 0)

    def rs_last(h):
        for q in (ol, xl):
            for d, w in ways:
                arrived(rdn, (w, 3, h, q), ("rs", d, 4, h), q=q)
            if q is ol:
                xs[h] = (
                    pown[h, q] + rdn[0, 3, h, q].astype(F32) + rdn[1, 3, h, q].astype(F32)
                ).astype(BF16)
                send(xs, (h,), xr, (h,), ("rx", h), dev["xl"])

    def take_stat():
        nstat[...] = collect(stat_in, tp_peers, "stat") / D

    def dx_part(h):
        arrived(xr, (h,), ("rx", h))
        cols = slice(h * TH, (h + 1) * TH)
        d_normed = (
            pown[h, xl]
            + rdn[0, 3, h, xl].astype(F32)
            + rdn[1, 3, h, xl].astype(F32)
            + xr[h].astype(F32)
        )
        u = unit[:, cols]
        dx = dy_all[z, xl, h].astype(F32) + scale[:, cols] * (
            d_normed * gain[:, 0:1] - u * nstat[:, cols]
        )
        dxs[h] = dx.astype(BF16)
        gx[h] = d_normed * u

    def dx_send(h):
        dx_part(h)
        for d, name in (
            ("xl", ("xl", h)),
            ("z+", ("z+", 1, 0, h)),
            ("z-", ("z-", 1, 0, h)),
            ("core", ("core", h)),
        ):
            send(dxs, (h,), dy_all, (z, xl, h), ("e", *name), across[d])

    def gain_dx():
        total = dot(
            jnp.ones((8, T), F32),
            jnp.concatenate([gx[h] for h in range(H)], axis=1),
            1,
            1,
            lax.Precision.HIGHEST,
        )
        gain_in[f] = total
        spread(gain_in, f, fs_peers, "gain")
        for h in range(H):
            dx_ref[h * TH : (h + 1) * TH, :] = dot(dxs[h], eye, 0, 0).astype(BF16)

    sg, rg, fg = {"u": sgu, "d": sgd}, {"u": rgu, "d": rgd}, {"u": fgu, "d": fgd}
    size_of = {"u": (PW, 32), "d": (DR, 48)}

    def wgrad(a, blk, dst, i):
        dy = act(dy_all, blk)
        if a == "u":
            cut = UW - 128
            n = n_all[blk].reshape(PW, T)
            dst[i, :, 0:cut] = dot(n, dgu[0:cut, :], 1, 1).astype(dst.dtype)
            edge = dot(n, dgu[cut:UW, :], 1, 1) + dot(dy, hid_mid[...], 1, 1)
            dst[i, :, cut:UW] = edge.astype(dst.dtype)
        else:
            dst[i, 0:PW, :] = dot(dy, hid[0:DH, :], 1, 1).astype(dst.dtype)
            dst[i, PW:DR, 0:PW] = dot(hid[FL - 16 : FL, :], dy, 1, 1).astype(dst.dtype)

    direct = [right["o"], left["o"], far["o"]]
    kept = [far["c"], own["o"], right["c"], left["c"], own["c"]]

    def g_first(a, lo=0, hi=3):
        rm = ident(("g", a, 0), 3)
        sm = [take(sg[a], (0,), "big") if lo <= i < hi else 0 for i in range(3)]

        def body(i, c):
            wgrad(a, pick(i, direct), sg[a], i)
            to = pick(i, [dev[d][1] for d in ("y+", "y-", "xh")])
            copy(sg[a].at[i], rg[a].at[i], pick(i, sm), rm + i, (s, to, t)).start()
            return c

        lax.fori_loop(lo, hi, body, 0)

    def g_kept(a, lo, hi):
        def body(i, c):
            wgrad(a, pick(i, kept), fg[a], i)
            return c

        lax.fori_loop(lo, hi, body, 0)

    def g_sum(a, slot, own_i, recv, span=None):
        n, st = size_of[a]
        lo, n = span if span else (0, n)
        st = 16 if span else st

        def body(r):
            r = pl.multiple_of(r + lo, 16)
            v = fg[a][own_i, pl.ds(r, st), :]
            for k in recv:
                v = v + rg[a][k, pl.ds(r, st), :].astype(F32)
            sg[a][slot, pl.ds(r, st), :] = v.astype(BF16)

        rows(n, st, body)

    def g_far(a):
        arrived(rg[a], (2,), ("g", a, 0), q=2)
        g_sum(a, 3, 0, (2,))
        for d, k in (("y+", 0), ("y-", 1)):
            part = pl.ds(*halves[a][k])
            send(sg[a], (3, part), rg[a], (3, part), ("g", a, 3, d), dev[d], kind="big")

    def g_near(a, waits):
        for d, k, slot in (("y+", 0, 4), ("y-", 1, 5)):
            half = halves[a][k if waits else 1 - k]
            part = pl.ds(*half)
            if waits:
                arrived(rg[a], (3, part), ("g", a, 3, d))
            g_sum(a, slot, 2 + k, (3,) if waits else (), half)
            send(sg[a], (slot, part), rg[a], (slot, part), ("g", a, slot, waits), dev[d], kind="big")

    def g_partner(a):
        arrived(rg[a], (0,), ("g", a, 0), q=0)
        arrived(rg[a], (1,), ("g", a, 0), q=1)
        g_sum(a, 6, 1, (0, 1))
        send(sg[a], (6,), rg[a], (6,), ("g", a, 6), dev["xh"], kind="big")

    def g_most(a):
        for k in (0, 1):
            part = pl.ds(*halves[a][1 - k])
            arrived(rg[a], (4 + k, part), ("g", a, 4 + k, False))
        arrived(rg[a], (6,), ("g", a, 6))
        for k in (0, 1):
            lo, n = halves[a][1 - k]

            def body(r, k=k, lo=lo):
                at = pl.ds(pl.multiple_of(r + lo, 16), 16)
                fg[a][4, at, :] += rg[a][4 + k, at, :].astype(F32) + rg[a][6, at, :].astype(F32)

            rows(n, 16, body)

    def g_last(a):
        for k in (0, 1):
            lo, n = halves[a][k]
            arrived(rg[a], (4 + k, pl.ds(lo, n)), ("g", a, 4 + k, True))

            def total(at, k=k):
                return fg[a][4, at, :] + rg[a][4 + k, at, :].astype(F32)

            def body(r, total=total, lo=lo):
                at = pl.ds(pl.multiple_of(r + lo, 16), 32)
                v = total(at)
                if a == "u":
                    gg_ref[at, :] = v[:, 0:FL]
                    ug_ref[at, :] = v[:, FL:GU]
                    dg_ref[at, DH : DH + 32] = v[:, GU:UW]
                else:
                    dg_ref[at, 0:DH] = v

            rows(160, 32, body)
            if n > 160:
                v = total(pl.ds(PW, 16))[:, 0:PW]
                unit16 = (
                    lax.broadcasted_iota(jnp.int32, (16, 16), 0)
                    == lax.broadcasted_iota(jnp.int32, (16, 16), 1)
                ).astype(F32)
                dg_ref[:, DH + 32 : FL] = dot(v, unit16, 0, 0, lax.Precision.HIGHEST)

    def finish():
        gn_ref[...] = collect(gain_in, fs_peers, "gain")[0:1]
        left_all()

    @pl.when(s == 1)
    def _():
        ctx[0] = 1
        ag_own(dy_all, "dy")
        ag_own(x_all, "n")
        w_own_x("d")
        w_own_y("d", 0, 1)
        w_own_y("u", 0, 1)
        w_own_x("u")
        take_gain()
        ag_partner(dy_all, "dy")
        ag_fwd(dy_all, "dy", 1, 0)
        normalize()
        ag_partner(x_all, "n")
        ag_fwd(x_all, "n", 1, 0)
        w_fwd("d")
        ag_fwd(dy_all, "dy", 1, 1)
        ag_fwd(dy_all, "dy", 2, 0)
        w_fwd("u")
        w_pass("d")
        ag_fwd(x_all, "n", 1, 1)
        ag_fwd(x_all, "n", 2, 0)
        w_far("d")
        norm_blocks(0, 1, 7)
        ag_fwd(dy_all, "dy", 2, 1)
        w_pass("u")
        w_far("u")
        ag_fwd(x_all, "n", 2, 1)
        norm_blocks(2, 6)
        ag_fwd3(dy_all, "dy")
        w_last("d")
        dhidden(0, 1, 7)
        ag_fwd3(x_all, "n")
        pl.semaphore_signal(go, inc=1, device_id=dev["core"], device_id_type=MESH)
        norm_blocks(3, 5)
        dhidden(2, 6, 3, 5)
        pl.semaphore_signal(go, inc=1, device_id=dev["core"], device_id_type=MESH)
        w_last("u")
        forward(0, 1, 7)
        forward(2, 6, 3, 5)
        ag_last(x_all, "n")
        norm_blocks(4)
        forward(4)
        ag_last(dy_all, "dy")
        dhidden(4)
        dhidden_mid()
        cotangents()
        rs_first()
        rs_compute(2)
        rs_free()
        rs_step(2, (False,), (0,))
        hidden()
        rs_compute(3)
        rs_step(2, (False,), (1,))
        left_all("big")
        g_first("u", 0, 1)
        rs_step(3, (True,), (0,))
        rs_step(3, (True,), (1,))
        rs_step(3, (False,), (0,))
        rs_compute(4)
        rs_step(3, (False,), (1,))
        g_first("u", 1, 2)
        rs_step(4, (True,), (0,))
        rs_own()
        rs_step(4, (False,), (0,))
        rs_step(4, (False,), (1,))
        rs_step(4, (True,), (1,))
        g_kept("d", 0, 1)
        rs_last(0)
        pl.semaphore_signal(go, inc=1, device_id=dev["core"], device_id_type=MESH)
        g_first("d", 1, 2)
        g_kept("d", 1, 2)
        rs_last(1)
        g_first("d", 0, 1)
        take_stat()
        dx_send(0)
        dx_send(1)
        g_first("u", 2, 3)
        g_kept("u", 1, 2)
        g_kept("u", 0, 1)
        g_first("d", 2, 3)
        g_kept("u", 2, 4)
        g_near("u", False)
        gain_dx()
        g_partner("u")
        g_kept("d", 4, 5)
        g_kept("d", 2, 4)
        g_near("d", False)
        g_far("u")
        g_partner("d")
        g_kept("u", 4, 5)
        g_far("d")
        g_near("u", True)
        g_near("d", True)
        g_most("u")
        g_last("u")
        g_most("d")
        g_last("d")
        finish()
        ctx[0] = None

    @pl.when(s == 0)
    def _():
        ctx[0] = 0
        take_gain()
        normalize()
        norm_own()
        ag_xl(n_all, "m")
        pl.semaphore_wait(go, 1)
        w_own_x("d")
        w_own_y("d", 0, 1)
        w_own_y("u", 0)
        w_own_x("u")
        pl.semaphore_wait(go, 1)
        ag_z(n_all, "m")
        ag_partner(n_all, "m")
        w_fwd("d")
        w_own_y("u", 1)
        own_wait(n_all, "m", 1)
        z_send(n_all, "m", 1, 0)
        w_fwd("u")
        w_pass("d")
        w_far("d")
        own_wait(n_all, "m", 2)
        pair_send(n_all, "m", 2, 6)
        w_pass("u")
        w_far("u")
        pl.semaphore_wait(go, 1)
        z_send(n_all, "m", 2, 0)
        pair_wait(n_all, "m", 2, 6)
        z_send(n_all, "m", 2, 1)
        ag_partner(dy_all, "e", (0,))
        ag_partner(dy_all, "e", (1,))
        ag_fwd(dy_all, "e", 1, 0, (0,))
        ag_fwd(dy_all, "e", 1, 0, (1,))
        ag_fwd(dy_all, "e", 1, 1, (0,))
        ag_fwd(dy_all, "e", 1, 1, (1,))
        w_last("d")
        w_last("u")
        for h in range(H):
            arrived(dy_all, (z, xl, h), ("e", "core", h))
        dhidden(0, 1, 7)
        ag_fwd(dy_all, "e", 2, 0, (0,))
        ag_fwd(dy_all, "e", 2, 0, (1,))
        ag_fwd(dy_all, "e", 2, 1, (0,))
        ag_fwd(dy_all, "e", 2, 1, (1,))
        ag_fwd3(n_all, "m")
        arrived(n_all, (zblk[7], ol), ("m", "z+", 1, 1))
        arrived(n_all, (zblk[1], ol), ("m", "z-", 1, 1))
        forward(0, 1, 7)
        ag_fwd3(dy_all, "e", (0,))
        ag_fwd3(dy_all, "e", (1,))
        forward(2, 6, 3, 5)
        ag_last(n_all, "m")
        forward(4)
        hidden()
        ag_last(dy_all, "e", (0,))
        dhidden(2, 6, 3, 5)
        ag_last(dy_all, "e", (1,))
        dhidden(4)
        dhidden_mid()
        cotangents()
        left_all("big")
        g_first("u", 0, 2)
        rs_first()
        g_first("u", 2, 3)
        rs_compute(2)
        rs_free()
        g_kept("u", 2, 4)
        g_near("u", False)
        g_first("d", 1, 2)
        rs_step(2, (False,), (0,))
        g_kept("u", 1, 2)
        rs_step(2, (False,), (1,))
        rs_compute(3)
        rs_step(3, (True,), (0,))
        g_first("d", 2, 3)
        g_first("d", 0, 1)
        rs_step(3, (True,), (1,))
        rs_compute(4)
        rs_step(3, (False,), (0,))
        rs_own()
        rs_step(3, (False,), (1,))
        g_partner("u")
        rs_step(4, (True,), (0,))
        g_kept("u", 0, 1)
        g_far("u")
        rs_step(4, (True,), (1,))
        g_kept("d", 0, 1)
        rs_step(4, (False,), (0,))
        g_kept("d", 4, 5)
        g_far("d")
        rs_step(4, (False,), (1,))
        g_kept("d", 1, 2)
        g_kept("d", 2, 4)
        g_near("d", False)
        rs_last(0)
        rs_last(1)
        g_near("u", True)
        g_partner("d")
        g_kept("u", 4, 5)
        g_near("d", True)
        take_stat()
        dx_part(0)
        g_most("u")
        dx_part(1)
        gain_dx()
        g_last("u")
        g_most("d")
        g_last("d")
        finish()
        ctx[0] = None

    spread_left(ssq_in, tp_peers, "ssq")
    spread_left(stat_in, tp_peers, "stat")
    spread_left(gain_in, fs_peers, "gain")


def put_kernel(*refs):
    copies = [pltpu.make_async_copy(refs[k], refs[5 + k], refs[10].at[k]) for k in range(5)]
    for c in copies:
        c.start()
    for c in copies:
        c.wait()


def body(saved_inputs, top_grad, norm_gain, gate_weight, up_weight, down_weight):
    x = saved_inputs.reshape(T, W)
    tg = top_grad.reshape(T, W)
    hbm = pl.BlockSpec(memory_space=pl.ANY)
    outs = (
        jax.ShapeDtypeStruct((T, W), BF16),
        jax.ShapeDtypeStruct((PW, FL), F32),
        jax.ShapeDtypeStruct((PW, FL), F32),
        jax.ShapeDtypeStruct((PW, FL), F32),
        jax.ShapeDtypeStruct((1, W), F32),
    )
    out = pl.pallas_call(
        fused_kernel,
        name="fused",
        out_shape=[pltpu.VMEM(o.shape, o.dtype) for o in outs],
        in_specs=[hbm] * 6,
        out_specs=[pl.BlockSpec(memory_space=pltpu.VMEM)] * 5,
        scratch_shapes=[
            pltpu.VMEM((T, W), BF16),
            pltpu.VMEM((T, W), BF16),
            pltpu.VMEM((1, D), F32),
            pltpu.VMEM((PW, FL), BF16),
            pltpu.VMEM((PW, FL), BF16),
            pltpu.VMEM((PW, FL), BF16),
            pltpu.VMEM((W, 128), F32),
            pltpu.VMEM((128, 128), F32),
            pltpu.VMEM((D, 128), F32),
            pltpu.VMEM((NZ, NXL, W, T), BF16),
            pltpu.VMEM((NF, PW, UW), BF16),
            pltpu.VMEM((NF, DR, DH), BF16),
            pltpu.VMEM((NZ, NXL, W, T), BF16),
            pltpu.VMEM((NZ, NXL, H, W, TH), BF16),
            pltpu.VMEM((UW, T), F32),
            pltpu.VMEM((DH + 128 + 16, T), F32),
            pltpu.VMEM((UW, T), BF16),
            pltpu.VMEM((FL, T), BF16),
            pltpu.VMEM((128, T), BF16),
            pltpu.VMEM((W, T), F32),
            pltpu.VMEM((1, T), F32),
            pltpu.VMEM((8, T), F32),
            pltpu.VMEM((NT, 1, T), F32),
            pltpu.VMEM((NT, 1, T), F32),
            pltpu.VMEM((NF, 8, W), F32),
            pltpu.VMEM((7, H, NXL, W, TH), BF16),
            pltpu.VMEM((2, 4, H, NXL, W, TH), BF16),
            pltpu.VMEM((3, 2, H, NXL, W, TH), F32),
            pltpu.VMEM((H, NXL, W, TH), F32),
            pltpu.VMEM((H, W, TH), F32),
            pltpu.VMEM((1, T), F32),
            pltpu.VMEM((H, W, TH), BF16),
            pltpu.VMEM((H, W, TH), BF16),
            pltpu.VMEM((H, W, TH), BF16),
            pltpu.VMEM((7, PW, UW), BF16),
            pltpu.VMEM((7, PW, UW), BF16),
            pltpu.VMEM((5, PW, UW), F32),
            pltpu.VMEM((7, DR, DH), BF16),
            pltpu.VMEM((7, DR, DH), BF16),
            pltpu.VMEM((5, DR, DH), F32),
            pltpu.SemaphoreType.DMA((NBIG + NSMALL + 3,)),
            pltpu.SemaphoreType.DMA((NCOMMON + NEACH,)),
            pltpu.SemaphoreType.DMA((6,)),
            pltpu.SemaphoreType.REGULAR,
        ],
        compiler_params=pltpu.CompilerParams(
            collective_id=0, has_side_effects=True, vmem_limit_bytes=58 * 2**20
        ),
    )(x, tg, norm_gain, gate_weight[0], up_weight[0], down_weight[0].T)
    dx, gg, ug, dg, gn = pl.pallas_call(
        put_kernel,
        name="put",
        out_shape=outs,
        in_specs=[pl.BlockSpec(memory_space=pltpu.VMEM)] * 5,
        out_specs=[hbm] * 5,
        scratch_shapes=[pltpu.SemaphoreType.DMA((5,))],
    )(*[pltpu.with_memory_space_constraint(o, pltpu.VMEM) for o in out])
    return (dx.reshape(1, MICRO, ROWS, W), gg[None], ug[None], dg.T[None], gn)


def solution(mesh):
    return jax.shard_map(
        body,
        mesh=mesh,
        in_specs=(
            P("section", None, "fsdp", "tp"),
            P(None, "fsdp", "tp"),
            P("section", None),
            P("section", "fsdp", "tp"),
            P("section", "fsdp", "tp"),
            P("section", "tp", "fsdp"),
        ),
        out_specs=(
            P("section", None, "fsdp", "tp"),
            P("section", "fsdp", "tp"),
            P("section", "fsdp", "tp"),
            P("section", "tp", "fsdp"),
            P("section", "tp"),
        ),
        check_vma=False,
    )
```

```python
import jax
import jax.numpy as jnp
from jax import lax
from jax.experimental import pallas as pl
from jax.experimental.pallas import tpu as pltpu
from jax.sharding import PartitionSpec as P

EPS = 1e-05
MESH = pl.DeviceIdType.MESH
F32 = jnp.float32
BF16 = jnp.bfloat16

NY, NXH, NZ, NXL = 4, 2, 8, 2
NF, NT = NY * NXH, NZ * NXL
MICRO = 8
ROWS = 64
T = MICRO * ROWS
H = 2
TH = T // H
W = 160
PW = NXL * W
FL = 432
GU = 2 * FL
D = W * NT
UW = 896
DH = 384
DR = PW + 16
NCOMMON = 79
NEACH = 48
NBIG = 16
NSMALL = 20


def dot(a, b, ca, cb, precision=None):
    return lax.dot_general(
        a, b, (((ca,), (cb,)), ((), ())), preferred_element_type=F32, precision=precision
    )


def fused_kernel(
    x_hbm,
    tg_hbm,
    gain_hbm,
    wg_hbm,
    wu_hbm,
    wd_hbm,
    dx_ref,
    gg_ref,
    ug_ref,
    dg_ref,
    gn_ref,
    x_ref,
    tg_ref,
    gain_row,
    wg_ref,
    wu_ref,
    wd_ref,
    gain,
    gain_sq,
    gain_all,
    x_all,
    wgu,
    wd,
    n_all,
    dy_all,
    gu,
    dh,
    dgu,
    hid,
    hid_mid,
    unit,
    scale,
    stat,
    ssq_in,
    stat_in,
    gain_in,
    pdn,
    rdn,
    pf,
    pown,
    gx,
    nstat,
    xs,
    xr,
    dxs,
    sgu,
    rgu,
    fgu,
    sgd,
    rgd,
    fgd,
    ssem,
    rsem,
    lsem,
    go,
):
    s = lax.axis_index("section")
    f = lax.axis_index("fsdp")
    t = lax.axis_index("tp")
    y, xh = lax.div(f, NXH), lax.rem(f, NXH)
    z, xl = lax.div(t, NXL), lax.rem(t, NXL)
    oh, ol = 1 - xh, 1 - xl

    def at_y(step):
        return (s, lax.rem(y + step + NY, NY) * NXH + xh, t)

    def at_z(step):
        return (s, f, lax.rem(z + step + NZ, NZ) * NXL + xl)

    dev = {
        "y+": at_y(1),
        "y-": at_y(-1),
        "z+": at_z(1),
        "z-": at_z(-1),
        "xh": (s, y * NXH + oh, t),
        "xl": (s, f, z * NXL + ol),
        "core": (1 - s, f, t),
    }
    across = {
        "core": (1 - s, f, t),
        "xl": (1 - s, *dev["xl"][1:]),
        "z+": (1 - s, *dev["z+"][1:]),
        "z-": (1 - s, *dev["z-"][1:]),
    }
    tp_peers = [(s, f, lax.rem(t + k, NT)) for k in range(1, NT)]
    fs_peers = [(s, lax.rem(f + k, NF), t) for k in range(1, NF)]
    zblk = [lax.rem(z + k, NZ) for k in range(NZ)]
    own, left, right, far = (
        {"c": lax.rem(y + k, NY) * NXH + xh, "o": lax.rem(y + k, NY) * NXH + oh} for k in (0, 3, 1, 2)
    )

    ids = {}
    size = {None: 0, 0: 0, 1: 0}
    private = {"dy": 1, "n": 1, "m": 0, "e": 0}
    ctx = [None]

    def ident(name, n=1):
        if name not in ids:
            sec = private.get(name[0])
            ids[name] = size[sec] + (0 if sec is None else NCOMMON)
            size[sec] += n
            assert size[sec] <= (NCOMMON if sec is None else NEACH), size
        return ids[name]

    def copy(src, dst, sm, rm, to):
        return pltpu.make_async_remote_copy(
            src_ref=src,
            dst_ref=dst,
            send_sem=ssem.at[sm],
            recv_sem=rsem.at[rm],
            device_id=to,
            device_id_type=MESH,
        )

    def static(idx):
        return tuple(i if isinstance(i, (int, pl.Slice)) else 0 for i in idx)

    turn = {sec: {"big": 0, "small": 0} for sec in (0, 1)}
    flying = {0: {}, 1: {}}

    def left_all(kind=None):
        mine = flying[ctx[0]]
        for m in sorted(mine):
            if kind is None or (m < NBIG) == (kind == "big"):
                src, si = mine.pop(m)
                r = src.at[si]
                copy(r, r, m, 0, dev["core"]).wait_send()

    def take(src, si, kind):
        mine, sec = flying[ctx[0]], ctx[0]
        base, n = (0, NBIG) if kind == "big" else (NBIG, NSMALL)
        m = base + turn[sec][kind] % n
        turn[sec][kind] += 1
        if m in mine:
            was, wi = mine.pop(m)
            r = was.at[wi]
            copy(r, r, m, 0, dev["core"]).wait_send()
        mine[m] = (src, static(si))
        return m

    def send(src, si, dst, di, name, to, q=None, kind="small"):
        rm = ident(name, 1 if q is None else 2)
        sm = take(src, si, kind)
        copy(src.at[si], dst.at[di], sm, rm if q is None else rm + q, to).start()

    def arrived(dst, di, name, q=None):
        m = ident(name, 1 if q is None else 2)
        r = dst.at[di]
        copy(r, r, 0, m if q is None else m + q, dev["core"]).wait_recv()

    def rows(n, step, fn):
        def body(i, c):
            fn(pl.multiple_of(i * step, step))
            return c

        lax.fori_loop(0, n // step, body, 0)

    barrier = pltpu.get_barrier_semaphore()
    everyone = tp_peers[4:11] + tp_peers[:4] + tp_peers[11:] + fs_peers + list(across.values())
    for to in everyone:
        pl.semaphore_signal(barrier, inc=1, device_id=to, device_id_type=MESH)

    loads = [
        pltpu.make_async_copy(src, dst, lsem.at[k])
        for k, (src, dst) in enumerate(
            (
                (x_hbm, x_ref),
                (tg_hbm, tg_ref),
                (gain_hbm, gain_row),
                (wd_hbm, wd_ref),
                (wg_hbm, wg_ref),
                (wu_hbm, wu_ref),
            )
        )
    ]
    for c in loads:
        c.start()
    eye = (
        lax.broadcasted_iota(jnp.int32, (W, W), 0) == lax.broadcasted_iota(jnp.int32, (W, W), 1)
    ).astype(BF16)
    loads[0].wait()
    xt = dot(eye, x_ref[...], 1, 1)
    ssq_in[t] = jnp.sum(xt * xt, axis=0, keepdims=True)
    unit[...] = xt
    loads[1].wait()

    @pl.when(s == 1)
    def _():
        x_all[z, xl] = xt.astype(BF16)
        top = dot(eye, tg_ref[...], 1, 1).astype(BF16)
        for h in range(H):
            dy_all[z, xl, h] = top[:, h * TH : (h + 1) * TH]

    def pack_d():
        loads[3].wait()

        def pack(r):
            wd[f, pl.ds(r, 32), :] = wd_ref[pl.ds(r, 32), 0:DH]
            wgu[f, pl.ds(r, 32), GU:UW] = wd_ref[pl.ds(r, 32), DH : DH + 32]

        rows(PW, 32, pack)
        last = (
            lax.broadcasted_iota(jnp.int32, (16, FL), 0) + (FL - 16)
            == lax.broadcasted_iota(jnp.int32, (16, FL), 1)
        ).astype(BF16)
        wd[f, PW:DR, 0:PW] = dot(last, wd_ref[...], 1, 1).astype(BF16)

    def pack_u():
        loads[4].wait()
        loads[5].wait()

        def pack(r):
            wgu[f, pl.ds(r, 32), 0:FL] = wg_ref[pl.ds(r, 32), :]
            wgu[f, pl.ds(r, 32), FL:GU] = wu_ref[pl.ds(r, 32), :]

        rows(PW, 32, pack)

    def take_gain():
        loads[2].wait()
        gain_sq[...] = jnp.zeros_like(gain_sq)
        for c in range(D // 128):
            gain_sq[c : c + 1, :] = gain_row[:, c * 128 : (c + 1) * 128]
        cols = gain_sq[...].T
        for c in range(D // 128):
            gain_all[c * 128 : (c + 1) * 128, :] = jnp.broadcast_to(cols[:, c : c + 1], (128, 128))
        gain[...] = gain_all[pl.ds(pl.multiple_of(t * W, 8), W), :]

    def spread(buf, me, peers, name):
        m = ident((name,))
        for to in peers:
            copy(buf.at[me], buf.at[me], NBIG + NSMALL + ("ssq", "stat", "gain").index(name), m, to).start()

    def collect(buf, peers, name):
        n = len(peers)
        r = buf.at[pl.ds(0, n)]
        copy(r, r, 0, ident((name,)), dev["core"]).wait_recv()
        total = buf[0]
        for k in range(1, n + 1):
            total = total + buf[k]
        return total

    def spread_left(buf, peers, name):
        r = buf.at[pl.ds(0, len(peers))]
        copy(r, r, NBIG + NSMALL + ("ssq", "stat", "gain").index(name), 0, dev["core"]).wait_send()

    pack_d()
    pack_u()

    pl.semaphore_wait(barrier, len(everyone))
    spread(ssq_in, t, tp_peers, "ssq")

    halves = {"u": ((0, 160), (160, 160)), "d": ((0, 160), (160, 176))}
    full = {"u": wgu, "d": wd}

    def w_own_x(a):
        send(full[a], (f,), full[a], (f,), ("w", a, "own", "xh"), dev["xh"], kind="big")

    def w_own_y(a, *parts):
        for i in parts:
            for d, k in (("y+", i), ("y-", 1 - i)):
                at = (f, pl.ds(*halves[a][k]))
                send(full[a], at, full[a], at, ("w", a, "own", d, i), dev[d], kind="big")

    def w_fwd(a):
        arr = full[a]
        for d, blk, k in (("y+", left["c"], 0), ("y-", right["c"], 1)):
            at = (blk, pl.ds(*halves[a][k]))
            arrived(arr, at, ("w", a, "own", d, 0))
            send(arr, at, arr, at, ("w", a, "fwd", d), dev[d], kind="big")

    def w_pass(a):
        arr, blk = full[a], own["o"]
        arrived(arr, (blk,), ("w", a, "own", "xh"))
        for d in ("y+", "y-"):
            send(arr, (blk,), arr, (blk,), ("w", a, "pass", d), dev[d], kind="big")

    def w_far(a):
        arr, blk = full[a], far["c"]
        for d, k in (("y+", 0), ("y-", 1)):
            arrived(arr, (blk, pl.ds(*halves[a][k])), ("w", a, "fwd", d))
        send(arr, (blk,), arr, (blk,), ("w", a, "far"), dev["xh"], kind="big")

    def w_last(a):
        arr = full[a]
        arrived(arr, (left["o"],), ("w", a, "pass", "y+"))
        arrived(arr, (right["o"],), ("w", a, "pass", "y-"))
        arrived(arr, (far["o"],), ("w", a, "far"))
        for d, blk, k in (("y+", left["c"], 1), ("y-", right["c"], 0)):
            arrived(arr, (blk, pl.ds(*halves[a][k])), ("w", a, "own", d, 1))

    def ag_xl(buf, nm):
        send(buf, (z, xl), buf, (z, xl), (nm, "xl"), dev["xl"])

    def ag_z(buf, nm):
        for d in ("z+", "z-"):
            send(buf, (z, xl), buf, (z, xl), (nm, d, 1, 0), dev[d])

    def ag_own(buf, nm):
        ag_xl(buf, nm)
        ag_z(buf, nm)

    def ag_partner(buf, nm, hh=()):
        at = (z, ol, *hh)
        arrived(buf, at, (nm, "xl", *hh))
        send(buf, at, buf, at, (nm, "z+", 1, 1, *hh), dev["z+"])
        send(buf, at, buf, at, (nm, "z-", 1, 1, *hh), dev["z-"])

    def ag_fwd(buf, nm, k, j, hh=()):
        q = (xl, ol)[j]
        for d, blk in (("z+", zblk[NZ - k]), ("z-", zblk[k])):
            at = (blk, q, *hh)
            arrived(buf, at, (nm, d, k, j, *hh))
            send(buf, at, buf, at, (nm, d, k + 1, j, *hh), dev[d])

    def ag_fwd3(buf, nm, hh=()):
        for d, blk, q in (("z+", zblk[5], 0), ("z-", zblk[3], 1)):
            for j in range(2):
                arrived(buf, (blk, (xl, ol)[j], *hh), (nm, d, 3, j, *hh))
            send(buf, (blk, q, *hh), buf, (blk, q, *hh), (nm, d, 4, *hh), dev[d])

    def ag_last(buf, nm, hh=()):
        arrived(buf, (zblk[4], 0, *hh), (nm, "z+", 4, *hh))
        arrived(buf, (zblk[4], 1, *hh), (nm, "z-", 4, *hh))

    def pair_send(buf, nm, *ks):
        for k in ks:
            at = (zblk[k], xl)
            send(buf, at, buf, at, (nm, "pair", k), dev["xl"])

    def pair_wait(buf, nm, *ks):
        for k in ks:
            arrived(buf, (zblk[k], ol), (nm, "pair", k))

    def own_wait(buf, nm, k):
        for d, b in (("z+", zblk[NZ - k]), ("z-", zblk[k])):
            arrived(buf, (b, xl), (nm, d, k, 0))

    def z_send(buf, nm, k, j):
        for d, b in (("z+", zblk[NZ - k]), ("z-", zblk[k])):
            at = (b, (xl, ol)[j])
            send(buf, at, buf, at, (nm, d, k + 1, j), dev[d])

    def act(buf, i):
        return jnp.concatenate([buf[i, :, h].reshape(PW, TH) for h in range(H)], axis=1)

    def pick(i, table):
        v = table[0]
        for k in range(1, len(table)):
            v = jnp.where(i == k, table[k], v)
        return v

    def together(parts):
        return jnp.concatenate(parts, axis=0)

    def forward(*ks):
        blks = [zblk[k] for k in ks]
        part = dot(
            together([wgu[b] for b in blks]),
            together([n_all[b].reshape(PW, T) for b in blks]),
            0,
            0,
        )
        gu[...] = part if 0 in ks else gu[...] + part

    def dhidden(*ks):
        blks = [zblk[k] for k in ks]
        dys = [act(dy_all, b) for b in blks]
        dy = together(dys)
        parts = (
            (0, dot(together([wd[b, 0:PW] for b in blks]), dy, 0, 0)),
        )
        for r, part in parts:
            at = pl.ds(r, part.shape[0])
            dh[at, :] = part if 0 in ks else dh[at, :] + part
        part = dot(wd[blks[0], PW:DR, 0:PW], dys[0], 1, 0)
        for b, d in zip(blks[1:], dys[1:]):
            part = part + dot(wd[b, PW:DR, 0:PW], d, 1, 0)
        at = pl.ds(DH + 128, 16)
        dh[at, :] = part if 0 in ks else dh[at, :] + part

    def dhidden_mid():
        lhs = together([wgu[b, :, UW - 128 : UW] for b in range(NF)])
        dh[DH : DH + 128, :] = dot(lhs, together([act(dy_all, b) for b in range(NF)]), 0, 0)

    def hidden():
        def body(r):
            gate = gu[pl.ds(r, 16), :]
            up = gu[pl.ds(pl.multiple_of(FL + r, 16), 16), :]
            hid[pl.ds(r, 16), :] = (gate * jax.nn.sigmoid(gate) * up).astype(BF16)

        rows(FL, 48, lambda r: [body(pl.multiple_of(r + k, 16)) for k in (0, 16, 32)])
        hid_mid[0:96, :] = jnp.zeros((96, T), BF16)
        hid_mid[96:128, :] = hid[DH : DH + 32, :]

    def normalize():
        row_scale = lax.rsqrt(collect(ssq_in, tp_peers, "ssq") / D + EPS)
        scale[...] = row_scale
        unit[...] = unit[...] * row_scale

    def norm_own():
        n_all[z, xl] = (unit[...] * gain[:, 0:1]).astype(BF16)

    def norm_blocks(*ks):
        for k in ks:
            b = zblk[k]
            for q in range(NXL):
                g = gain_all[pl.ds(pl.multiple_of(b * PW + q * W, 8), W), :]
                for c in range(T // 128):
                    at = slice(c * 128, (c + 1) * 128)
                    n_all[b, q, :, at] = (
                        x_all[b, q, :, at].astype(F32) * scale[:, at] * g
                    ).astype(BF16)

    def cotangents():
        stat[...] = jnp.zeros_like(stat)
        dgu[GU:UW, :] = jnp.zeros((UW - GU, T), BF16)

        def elementwise(r):
            gate = gu[pl.ds(r, 16), :]
            up = gu[pl.ds(pl.multiple_of(FL + r, 16), 16), :]
            dd = dh[pl.ds(pl.multiple_of(jnp.where(r < DH, r, r + 96), 16), 16), :]
            sig = jax.nn.sigmoid(gate)
            silu = gate * sig
            d_gate = (dd * up * sig * (1.0 + gate * (1.0 - sig))).astype(BF16)
            d_up = (dd * silu).astype(BF16)
            dgu[pl.ds(r, 16), :] = d_gate
            dgu[pl.ds(pl.multiple_of(FL + r, 16), 16), :] = d_up
            both = d_gate.astype(F32) * gate + d_up.astype(F32) * up
            stat[...] += both[0:8] + both[8:16]

        rows(FL, 48, lambda r: [elementwise(pl.multiple_of(r + k, 16)) for k in (0, 16, 32)])
        stat_in[t] = jnp.sum(stat[...], axis=0, keepdims=True)
        spread(stat_in, t, tp_peers, "stat")

    ways = (("z+", 0), ("z-", 1))

    def rs_first():
        def body(h, c):
            part = dot(wgu[zblk[4], :, 0:GU], dgu[0:GU, :], 1, 0).reshape(NXL, W, T)
            for hh in range(H):
                pdn[0, hh] = part[:, :, hh * TH : (hh + 1) * TH].astype(BF16)
            return c

        lax.fori_loop(0, 1, body, 0)
        for h in range(H):
            for d, w in ways:
                send(pdn, (0, h, w), rdn, (w, 0, h, w), ("rs", d, 1, h), dev[d], q=w)

    def rs_compute(k):
        def body(w, c):
            blk = jnp.where(w == 0, zblk[5 - k], zblk[3 + k])
            part = dot(wgu[blk, :, 0:GU], dgu[0:GU, :], 1, 0).reshape(NXL, W, T)
            for hh in range(H):
                pf[k - 2, w, hh] = part[:, :, hh * TH : (hh + 1) * TH]
            return c

        lax.fori_loop(0, 2, body, 0)

    def rs_free():
        for h in range(H):
            for d, w in ways:
                q = 1 - w
                pdn[1 + w, h, q] = pf[0, w, h, q].astype(BF16)
                send(pdn, (1 + w, h, q), rdn, (w, 1, h, q), ("rs", d, 2, h), dev[d], q=q)

    def rs_step(k, ahead=(True, False), hs=range(H)):
        slot = 2 * k - 3
        for first in ahead:
            for h in hs:
                for d, w in ways:
                    q = 1 - w if first else w
                    arrived(rdn, (w, k - 2, h, q), ("rs", d, k - 1, h), q=q)
                    pdn[slot + w, h, q] = (
                        pf[k - 2, w, h, q] + rdn[w, k - 2, h, q].astype(F32)
                    ).astype(BF16)
                    send(pdn, (slot + w, h, q), rdn, (w, k - 1, h, q), ("rs", d, k, h), dev[d], q=q)

    def rs_own():
        def body(h, c):
            part = dot(wgu[z, :, 0:GU], dgu[0:GU, :], 1, 0).reshape(NXL, W, T)
            for hh in range(H):
                pown[hh] = part[:, :, hh * TH : (hh + 1) * TH]
            return c

        lax.fori_loop(0, 1, body, 0)

    def rs_last(h):
        for q in (ol, xl):
            for d, w in ways:
                arrived(rdn, (w, 3, h, q), ("rs", d, 4, h), q=q)
            if q is ol:
                xs[h] = (
                    pown[h, q] + rdn[0, 3, h, q].astype(F32) + rdn[1, 3, h, q].astype(F32)
                ).astype(BF16)
                send(xs, (h,), xr, (h,), ("rx", h), dev["xl"])

    def take_stat():
        nstat[...] = collect(stat_in, tp_peers, "stat") / D

    def dx_part(h):
        arrived(xr, (h,), ("rx", h))
        cols = slice(h * TH, (h + 1) * TH)
        d_normed = (
            pown[h, xl]
            + rdn[0, 3, h, xl].astype(F32)
            + rdn[1, 3, h, xl].astype(F32)
            + xr[h].astype(F32)
        )
        u = unit[:, cols]
        dx = dy_all[z, xl, h].astype(F32) + scale[:, cols] * (
            d_normed * gain[:, 0:1] - u * nstat[:, cols]
        )
        dxs[h] = dx.astype(BF16)
        gx[h] = d_normed * u

    def dx_send(h):
        dx_part(h)
        for d, name in (
            ("xl", ("xl", h)),
            ("z+", ("z+", 1, 0, h)),
            ("z-", ("z-", 1, 0, h)),
            ("core", ("core", h)),
        ):
            send(dxs, (h,), dy_all, (z, xl, h), ("e", *name), across[d])

    def gain_dx():
        total = dot(
            jnp.ones((8, T), F32),
            jnp.concatenate([gx[h] for h in range(H)], axis=1),
            1,
            1,
            lax.Precision.HIGHEST,
        )
        gain_in[f] = total
        spread(gain_in, f, fs_peers, "gain")
        for h in range(H):
            dx_ref[h * TH : (h + 1) * TH, :] = dot(dxs[h], eye, 0, 0).astype(BF16)

    sg, rg, fg = {"u": sgu, "d": sgd}, {"u": rgu, "d": rgd}, {"u": fgu, "d": fgd}
    size_of = {"u": (PW, 32), "d": (DR, 48)}

    def wgrad(a, blk, dst, i):
        dy = act(dy_all, blk)
        if a == "u":
            cut = UW - 128
            n = n_all[blk].reshape(PW, T)
            dst[i, :, 0:cut] = dot(n, dgu[0:cut, :], 1, 1).astype(dst.dtype)
            edge = dot(n, dgu[cut:UW, :], 1, 1) + dot(dy, hid_mid[...], 1, 1)
            dst[i, :, cut:UW] = edge.astype(dst.dtype)
        else:
            dst[i, 0:PW, :] = dot(dy, hid[0:DH, :], 1, 1).astype(dst.dtype)
            dst[i, PW:DR, 0:PW] = dot(hid[FL - 16 : FL, :], dy, 1, 1).astype(dst.dtype)

    direct = [right["o"], left["o"], far["o"]]
    kept = [far["c"], own["o"], right["c"], left["c"], own["c"]]

    def g_first(a, lo=0, hi=3):
        rm = ident(("g", a, 0), 3)
        sm = [take(sg[a], (0,), "big") if lo <= i < hi else 0 for i in range(3)]

        def body(i, c):
            wgrad(a, pick(i, direct), sg[a], i)
            to = pick(i, [dev[d][1] for d in ("y+", "y-", "xh")])
            copy(sg[a].at[i], rg[a].at[i], pick(i, sm), rm + i, (s, to, t)).start()
            return c

        lax.fori_loop(lo, hi, body, 0)

    def g_kept(a, lo, hi):
        def body(i, c):
            wgrad(a, pick(i, kept), fg[a], i)
            return c

        lax.fori_loop(lo, hi, body, 0)

    def g_sum(a, slot, own_i, recv, span=None):
        n, st = size_of[a]
        lo, n = span if span else (0, n)
        st = 16 if span else st

        def body(r):
            r = pl.multiple_of(r + lo, 16)
            v = fg[a][own_i, pl.ds(r, st), :]
            for k in recv:
                v = v + rg[a][k, pl.ds(r, st), :].astype(F32)
            sg[a][slot, pl.ds(r, st), :] = v.astype(BF16)

        rows(n, st, body)

    def g_far(a):
        arrived(rg[a], (2,), ("g", a, 0), q=2)
        g_sum(a, 3, 0, (2,))
        for d, k in (("y+", 0), ("y-", 1)):
            part = pl.ds(*halves[a][k])
            send(sg[a], (3, part), rg[a], (3, part), ("g", a, 3, d), dev[d], kind="big")

    def g_near(a, waits):
        for d, k, slot in (("y+", 0, 4), ("y-", 1, 5)):
            half = halves[a][k if waits else 1 - k]
            part = pl.ds(*half)
            if waits:
                arrived(rg[a], (3, part), ("g", a, 3, d))
            g_sum(a, slot, 2 + k, (3,) if waits else (), half)
            send(sg[a], (slot, part), rg[a], (slot, part), ("g", a, slot, waits), dev[d], kind="big")

    def g_partner(a):
        arrived(rg[a], (0,), ("g", a, 0), q=0)
        arrived(rg[a], (1,), ("g", a, 0), q=1)
        g_sum(a, 6, 1, (0, 1))
        send(sg[a], (6,), rg[a], (6,), ("g", a, 6), dev["xh"], kind="big")

    def g_most(a):
        for k in (0, 1):
            part = pl.ds(*halves[a][1 - k])
            arrived(rg[a], (4 + k, part), ("g", a, 4 + k, False))
        arrived(rg[a], (6,), ("g", a, 6))
        for k in (0, 1):
            lo, n = halves[a][1 - k]

            def body(r, k=k, lo=lo):
                at = pl.ds(pl.multiple_of(r + lo, 16), 16)
                fg[a][4, at, :] += rg[a][4 + k, at, :].astype(F32) + rg[a][6, at, :].astype(F32)

            rows(n, 16, body)

    def g_last(a):
        for k in (0, 1):
            lo, n = halves[a][k]
            arrived(rg[a], (4 + k, pl.ds(lo, n)), ("g", a, 4 + k, True))

            def total(at, k=k):
                return fg[a][4, at, :] + rg[a][4 + k, at, :].astype(F32)

            def body(r, total=total, lo=lo):
                at = pl.ds(pl.multiple_of(r + lo, 16), 32)
                v = total(at)
                if a == "u":
                    gg_ref[at, :] = v[:, 0:FL]
                    ug_ref[at, :] = v[:, FL:GU]
                    dg_ref[at, DH : DH + 32] = v[:, GU:UW]
                else:
                    dg_ref[at, 0:DH] = v

            rows(160, 32, body)
            if n > 160:
                v = total(pl.ds(PW, 16))[:, 0:PW]
                unit16 = (
                    lax.broadcasted_iota(jnp.int32, (16, 16), 0)
                    == lax.broadcasted_iota(jnp.int32, (16, 16), 1)
                ).astype(F32)
                dg_ref[:, DH + 32 : FL] = dot(v, unit16, 0, 0, lax.Precision.HIGHEST)

    def finish():
        gn_ref[...] = collect(gain_in, fs_peers, "gain")[0:1]
        left_all()

    @pl.when(s == 1)
    def _():
        ctx[0] = 1
        ag_own(dy_all, "dy")
        ag_own(x_all, "n")
        w_own_x("d")
        w_own_y("d", 0, 1)
        w_own_y("u", 0, 1)
        w_own_x("u")
        take_gain()
        ag_partner(dy_all, "dy")
        ag_fwd(dy_all, "dy", 1, 0)
        normalize()
        ag_partner(x_all, "n")
        ag_fwd(x_all, "n", 1, 0)
        w_fwd("d")
        ag_fwd(dy_all, "dy", 1, 1)
        ag_fwd(dy_all, "dy", 2, 0)
        w_fwd("u")
        w_pass("d")
        ag_fwd(x_all, "n", 1, 1)
        ag_fwd(x_all, "n", 2, 0)
        w_far("d")
        norm_blocks(0, 1, 7)
        ag_fwd(dy_all, "dy", 2, 1)
        w_pass("u")
        w_far("u")
        ag_fwd(x_all, "n", 2, 1)
        norm_blocks(2, 6)
        ag_fwd3(dy_all, "dy")
        w_last("d")
        dhidden(0, 1, 7)
        ag_fwd3(x_all, "n")
        pl.semaphore_signal(go, inc=1, device_id=dev["core"], device_id_type=MESH)
        norm_blocks(3, 5)
        dhidden(2, 6, 3, 5)
        pl.semaphore_signal(go, inc=1, device_id=dev["core"], device_id_type=MESH)
        w_last("u")
        forward(0, 1, 7)
        forward(2, 6, 3, 5)
        ag_last(x_all, "n")
        norm_blocks(4)
        forward(4)
        ag_last(dy_all, "dy")
        dhidden(4)
        dhidden_mid()
        cotangents()
        rs_first()
        rs_compute(2)
        rs_free()
        rs_step(2, (False,), (0,))
        hidden()
        rs_compute(3)
        rs_step(2, (False,), (1,))
        left_all("big")
        g_first("u", 0, 1)
        rs_step(3, (True,), (0,))
        rs_step(3, (True,), (1,))
        rs_step(3, (False,), (0,))
        rs_compute(4)
        rs_step(3, (False,), (1,))
        g_first("u", 1, 2)
        rs_step(4, (True,), (0,))
        rs_own()
        rs_step(4, (False,), (0,))
        rs_step(4, (False,), (1,))
        rs_step(4, (True,), (1,))
        g_kept("d", 0, 1)
        rs_last(0)
        pl.semaphore_signal(go, inc=1, device_id=dev["core"], device_id_type=MESH)
        g_first("d", 1, 2)
        g_kept("d", 1, 2)
        rs_last(1)
        g_first("d", 0, 1)
        take_stat()
        dx_send(0)
        dx_send(1)
        g_first("u", 2, 3)
        g_kept("u", 1, 2)
        g_kept("u", 0, 1)
        g_first("d", 2, 3)
        g_kept("u", 2, 4)
        g_near("u", False)
        gain_dx()
        g_partner("u")
        g_kept("d", 4, 5)
        g_kept("d", 2, 4)
        g_near("d", False)
        g_far("u")
        g_partner("d")
        g_kept("u", 4, 5)
        g_far("d")
        g_near("u", True)
        g_near("d", True)
        g_most("u")
        g_last("u")
        g_most("d")
        g_last("d")
        finish()
        ctx[0] = None

    @pl.when(s == 0)
    def _():
        ctx[0] = 0
        take_gain()
        normalize()
        norm_own()
        ag_xl(n_all, "m")
        pl.semaphore_wait(go, 1)
        w_own_x("d")
        w_own_y("d", 0, 1)
        w_own_y("u", 0)
        w_own_x("u")
        pl.semaphore_wait(go, 1)
        ag_z(n_all, "m")
        ag_partner(n_all, "m")
        w_fwd("d")
        w_own_y("u", 1)
        own_wait(n_all, "m", 1)
        z_send(n_all, "m", 1, 0)
        w_fwd("u")
        w_pass("d")
        w_far("d")
        own_wait(n_all, "m", 2)
        pair_send(n_all, "m", 2, 6)
        w_pass("u")
        w_far("u")
        pl.semaphore_wait(go, 1)
        z_send(n_all, "m", 2, 0)
        pair_wait(n_all, "m", 2, 6)
        z_send(n_all, "m", 2, 1)
        ag_partner(dy_all, "e", (0,))
        ag_partner(dy_all, "e", (1,))
        ag_fwd(dy_all, "e", 1, 0, (0,))
        ag_fwd(dy_all, "e", 1, 0, (1,))
        ag_fwd(dy_all, "e", 1, 1, (0,))
        ag_fwd(dy_all, "e", 1, 1, (1,))
        w_last("d")
        w_last("u")
        for h in range(H):
            arrived(dy_all, (z, xl, h), ("e", "core", h))
        dhidden(0, 1, 7)
        ag_fwd(dy_all, "e", 2, 0, (0,))
        ag_fwd(dy_all, "e", 2, 0, (1,))
        ag_fwd(dy_all, "e", 2, 1, (0,))
        ag_fwd(dy_all, "e", 2, 1, (1,))
        ag_fwd3(n_all, "m")
        arrived(n_all, (zblk[7], ol), ("m", "z+", 1, 1))
        arrived(n_all, (zblk[1], ol), ("m", "z-", 1, 1))
        forward(0, 1, 7)
        ag_fwd3(dy_all, "e", (0,))
        ag_fwd3(dy_all, "e", (1,))
        forward(2, 6, 3, 5)
        dhidden(2, 6, 3, 5)
        ag_last(n_all, "m")
        forward(4)
        hidden()
        ag_last(dy_all, "e", (0,))
        ag_last(dy_all, "e", (1,))
        dhidden(4)
        dhidden_mid()
        cotangents()
        left_all("big")
        g_first("u", 0, 2)
        rs_first()
        g_first("u", 2, 3)
        rs_compute(2)
        rs_free()
        g_kept("u", 2, 4)
        g_near("u", False)
        g_first("d", 1, 2)
        rs_step(2, (False,), (0,))
        g_kept("u", 1, 2)
        rs_step(2, (False,), (1,))
        rs_compute(3)
        rs_step(3, (True,), (0,))
        g_first("d", 2, 3)
        g_first("d", 0, 1)
        rs_step(3, (True,), (1,))
        rs_compute(4)
        rs_step(3, (False,), (0,))
        rs_own()
        rs_step(3, (False,), (1,))
        g_partner("u")
        rs_step(4, (True,), (0,))
        g_kept("u", 0, 1)
        g_far("u")
        rs_step(4, (True,), (1,))
        g_kept("d", 0, 1)
        rs_step(4, (False,), (0,))
        g_kept("d", 4, 5)
        g_far("d")
        rs_step(4, (False,), (1,))
        g_kept("d", 1, 2)
        g_kept("d", 2, 4)
        g_near("d", False)
        rs_last(0)
        rs_last(1)
        g_near("u", True)
        g_partner("d")
        g_kept("u", 4, 5)
        g_near("d", True)
        take_stat()
        dx_part(0)
        g_most("u")
        dx_part(1)
        gain_dx()
        g_last("u")
        g_most("d")
        g_last("d")
        finish()
        ctx[0] = None

    spread_left(ssq_in, tp_peers, "ssq")
    spread_left(stat_in, tp_peers, "stat")
    spread_left(gain_in, fs_peers, "gain")


def put_kernel(*refs):
    copies = [pltpu.make_async_copy(refs[k], refs[5 + k], refs[10].at[k]) for k in range(5)]
    for c in copies:
        c.start()
    for c in copies:
        c.wait()


def body(saved_inputs, top_grad, norm_gain, gate_weight, up_weight, down_weight):
    x = saved_inputs.reshape(T, W)
    tg = top_grad.reshape(T, W)
    hbm = pl.BlockSpec(memory_space=pl.ANY)
    outs = (
        jax.ShapeDtypeStruct((T, W), BF16),
        jax.ShapeDtypeStruct((PW, FL), F32),
        jax.ShapeDtypeStruct((PW, FL), F32),
        jax.ShapeDtypeStruct((PW, FL), F32),
        jax.ShapeDtypeStruct((1, W), F32),
    )
    out = pl.pallas_call(
        fused_kernel,
        name="fused",
        out_shape=[pltpu.VMEM(o.shape, o.dtype) for o in outs],
        in_specs=[hbm] * 6,
        out_specs=[pl.BlockSpec(memory_space=pltpu.VMEM)] * 5,
        scratch_shapes=[
            pltpu.VMEM((T, W), BF16),
            pltpu.VMEM((T, W), BF16),
            pltpu.VMEM((1, D), F32),
            pltpu.VMEM((PW, FL), BF16),
            pltpu.VMEM((PW, FL), BF16),
            pltpu.VMEM((PW, FL), BF16),
            pltpu.VMEM((W, 128), F32),
            pltpu.VMEM((128, 128), F32),
            pltpu.VMEM((D, 128), F32),
            pltpu.VMEM((NZ, NXL, W, T), BF16),
            pltpu.VMEM((NF, PW, UW), BF16),
            pltpu.VMEM((NF, DR, DH), BF16),
            pltpu.VMEM((NZ, NXL, W, T), BF16),
            pltpu.VMEM((NZ, NXL, H, W, TH), BF16),
            pltpu.VMEM((UW, T), F32),
            pltpu.VMEM((DH + 128 + 16, T), F32),
            pltpu.VMEM((UW, T), BF16),
            pltpu.VMEM((FL, T), BF16),
            pltpu.VMEM((128, T), BF16),
            pltpu.VMEM((W, T), F32),
            pltpu.VMEM((1, T), F32),
            pltpu.VMEM((8, T), F32),
            pltpu.VMEM((NT, 1, T), F32),
            pltpu.VMEM((NT, 1, T), F32),
            pltpu.VMEM((NF, 8, W), F32),
            pltpu.VMEM((7, H, NXL, W, TH), BF16),
            pltpu.VMEM((2, 4, H, NXL, W, TH), BF16),
            pltpu.VMEM((3, 2, H, NXL, W, TH), F32),
            pltpu.VMEM((H, NXL, W, TH), F32),
            pltpu.VMEM((H, W, TH), F32),
            pltpu.VMEM((1, T), F32),
            pltpu.VMEM((H, W, TH), BF16),
            pltpu.VMEM((H, W, TH), BF16),
            pltpu.VMEM((H, W, TH), BF16),
            pltpu.VMEM((7, PW, UW), BF16),
            pltpu.VMEM((7, PW, UW), BF16),
            pltpu.VMEM((5, PW, UW), F32),
            pltpu.VMEM((7, DR, DH), BF16),
            pltpu.VMEM((7, DR, DH), BF16),
            pltpu.VMEM((5, DR, DH), F32),
            pltpu.SemaphoreType.DMA((NBIG + NSMALL + 3,)),
            pltpu.SemaphoreType.DMA((NCOMMON + NEACH,)),
            pltpu.SemaphoreType.DMA((6,)),
            pltpu.SemaphoreType.REGULAR,
        ],
        compiler_params=pltpu.CompilerParams(
            collective_id=0, has_side_effects=True, vmem_limit_bytes=58 * 2**20
        ),
    )(x, tg, norm_gain, gate_weight[0], up_weight[0], down_weight[0].T)
    dx, gg, ug, dg, gn = pl.pallas_call(
        put_kernel,
        name="put",
        out_shape=outs,
        in_specs=[pl.BlockSpec(memory_space=pltpu.VMEM)] * 5,
        out_specs=[hbm] * 5,
        scratch_shapes=[pltpu.SemaphoreType.DMA((5,))],
    )(*[pltpu.with_memory_space_constraint(o, pltpu.VMEM) for o in out])
    return (dx.reshape(1, MICRO, ROWS, W), gg[None], ug[None], dg.T[None], gn)


def solution(mesh):
    return jax.shard_map(
        body,
        mesh=mesh,
        in_specs=(
            P("section", None, "fsdp", "tp"),
            P(None, "fsdp", "tp"),
            P("section", None),
            P("section", "fsdp", "tp"),
            P("section", "fsdp", "tp"),
            P("section", "tp", "fsdp"),
        ),
        out_specs=(
            P("section", None, "fsdp", "tp"),
            P("section", "fsdp", "tp"),
            P("section", "fsdp", "tp"),
            P("section", "tp", "fsdp"),
            P("section", "tp"),
        ),
        check_vma=False,
    )
```
